32 devices in a mesh: heads: 4 (over y, core), blk: 8 (over z, x).
Axes of the slice: x: 2, y: 2, z: 4, core: 2. Of those that a mesh axis runs over, the one named last changes fastest.
Arguments:
- tokens: bfloat16 [4096, 4096], P(('blk', 'heads')), may hold values from -6 to 6
- w_query: bfloat16 [4096, 2048], P('blk', 'heads'), may hold values from -0.75 to 0.75
- key_value_weight: bfloat16 [4096, 2, 512], P('blk', None, 'heads'), may hold values from -0.75 to 0.75
- w_out: bfloat16 [2048, 4096], P(('heads', 'blk')), may hold values from -0.5 to 0.5
- doc_lengths: int32 [16], replicated, may hold values from 1 to 1024, 4096 in all
Outputs:
- attended: bfloat16 [4096, 4096], P(('blk', 'heads'))
The draws below stay inside these ranges and needn't reach their ends.
Inputs may be any that keep to these rules, and one draw needn't show every extreme that they name: `doc_lengths`: the 16 lengths sum to 4096; the longest document has exactly 1024 tokens.
All inputs are finite; a program needn't handle non-finite values.
Results may differ from the reference program's by a relative error of at most 0.012.
Values may be sent and summed in bfloat16 or wider, within the bound.
A program may use at most 128 MiB of HBM per device.

```python
import math
import jax
import jax.numpy as jnp
import numpy as np
from jax import lax

MODEL_WIDTH = 4096
QUERY_HEADS = 16
KEY_VALUE_HEADS = 4
HEAD_SIZE = 128
NDOC = 16
PACK_TOKENS = 4096
BLOCK_TOKENS = 512
DOC_MAX = 1024
REACH = 2


def shared_weights(key):
    expand_heads = MODEL_WIDTH ** (-0.5)
    base_query = jax.random.truncated_normal(jax.random.fold_in(key, 11), -6.0, 6.0, (MODEL_WIDTH, QUERY_HEADS, HEAD_SIZE), jnp.float32) * expand_heads
    unrotated_keys = jax.random.truncated_normal(jax.random.fold_in(key, 12), -6.0, 6.0, (MODEL_WIDTH, KEY_VALUE_HEADS, HEAD_SIZE), jnp.float32) * expand_heads
    projected_values = jax.random.truncated_normal(jax.random.fold_in(key, 13), -6.0, 6.0, (MODEL_WIDTH, KEY_VALUE_HEADS, HEAD_SIZE), jnp.float32) * expand_heads
    key_matrix = unrotated_keys
    query_weights = base_query
    limit = 48.0 * expand_heads
    query_weights = jnp.clip(query_weights, -limit, limit).reshape(MODEL_WIDTH, QUERY_HEADS * HEAD_SIZE)
    key_value_matrix = jnp.stack([key_matrix.reshape(MODEL_WIDTH, KEY_VALUE_HEADS * HEAD_SIZE), projected_values.reshape(MODEL_WIDTH, KEY_VALUE_HEADS * HEAD_SIZE)], axis=1)
    key_value_matrix = jnp.clip(key_value_matrix, -limit, limit)
    return (query_weights, key_value_matrix)


def draw_w_query(key, part):
    return shared_weights(key)[0].astype(jnp.bfloat16)


def draw_key_value_weight(key, part):
    return shared_weights(key)[1].astype(jnp.bfloat16)


def draw_tokens(key, part):
    own_part = jax.random.normal(jax.random.fold_in(key, 21), (PACK_TOKENS, MODEL_WIDTH), jnp.float32)
    result = own_part
    return jnp.clip(result, -6.0, 6.0).astype(jnp.bfloat16)


def block_scale(own_key, dims, cuts, low, high):
    loudness = 1.0
    for position, blocks in cuts:
        steps = jax.random.uniform(jax.random.fold_in(jax.random.fold_in(own_key, 6), position), (blocks,), jnp.float32, low / len(cuts), high / len(cuts))
        loudness = loudness * jnp.repeat(jnp.exp(steps), dims[position] // blocks).reshape((-1,) + (1,) * (len(dims) - 1 - position))
    return loudness


def split_up(count, total, most, slope):
    weights = [(1 << 20) // math.isqrt(rank ** slope) + 1 for rank in range(2, count + 1)]
    surplus, holding = total - most - (count - 1), [1] * (count - 1)
    while surplus > 0:
        movable = [i for i in range(count - 1) if holding[i] < most]
        pool, budget = sum([weights[i] for i in movable]), surplus
        for i in movable:
            more = min(most - holding[i], max(1, budget * weights[i] // pool), surplus)
            holding[i] = holding[i] + more
            surplus = surplus - more
    return np.array([most] + holding)


def ragged_sizes(key, amount, total, most, slope):
    if amount == 2:
        one = jax.random.randint(key, (), max(1, total - most), min(most, total - 1) + 1)
        return jnp.stack([one, total - one])
    sizes = jnp.asarray(split_up(amount, total, most, slope), jnp.int32)
    twos = (amount - 1) // 2
    source_of, sink = sizes[1:1 + 2 * twos:2], sizes[2:2 + 2 * twos:2]
    room = jnp.minimum(source_of - 1, most - sink)
    passed = jax.random.randint(jax.random.fold_in(key, 1), (twos,), 0, 1 << 20) % (room + 1)
    sizes = sizes.at[1:1 + 2 * twos:2].set(source_of - passed).at[2:2 + 2 * twos:2].set(sink + passed)
    return sizes[jax.random.permutation(jax.random.fold_in(key, 2), amount)]


def scatter_about(stream_key, shape, scale, most, split=(), kind=jnp.bfloat16):
    values = jax.random.normal(stream_key, shape, jnp.float32) * scale
    if len(split) > 0:
        values = block_scale(stream_key, shape, split, -0.22, 0.18) * values
    return jnp.clip(values, min=-most, max=most).astype(kind)


def setup_inputs(seed: int = 0) -> dict:
    keys = jax.random.split(jax.random.key(seed), 6)
    return {
        "tokens": draw_tokens(jax.random.fold_in(keys[5], 71), 0),
        "w_query": draw_w_query(jax.random.fold_in(keys[5], 71), 0),
        "key_value_weight": draw_key_value_weight(jax.random.fold_in(keys[5], 71), 0),
        "w_out": scatter_about(keys[3], (QUERY_HEADS * HEAD_SIZE, MODEL_WIDTH), HEAD_SIZE ** -0.5, 0.5, ((0, 32),)),
        "doc_lengths": ragged_sizes(keys[4], NDOC, PACK_TOKENS, DOC_MAX, 2).astype(jnp.int32),
    }


norm_epsilon = 1e-05
rope_base = 500000.0
masked_score = -1e+30

def locate_documents(positions, doc_lengths):
    ends = jnp.cumsum(doc_lengths).astype(jnp.int32)
    after = positions[:, None] >= ends[None, :]
    ident = lax.optimization_barrier(jnp.sum(after.astype(jnp.int32), axis=1))
    starts = lax.optimization_barrier(jnp.sum(jnp.where(after, doc_lengths[None, :], 0), axis=1)).astype(jnp.int32)
    return (ident, starts)

def apply_rotation(values, relative_offset):
    half = values.shape[-1] // 2
    freqs = jnp.power(rope_base, -2.0 * jnp.arange(half, dtype=jnp.float32) / values.shape[-1])
    angle = relative_offset.astype(jnp.float32)[:, None] * freqs[None, :]
    cosine = jnp.cos(angle)[:, None, :]
    sine = jnp.sin(angle)[:, None, :]
    first = values[..., :half]
    second = values[..., half:]
    return jnp.concatenate([first * cosine - second * sine, second * cosine + first * sine], axis=-1)

def reference(tokens, w_query, key_value_weight, w_out, doc_lengths):
    values = tokens.astype(jnp.float32)
    normalized_input = (values * lax.rsqrt(lax.optimization_barrier(jnp.mean(values * values, axis=1, keepdims=True)) + norm_epsilon)).astype(jnp.bfloat16)
    query_raw = jnp.dot(normalized_input, w_query, preferred_element_type=jnp.float32)
    key_value_projected = jnp.dot(normalized_input, key_value_weight.reshape(MODEL_WIDTH, 2 * KEY_VALUE_HEADS * HEAD_SIZE), preferred_element_type=jnp.float32)
    positions = jnp.arange(PACK_TOKENS, dtype=jnp.int32)
    ident, starts = locate_documents(positions, doc_lengths)
    relative_offset = positions - starts
    query_rows = apply_rotation(query_raw.reshape(PACK_TOKENS, QUERY_HEADS, HEAD_SIZE), relative_offset).astype(jnp.bfloat16)
    rotated_keys = apply_rotation(key_value_projected[:, :KEY_VALUE_HEADS * HEAD_SIZE].reshape(PACK_TOKENS, KEY_VALUE_HEADS, HEAD_SIZE), relative_offset).astype(jnp.bfloat16)
    value_rows = key_value_projected[:, KEY_VALUE_HEADS * HEAD_SIZE:].reshape(PACK_TOKENS, KEY_VALUE_HEADS, HEAD_SIZE).astype(jnp.bfloat16)
    front_offset = REACH * BLOCK_TOKENS
    window = (REACH + 1) * BLOCK_TOKENS
    padded_key_rows = jnp.concatenate([jnp.zeros((front_offset, KEY_VALUE_HEADS, HEAD_SIZE), jnp.bfloat16), rotated_keys], axis=0)
    padded_value_rows = jnp.concatenate([jnp.zeros((front_offset, KEY_VALUE_HEADS, HEAD_SIZE), jnp.bfloat16), value_rows], axis=0)
    head_group = QUERY_HEADS // KEY_VALUE_HEADS
    scale = HEAD_SIZE ** (-0.5)

    def one_block(block_index):
        leading_row = (block_index * BLOCK_TOKENS).astype(jnp.int32)
        query_block_rows = lax.dynamic_slice_in_dim(query_rows, leading_row, BLOCK_TOKENS, 0).reshape(BLOCK_TOKENS, KEY_VALUE_HEADS, head_group, HEAD_SIZE).astype(jnp.float32)
        key_block = lax.dynamic_slice_in_dim(padded_key_rows, leading_row, window, 0).astype(jnp.float32)
        value_block = lax.dynamic_slice_in_dim(padded_value_rows, leading_row, window, 0).astype(jnp.float32)
        query_pos = leading_row + jnp.arange(BLOCK_TOKENS, dtype=jnp.int32)
        key_pos = leading_row - front_offset + jnp.arange(window, dtype=jnp.int32)
        query_doc, unused_q = locate_documents(query_pos, doc_lengths)
        key_doc, unused_k = locate_documents(key_pos, doc_lengths)
        keep = (key_pos[None, :] >= 0) & (key_pos[None, :] <= query_pos[:, None]) & (key_doc[None, :] == query_doc[:, None])
        scores = jnp.einsum('qhgd,khd->hgqk', query_block_rows, key_block) * scale
        scores = jnp.where(keep, scores, masked_score)
        highest = lax.optimization_barrier(jnp.max(scores, axis=-1, keepdims=True))
        probs = jnp.where(keep, jnp.exp(scores - highest), 0.0)
        totals = lax.optimization_barrier(jnp.sum(probs, axis=-1))
        probs_b = lax.optimization_barrier(probs.astype(jnp.bfloat16))
        mixed = jnp.einsum('hgqk,khd->hgqd', probs_b.astype(jnp.float32), value_block)
        mixed = mixed / totals[..., None]
        return mixed.transpose(2, 0, 1, 3).reshape(BLOCK_TOKENS, QUERY_HEADS * HEAD_SIZE).astype(jnp.bfloat16)
    mixed_all = lax.map(one_block, jnp.arange(PACK_TOKENS // BLOCK_TOKENS, dtype=jnp.int32)).reshape(PACK_TOKENS, QUERY_HEADS * HEAD_SIZE)
    return jnp.dot(mixed_all, w_out, preferred_element_type=jnp.float32).astype(jnp.bfloat16)
```

```python
import functools

import jax
import jax.numpy as jnp
import numpy as np
from jax import lax
from jax.experimental import pallas as pl
from jax.experimental.pallas import tpu as pltpu
from jax.sharding import PartitionSpec as P

HEAD_SIZE = 128
LINE = 2
Q_UNITS = 2
CHUNKS = 4

norm_epsilon = 1e-05
rope_base = 500000.0
masked_score = -1e30
MESH = pl.DeviceIdType.MESH
UP, DOWN = 0, 1


def layer_kernel(
    n, heads, chunks, q_units,
    tok_ref, w_query_ref, w_keyval_ref, w_out_ref, len_ref, freq_ref, out_ref,
    w_kv, w_q, w_proj, kv_stage, act_stage, acts, qkv, query, kv, high, total, accum, mixed, rope, osend, obuf,
    line_send, mate_send, recv, cross_send, local_sem, redis_send, redis_recv,
    act_send, act_recv, kv_send, kv_recv, mix_send, mix_recv, out_send, out_recv,
):
    f32, bf16 = jnp.float32, jnp.bfloat16
    b = lax.axis_index("blk")
    h = lax.axis_index("heads")
    steps = n // LINE
    z, x = b // LINE, b % LINE
    y, core = h // 2, h % 2
    group = 2 * y + x
    block_id = LINE * z + core
    apart = (x + core) % 2
    reach = n // 4
    own, width = tok_ref.shape
    rows_in = w_query_ref.shape[0]
    block = own * heads
    q_cols = query.shape[1]
    q_heads = q_cols // HEAD_SIZE
    unit_cols = q_cols // q_units
    unit_heads = q_heads // q_units
    col_width = width // heads
    chunk_cols = col_width // chunks
    half = width // 2
    first_out = 1 + q_units
    units = first_out + chunks

    def dev(x_, y_, z_, c_):
        return {"blk": LINE * z_ + x_, "heads": 2 * y_ + c_}

    mate = dev(x, y, z, 1 - core)

    def remote(src, dst, ss, rs, device):
        return pltpu.make_async_remote_copy(
            src_ref=src, dst_ref=dst, send_sem=ss, recv_sem=rs, device_id=device, device_id_type=MESH
        )

    barrier = pltpu.get_barrier_semaphore()
    for dx, dy, dc in [(i, j, k) for i in (0, 1) for j in (0, 1) for k in (0, 1) if i + j + k]:
        pl.semaphore_signal(
            barrier, inc=1, device_id=dev((x + dx) % 2, (y + dy) % 2, z, (core + dc) % 2), device_id_type=MESH
        )
    span = (reach + 1) // 2
    for d in range(1, span + 1):
        for c_ in (0, 1):
            @pl.when(z + d < steps)
            def _():
                pl.semaphore_signal(barrier, inc=1, device_id=dev(x, y, z + d, c_), device_id_type=MESH)

            @pl.when(z - d >= 0)
            def _():
                pl.semaphore_signal(barrier, inc=1, device_id=dev(x, y, z - d, c_), device_id_type=MESH)
    near = jnp.minimum(z, span) + jnp.minimum(steps - 1 - z, span)
    pl.semaphore_wait(barrier, 7 + 2 * near)

    def unit_ref(u, k, row):
        i = LINE * row + k
        if u == 0:
            return w_kv.at[pl.ds(pl.multiple_of(i * rows_in, rows_in), rows_in)]
        if u < first_out:
            return w_q.at[u - 1, pl.ds(pl.multiple_of(i * rows_in, rows_in), rows_in)]
        return w_proj.at[:, k, pl.ds(LINE * row, LINE), :, pl.ds((u - first_out) * chunk_cols, chunk_cols)]

    def line_copy(u, direction, row):
        ref = unit_ref(u, core, row)
        z_ = z + 1 if direction == UP else z - 1
        return remote(ref, ref, line_send.at[u, direction, row], recv.at[u, core, row], dev(x, y, z_, core))

    def mate_copy(u, row):
        ref = unit_ref(u, core, row)
        return remote(ref, ref, mate_send.at[u, row], recv.at[u, core, row], mate)

    def arrive(u, k, row):
        ref = unit_ref(u, k, row)
        remote(ref, ref, mate_send.at[u, 0], recv.at[u, k, row], mate).wait_recv()

    def query_cols(u):
        return w_query_ref.at[:, pl.ds((u - 1) * unit_cols, unit_cols)]

    def cross_copy(u):
        src = kv_stage if u == 0 else query_cols(u)
        return remote(src, unit_ref(u, x, z), cross_send.at[u], recv.at[u, x, z], dev(1 - x, y, z, 1 - core))

    def keep_query(u):
        return pltpu.make_async_copy(query_cols(u), unit_ref(u, core, z), local_sem.at[u])

    def own_start(u):
        @pl.when(z < steps - 1)
        def _():
            line_copy(u, UP, z).start()

        @pl.when(z > 0)
        def _():
            line_copy(u, DOWN, z).start()

        mate_copy(u, z).start()

    def redis_peers():
        return [(1 - x, y), (x, 1 - y), (1 - x, 1 - y)]

    def redis_copy(i, x_, y_):
        cols = pl.ds(pl.multiple_of((2 * y_ + x_) * col_width, col_width), col_width)
        return remote(
            w_out_ref.at[:, cols], w_proj.at[y, core, b], redis_send.at[i], redis_recv.at[group],
            dev(x_, y_, z, core),
        )

    def keep_out():
        cols = pl.ds(pl.multiple_of(group * col_width, col_width), col_width)
        return pltpu.make_async_copy(w_out_ref.at[:, cols], w_proj.at[y, core, b], local_sem.at[0])

    def own_wait(u):
        if u == 0:
            @pl.when(apart == 1)
            def _():
                arrive(u, core, z)
        elif u < first_out:
            @pl.when(apart == 1)
            def _():
                arrive(u, core, z)

            @pl.when(apart == 0)
            def _():
                keep_query(u).wait()
        elif u == first_out:
            keep_out().wait()
            for x_, y_ in redis_peers():
                ref = w_proj.at[y_, core, LINE * z + x_]
                remote(ref, ref, redis_send.at[0], redis_recv.at[2 * y_ + x_], mate).wait_recv()

    def line_step(u, s):
        @pl.when(z - s >= 0)
        def _():
            arrive(u, core, z - s)

            @pl.when(z < steps - 1)
            def _():
                line_copy(u, UP, z - s).start()

            mate_copy(u, z - s).start()

        @pl.when(z + s <= steps - 1)
        def _():
            arrive(u, core, z + s)

            @pl.when(z > 0)
            def _():
                line_copy(u, DOWN, z + s).start()

            mate_copy(u, z + s).start()

    def line_steps(u, low, high_):
        def one(s, _):
            line_step(u, s)
            return 0

        lax.fori_loop(low, high_, one, 0)

    inner = (z > 0) & (z < steps - 1)

    def inner_steps(u, low, high_):
        @pl.when(inner)
        def _():
            line_steps(u, low, high_)

    def outer_steps(u, low, high_):
        @pl.when(jnp.logical_not(inner))
        def _():
            line_steps(u, low, high_)

    def mate_wait(u):
        def one(row, _):
            arrive(u, 1 - core, row)
            return 0

        lax.fori_loop(0, steps, one, 0)

    own_kv = w_keyval_ref[...].reshape(rows_in, w_kv.shape[1])

    @pl.when(apart == 0)
    def _():
        w_kv[pl.ds(pl.multiple_of(b * rows_in, rows_in), rows_in), :] = own_kv
        own_start(0)
        for u in range(1, first_out):
            keep_query(u).start()

    @pl.when(apart == 1)
    def _():
        kv_stage[...] = own_kv
        for u in range(first_out):
            cross_copy(u).start()

    keep_out().start()

    values = tok_ref[...].astype(f32)
    normed = (
        values * lax.rsqrt(jnp.mean(values * values, axis=1, keepdims=True) + norm_epsilon)
    ).astype(bf16)
    act_stage[...] = normed

    @pl.when(apart == 0)
    def _():
        acts[h] = normed

    def act_ref(h_, f):
        return acts.at[h_, :, pl.ds(pl.multiple_of(f * half, half), half)]

    def act_copy(i, h_, f, device, src=None):
        src = act_ref(h_, f) if src is None else src
        return remote(src, act_ref(h_, f), act_send.at[i], act_recv.at[f, h_], device)

    def act_own(i, f, device):
        return act_copy(i, h, f, device, act_stage.at[:, pl.ds(f * half, half)])

    def act_wait(h_, f):
        remote(act_ref(h_, f), act_ref(h_, f), act_send.at[0], act_recv.at[f, h_], mate).wait_recv()

    act_copies = [
        act_own(0, 1, dev(x, 1 - y, z, x)),
        act_own(1, 0, dev(1 - x, y, z, x)),
        act_own(2, 0, dev(x, 1 - y, z, x)),
        act_own(3, 1, dev(1 - x, y, z, x)),
    ]
    act_mate = [act_own(4 + f, f, mate) for f in (0, 1)]
    for copy in act_copies:
        copy.start()

    @pl.when(apart == 1)
    def _():
        for copy in act_mate:
            copy.start()

    redis_copies = [redis_copy(i, x_, y_) for i, (x_, y_) in enumerate(redis_peers())]
    for copy in redis_copies:
        copy.start()

    relay_half = 1 - apart
    relay_y = apart * y + (1 - apart) * (1 - y)
    relay_to = dev(
        apart * x + (1 - apart) * (1 - x), apart * (1 - y) + (1 - apart) * y, z, core
    )
    relays = [act_copy(6 + c, 2 * relay_y + c, relay_half, relay_to) for c in (0, 1)]

    def relay():
        for c, copy in enumerate(relays):
            act_wait(2 * relay_y + c, relay_half)
            copy.start()

    def acts_wait():
        for h_ in range(heads):
            for f in (0, 1):
                mine = (apart == 0) & (h == h_)
                relayed = (relay_half == f) & (relay_y == h_ // 2)

                @pl.when(jnp.logical_not(mine | relayed))
                def _():
                    act_wait(h_, f)

    @pl.when(apart == 1)
    def _():
        own_wait(0)
        own_start(0)

    pos = block_id * block + lax.broadcasted_iota(jnp.int32, (block, 1), 0)
    start = jnp.zeros((block, 1), jnp.int32)
    end = jnp.int32(0)
    for i in range(len_ref.shape[0]):
        size = len_ref[i]
        end = end + size
        start = start + jnp.where(pos >= end, size, 0)
    angle = (pos - start).astype(f32) * freq_ref[...]
    lane = lax.broadcasted_iota(jnp.int32, (block, HEAD_SIZE), 1)
    rope[0] = jnp.cos(angle)
    rope[1] = jnp.where(lane < HEAD_SIZE // 2, -jnp.sin(angle), jnp.sin(angle))
    qkv[...] = jnp.zeros_like(qkv)

    own_wait(1)
    own_start(1)
    line_steps(0, 1, 2)
    relay()
    line_steps(0, 2, steps)
    for u in range(2, first_out):
        own_wait(u)
        own_start(u)
        line_steps(u - 1, 1, steps)
    last_in = first_out - 1
    line_steps(last_in, 1, 2)
    acts_wait()

    depth = min(1024, width)

    def project(weights, cols):
        def one(k, _):
            rows = pl.ds(pl.multiple_of(k * depth, depth), depth)
            left = acts[:, :, rows].reshape(block, depth)
            qkv[:, cols] += jnp.dot(left, weights[rows, :], preferred_element_type=f32)
            return 0

        lax.fori_loop(0, width // depth, one, 0)

    def rotated(first):
        v = qkv[:, first:first + HEAD_SIZE]
        return (v * rope[0] + pltpu.roll(v, HEAD_SIZE // 2, 1) * rope[1]).astype(bf16)

    def project_query(u):
        mate_wait(u)
        first = (u - 1) * unit_cols
        project(w_q.at[u - 1], slice(first, first + unit_cols))
        for j in range(first // HEAD_SIZE, (first + unit_cols) // HEAD_SIZE):
            query[:, j * HEAD_SIZE:(j + 1) * HEAD_SIZE] = rotated(j * HEAD_SIZE)

    def kv_copy(d):
        to = block_id + d
        return remote(
            kv.at[0], kv.at[d], kv_send.at[d], kv_recv.at[d], dev(x, y, to // LINE, to % LINE)
        )

    def kv_start(d, _):
        @pl.when(block_id + d < n)
        def _():
            kv_copy(d).start()
        return 0

    own_pos = lax.broadcasted_iota(jnp.int32, (block, 1), 0)
    own_start_pos = start - block_id * block
    key_lane = lax.broadcasted_iota(jnp.int32, (1, block), 1)
    scale = HEAD_SIZE ** (-0.5) * float(np.log2(np.e))

    def attend_own(u):
        def one(j, _):
            cols = pl.ds(pl.multiple_of(j * HEAD_SIZE, HEAD_SIZE), HEAD_SIZE)
            keep = (key_lane >= own_start_pos) & (key_lane <= own_pos)
            scores = lax.dot_general(
                query[:, cols], kv[0, :, :HEAD_SIZE], (((1,), (1,)), ((), ())),
                preferred_element_type=f32,
            )
            scores = jnp.where(keep, scores, masked_score)
            new = jnp.max(scores, axis=1, keepdims=True)
            probs = jnp.exp2((scores - new) * scale)
            high[j] = new
            total[j] = jnp.sum(probs, axis=1, keepdims=True)
            accum[:, cols] = jnp.dot(probs.astype(bf16), kv[0, :, HEAD_SIZE:], preferred_element_type=f32)
            return 0

        lax.fori_loop((u - 1) * unit_heads, u * unit_heads, one, 0)

    def attend_earlier(u, d):
        keep = key_lane - d * block >= own_start_pos

        def one(j, _):
            cols = pl.ds(pl.multiple_of(j * HEAD_SIZE, HEAD_SIZE), HEAD_SIZE)
            scores = lax.dot_general(
                query[:, cols], kv[d, :, :HEAD_SIZE], (((1,), (1,)), ((), ())),
                preferred_element_type=f32,
            )
            scores = jnp.where(keep, scores, masked_score)
            old = high[j]
            new = jnp.maximum(old, jnp.max(scores, axis=1, keepdims=True))
            fading = jnp.exp2((old - new) * scale)
            probs = jnp.exp2((scores - new) * scale)
            total[j] = total[j] * fading + jnp.sum(probs, axis=1, keepdims=True)
            update = jnp.dot(probs.astype(bf16), kv[d, :, HEAD_SIZE:], preferred_element_type=f32)
            accum[:, cols] = accum[:, cols] * fading + update
            high[j] = new
            return 0

        lax.fori_loop((u - 1) * unit_heads, u * unit_heads, one, 0)

    def mix_cols(u):
        return pl.ds((u - 1) * unit_cols, unit_cols)

    def mix_copy(u, i, x_, y_):
        ref = mixed.at[group, :, mix_cols(u)]
        return remote(ref, ref, mix_send.at[u - 1, i], mix_recv.at[u - 1, group], dev(x_, y_, z, core))

    def finish_heads(u, first):
        def one(d, _):
            @pl.when(block_id >= d)
            def _():
                if first:
                    remote(kv.at[d], kv.at[d], kv_send.at[d], kv_recv.at[d], mate).wait_recv()
                attend_earlier(u, d)
            return 0

        lax.fori_loop(1, reach + 1, one, 0)
        for j in range((u - 1) * unit_heads, u * unit_heads):
            cols = slice(j * HEAD_SIZE, (j + 1) * HEAD_SIZE)
            mixed[group, :, cols] = (accum[:, cols] / total[j]).astype(bf16)
        for i, (x_, y_) in enumerate(redis_peers()):
            mix_copy(u, i, x_, y_).start()

    def mix_wait():
        for u in range(1, first_out):
            for x_, y_ in redis_peers():
                ref = mixed.at[2 * y_ + x_, :, mix_cols(u)]
                remote(ref, ref, mix_send.at[0, 0], mix_recv.at[u - 1, 2 * y_ + x_], mate).wait_recv()

    mate_wait(0)
    project(w_kv, slice(q_cols, q_cols + w_kv.shape[1]))
    kv[0, :, :HEAD_SIZE] = rotated(q_cols)
    kv[0, :, HEAD_SIZE:] = qkv[:, q_cols + HEAD_SIZE:].astype(bf16)
    lax.fori_loop(1, reach + 1, kv_start, 0)
    own_wait(first_out)
    own_start(first_out)
    inner_steps(last_in, 2, steps)
    for u in range(1, last_in):
        project_query(u)
        attend_own(u)
    outer_steps(last_in, 2, steps)
    own_start(first_out + 1)
    inner_steps(first_out, 1, steps)
    project_query(last_in)
    attend_own(last_in)
    own_start(first_out + 2)
    inner_steps(first_out + 1, 1, steps)
    finish_heads(1, True)
    for u in range(first_out + 2, units):
        if u + 1 < units:
            own_start(u + 1)
        inner_steps(u, 1, steps)
        if u == first_out + 2:
            for i in range(2, first_out):
                finish_heads(i, False)

    def out_copy(c, r):
        cols = pl.ds(pl.multiple_of(group * col_width + c * chunk_cols, chunk_cols), chunk_cols)
        return remote(
            osend.at[c, r], obuf.at[:, cols], out_send.at[c, r], out_recv.at[c, group],
            dev(core, r // 2, z, r % 2),
        )

    def away(r):
        return (apart == 1) | (h != r)

    def project_out(c):
        cols = slice(c * chunk_cols, (c + 1) * chunk_cols)
        result = None
        for g in range(heads):
            right = w_proj[g // 2, g % 2, :, :, cols]
            if right.shape[1] % 16:
                right = right.astype(f32).reshape(-1, chunk_cols).astype(bf16)
            else:
                right = right.reshape(-1, chunk_cols)
            term = jnp.dot(mixed[g], right, preferred_element_type=f32)
            result = term if result is None else result + term
        osend[c] = result.astype(bf16).reshape(heads, own, chunk_cols)
        for r in range(heads):
            @pl.when(away(r))
            def _():
                out_copy(c, r).start()

        @pl.when(apart == 0)
        def _():
            at = pl.ds(pl.multiple_of(group * col_width + c * chunk_cols, chunk_cols), chunk_cols)
            obuf[:, at] = osend[c, h]

    for c in range(chunks):
        outer_steps(first_out + c, 1, steps)
        mate_wait(first_out + c)
        if c == 0:
            mix_wait()
        project_out(c)

    for c in range(chunks):
        for g in range(heads):
            @pl.when((apart == 1) | (group != g))
            def _():
                first = g * col_width + c * chunk_cols
                ref = obuf.at[:, pl.ds(first, chunk_cols)]
                remote(ref, ref, out_send.at[0, 0], out_recv.at[c, g], mate).wait_recv()
    out_ref[...] = obuf[...]

    for u in range(units):
        def one(row, _):
            @pl.when((row <= z) & (z < steps - 1))
            def _():
                line_copy(u, UP, row).wait_send()

            @pl.when((row >= z) & (z > 0))
            def _():
                line_copy(u, DOWN, row).wait_send()

            mate_copy(u, row).wait_send()
            return 0

        lax.fori_loop(0, steps, one, 0)

    @pl.when(apart == 1)
    def _():
        for u in range(first_out):
            cross_copy(u).wait_send()
        for copy in act_mate:
            copy.wait_send()

    for copy in act_copies + relays + redis_copies:
        copy.wait_send()

    def kv_drain(d, _):
        @pl.when(block_id + d < n)
        def _():
            kv_copy(d).wait_send()
        return 0

    lax.fori_loop(1, reach + 1, kv_drain, 0)
    for u in range(1, first_out):
        for i, (x_, y_) in enumerate(redis_peers()):
            mix_copy(u, i, x_, y_).wait_send()
    for c in range(chunks):
        for r in range(heads):
            @pl.when(away(r))
            def _():
                out_copy(c, r).wait_send()


def on_device(tokens, w_query, key_value_weight, w_out, doc_lengths):
    n = lax.axis_size("blk")
    heads = lax.axis_size("heads")
    assert heads == 4
    chunks, q_units = CHUNKS, Q_UNITS
    steps = n // LINE
    own, width = tokens.shape
    block = own * heads
    rows_in, q_cols = w_query.shape
    kv_cols = 2 * key_value_weight.shape[2]
    rows_out = w_out.shape[0]
    col_width = width // heads
    chunk_cols = col_width // chunks
    q_heads = q_cols // HEAD_SIZE
    reach = n // 4
    units = 1 + q_units + chunks
    half = HEAD_SIZE // 2
    freqs = np.power(rope_base, -2.0 * np.arange(half) / HEAD_SIZE).astype(np.float32)
    freqs = jnp.asarray(np.concatenate([freqs, freqs])[None, :])
    bf16, f32 = jnp.bfloat16, jnp.float32
    dma = pltpu.SemaphoreType.DMA
    return pl.pallas_call(
        functools.partial(layer_kernel, n, heads, chunks, q_units),
        out_shape=jax.ShapeDtypeStruct((own, width), bf16),
        in_specs=[
            pl.BlockSpec(memory_space=pltpu.VMEM),
            pl.BlockSpec(memory_space=pl.ANY),
            pl.BlockSpec(memory_space=pltpu.VMEM),
            pl.BlockSpec(memory_space=pl.ANY),
            pl.BlockSpec(memory_space=pltpu.SMEM),
            pl.BlockSpec(memory_space=pltpu.VMEM),
        ],
        out_specs=pl.BlockSpec(memory_space=pltpu.VMEM),
        scratch_shapes=[
            pltpu.VMEM((n * rows_in, kv_cols), bf16),
            pltpu.VMEM((q_units, n * rows_in, q_cols // q_units), bf16),
            pltpu.VMEM((2, 2, n, rows_out, col_width), bf16),
            pltpu.VMEM((rows_in, kv_cols), bf16),
            pltpu.VMEM((own, width), bf16),
            pltpu.VMEM((heads, own, width), bf16),
            pltpu.VMEM((block, q_cols + kv_cols), f32),
            pltpu.VMEM((block, q_cols), bf16),
            pltpu.VMEM((reach + 1, block, kv_cols), bf16),
            pltpu.VMEM((q_heads, block, 1), f32),
            pltpu.VMEM((q_heads, block, 1), f32),
            pltpu.VMEM((block, q_cols), f32),
            pltpu.VMEM((heads, block, q_cols), bf16),
            pltpu.VMEM((2, block, HEAD_SIZE), f32),
            pltpu.VMEM((chunks, heads, own, chunk_cols), bf16),
            pltpu.VMEM((own, width), bf16),
            dma((units, 2, steps)),
            dma((units, steps)),
            dma((units, 2, steps)),
            dma((1 + q_units,)),
            dma((1 + q_units,)),
            dma((3,)),
            dma((heads,)),
            dma((8,)),
            dma((2, heads)),
            dma((reach + 1,)),
            dma((reach + 1,)),
            dma((q_units, 3)),
            dma((q_units, heads)),
            dma((chunks, heads)),
            dma((chunks, heads)),
        ],
        compiler_params=pltpu.CompilerParams(
            collective_id=0, has_side_effects=True, vmem_limit_bytes=60 * 1024 * 1024
        ),
    )(tokens, w_query, key_value_weight, w_out, doc_lengths, freqs)


def solution(mesh):
    return jax.shard_map(
        on_device,
        mesh=mesh,
        in_specs=(
            P(("blk", "heads"), None),
            P("blk", "heads"),
            P("blk", None, "heads"),
            P(("heads", "blk"), None),
            P(),
        ),
        out_specs=P(("blk", "heads"), None),
        check_vma=False,
    )
```

```python
import functools

import jax
import jax.numpy as jnp
import numpy as np
from jax import lax
from jax.experimental import pallas as pl
from jax.experimental.pallas import tpu as pltpu
from jax.sharding import PartitionSpec as P

HEAD_SIZE = 128
LINE = 2
Q_UNITS = 2
OUT_PARTS = (2, 2, 2, 1, 1)
LEFT_PARTS = (5, 8)

norm_epsilon = 1e-05
rope_base = 500000.0
masked_score = -1e30
MESH = pl.DeviceIdType.MESH
UP, DOWN = 0, 1


def layer_kernel(
    n, heads, out_cols, q_units,
    tok_ref, w_query_ref, w_keyval_ref, w_out_ref, len_ref, freq_ref, out_ref,
    w_kv, w_q, w_proj, kv_stage, act_stage, acts, qkv, query, kv, high, total, accum, mixed, rope, osend, obuf,
    line_send, mate_send, recv, cross_send, local_sem, redis_send, redis_recv,
    act_send, act_recv, kv_send, kv_recv, kv_pass_send, mix_send, mix_recv, out_send, out_recv,
):
    f32, bf16 = jnp.float32, jnp.bfloat16
    b = lax.axis_index("blk")
    h = lax.axis_index("heads")
    steps = n // LINE
    z, x = b // LINE, b % LINE
    y, core = h // 2, h % 2
    group = 2 * y + x
    block_id = LINE * z + core
    apart = (x + core) % 2
    reach = n // 4
    own, width = tok_ref.shape
    rows_in = w_query_ref.shape[0]
    block = own * heads
    q_cols = query.shape[1]
    q_heads = q_cols // HEAD_SIZE
    unit_cols = q_cols // q_units
    unit_heads = q_heads // q_units
    col_width = width // heads
    chunks = len(out_cols)
    out_first = [sum(out_cols[:c]) for c in range(chunks)]
    left = width * LEFT_PARTS[0] // LEFT_PARTS[1]
    first_out = 1 + q_units
    units = first_out + chunks

    def dev(x_, y_, z_, c_):
        return {"blk": LINE * z_ + x_, "heads": 2 * y_ + c_}

    mate = dev(x, y, z, 1 - core)

    def remote(src, dst, ss, rs, device):
        return pltpu.make_async_remote_copy(
            src_ref=src, dst_ref=dst, send_sem=ss, recv_sem=rs, device_id=device, device_id_type=MESH
        )

    barrier = pltpu.get_barrier_semaphore()
    for dx, dy, dc in [(i, j, k) for i in (0, 1) for j in (0, 1) for k in (0, 1) if i + j + k]:
        pl.semaphore_signal(
            barrier, inc=1, device_id=dev((x + dx) % 2, (y + dy) % 2, z, (core + dc) % 2), device_id_type=MESH
        )
    span = (reach + 1) // 2
    for d in range(1, span + 1):
        for c_ in (0, 1):
            @pl.when(z + d < steps)
            def _():
                pl.semaphore_signal(barrier, inc=1, device_id=dev(x, y, z + d, c_), device_id_type=MESH)

            @pl.when(z - d >= 0)
            def _():
                pl.semaphore_signal(barrier, inc=1, device_id=dev(x, y, z - d, c_), device_id_type=MESH)
    near = jnp.minimum(z, span) + jnp.minimum(steps - 1 - z, span)
    pl.semaphore_wait(barrier, 7 + 2 * near)

    def unit_ref(u, k, row):
        i = LINE * row + k
        if u == 0:
            return w_kv.at[pl.ds(pl.multiple_of(i * rows_in, rows_in), rows_in)]
        if u < first_out:
            return w_q.at[u - 1, pl.ds(pl.multiple_of(i * rows_in, rows_in), rows_in)]
        return w_proj.at[:, k, pl.ds(LINE * row, LINE), :, pl.ds(out_first[u - first_out], out_cols[u - first_out])]

    def line_copy(u, direction, row):
        ref = unit_ref(u, core, row)
        z_ = z + 1 if direction == UP else z - 1
        return remote(ref, ref, line_send.at[u, direction, row], recv.at[u, core, row], dev(x, y, z_, core))

    def mate_copy(u, row):
        ref = unit_ref(u, core, row)
        return remote(ref, ref, mate_send.at[u, row], recv.at[u, core, row], mate)

    def arrive(u, k, row):
        ref = unit_ref(u, k, row)
        remote(ref, ref, mate_send.at[u, 0], recv.at[u, k, row], mate).wait_recv()

    def query_cols(u):
        return w_query_ref.at[:, pl.ds((u - 1) * unit_cols, unit_cols)]

    def cross_copy(u):
        src = kv_stage if u == 0 else query_cols(u)
        return remote(src, unit_ref(u, x, z), cross_send.at[u], recv.at[u, x, z], dev(1 - x, y, z, 1 - core))

    def keep_query(u):
        return pltpu.make_async_copy(query_cols(u), unit_ref(u, core, z), local_sem.at[u])

    def own_start(u):
        @pl.when(z < steps - 1)
        def _():
            line_copy(u, UP, z).start()

        @pl.when(z > 0)
        def _():
            line_copy(u, DOWN, z).start()

        mate_copy(u, z).start()

    def redis_peers():
        return [(1 - x, y), (x, 1 - y), (1 - x, 1 - y)]

    def redis_copy(i, x_, y_):
        cols = pl.ds(pl.multiple_of((2 * y_ + x_) * col_width, col_width), col_width)
        return remote(
            w_out_ref.at[:, cols], w_proj.at[y, core, b], redis_send.at[i], redis_recv.at[group],
            dev(x_, y_, z, core),
        )

    def keep_out():
        cols = pl.ds(pl.multiple_of(group * col_width, col_width), col_width)
        return pltpu.make_async_copy(w_out_ref.at[:, cols], w_proj.at[y, core, b], local_sem.at[0])

    def own_wait(u):
        if u == 0:
            @pl.when(apart == 1)
            def _():
                arrive(u, core, z)
        elif u < first_out:
            @pl.when(apart == 1)
            def _():
                arrive(u, core, z)

            @pl.when(apart == 0)
            def _():
                keep_query(u).wait()
        elif u == first_out:
            keep_out().wait()
            for x_, y_ in redis_peers():
                ref = w_proj.at[y_, core, LINE * z + x_]
                remote(ref, ref, redis_send.at[0], redis_recv.at[2 * y_ + x_], mate).wait_recv()

    def line_step(u, s):
        @pl.when(z - s >= 0)
        def _():
            arrive(u, core, z - s)

            @pl.when(z < steps - 1)
            def _():
                line_copy(u, UP, z - s).start()

            mate_copy(u, z - s).start()

        @pl.when(z + s <= steps - 1)
        def _():
            arrive(u, core, z + s)

            @pl.when(z > 0)
            def _():
                line_copy(u, DOWN, z + s).start()

            mate_copy(u, z + s).start()

    def line_steps(u, low, high_):
        def one(s, _):
            line_step(u, s)
            return 0

        lax.fori_loop(low, high_, one, 0)

    inner = (z > 0) & (z < steps - 1)

    def inner_steps(u, low, high_):
        @pl.when(inner)
        def _():
            line_steps(u, low, high_)

    def outer_steps(u, low, high_):
        @pl.when(jnp.logical_not(inner))
        def _():
            line_steps(u, low, high_)

    def mate_wait(u):
        def one(row, _):
            arrive(u, 1 - core, row)
            return 0

        lax.fori_loop(0, steps, one, 0)

    own_kv = w_keyval_ref[...].reshape(rows_in, w_kv.shape[1])

    @pl.when(apart == 0)
    def _():
        w_kv[pl.ds(pl.multiple_of(b * rows_in, rows_in), rows_in), :] = own_kv
        own_start(0)
        for u in range(1, first_out):
            keep_query(u).start()

    @pl.when(apart == 1)
    def _():
        kv_stage[...] = own_kv
        for u in range(2):
            cross_copy(u).start()

    keep_out().start()

    values = tok_ref[...].astype(f32)
    normed = (
        values * lax.rsqrt(jnp.mean(values * values, axis=1, keepdims=True) + norm_epsilon)
    ).astype(bf16)
    act_stage[...] = normed

    @pl.when(apart == 0)
    def _():
        acts[h] = normed

    act_cols = [(0, left), (left, width - left)]

    def act_ref(h_, f):
        return acts.at[h_, :, pl.ds(*act_cols[f])]

    def act_copy(i, h_, f, device, src=None):
        src = act_ref(h_, f) if src is None else src
        return remote(src, act_ref(h_, f), act_send.at[i], act_recv.at[f, h_], device)

    def act_own(i, f, device):
        return act_copy(i, h, f, device, act_stage.at[:, pl.ds(*act_cols[f])])

    def act_wait(h_, f):
        remote(act_ref(h_, f), act_ref(h_, f), act_send.at[0], act_recv.at[f, h_], mate).wait_recv()

    act_copies = [
        act_own(0, 1, dev(x, 1 - y, z, x)),
        act_own(1, 0, dev(1 - x, y, z, x)),
        act_own(2, 0, dev(x, 1 - y, z, x)),
        act_own(3, 1, dev(1 - x, y, z, x)),
    ]
    act_mate = [act_own(4 + f, f, mate) for f in (0, 1)]
    act_copies[0].start()
    act_copies[1].start()

    @pl.when(apart == 1)
    def _():
        for u in range(2, first_out):
            cross_copy(u).start()
        for copy in act_mate:
            copy.start()

    act_copies[2].start()
    act_copies[3].start()
    redis_copies = [redis_copy(i, x_, y_) for i, (x_, y_) in enumerate(redis_peers())]

    relay_y = apart * y + (1 - apart) * (1 - y)

    def relay_copy(i, f):
        c = core if i == 0 else 1 - core
        to = dev(x, 1 - y, z, core) if f == 0 else dev(1 - x, y, z, core)
        return act_copy(6 + i, 2 * relay_y + c, f, to)

    def relay(i):
        for f in (0, 1):
            @pl.when(apart == 1 - f)
            def _():
                act_wait(2 * relay_y + (core if i == 0 else 1 - core), f)
                relay_copy(i, f).start()

    def acts_wait():
        for h_ in range(heads):
            for f in (0, 1):
                mine = (apart == 0) & (h == h_)
                relayed = (apart == 1 - f) & (relay_y == h_ // 2)

                @pl.when(jnp.logical_not(mine | relayed))
                def _():
                    act_wait(h_, f)

    @pl.when(apart == 1)
    def _():
        own_wait(0)
        own_start(0)

    pos = block_id * block + lax.broadcasted_iota(jnp.int32, (block, 1), 0)
    start = jnp.zeros((block, 1), jnp.int32)
    end = jnp.int32(0)
    for i in range(len_ref.shape[0]):
        size = len_ref[i]
        end = end + size
        start = start + jnp.where(pos >= end, size, 0)
    angle = (pos - start).astype(f32) * freq_ref[...]
    lane = lax.broadcasted_iota(jnp.int32, (block, HEAD_SIZE), 1)
    rope[0] = jnp.cos(angle)
    rope[1] = jnp.where(lane < HEAD_SIZE // 2, -jnp.sin(angle), jnp.sin(angle))
    qkv[...] = jnp.zeros_like(qkv)

    own_wait(1)
    own_start(1)
    line_steps(0, 1, 2)
    relay(0)
    line_steps(0, 2, steps)
    relay(1)
    for copy in redis_copies:
        copy.start()
    last_in = first_out - 1

    @pl.when(inner)
    def _():
        for u in range(2, first_out):
            line_steps(u - 1, 1, steps)
            own_wait(u)
            own_start(u)
        line_steps(last_in, 1, 2)

    @pl.when(jnp.logical_not(inner))
    def _():
        for u in range(2, first_out):
            own_wait(u)
            own_start(u)

    for d in range(1, reach + 1):
        @pl.when(block_id < d)
        def _():
            kv[d] = jnp.zeros_like(kv[d])

    acts_wait()

    depth = min(1024, width)

    def project(weights, cols):
        def one(k, _):
            rows = pl.ds(pl.multiple_of(k * depth, depth), depth)
            left = acts[:, :, rows].reshape(block, depth)
            qkv[:, cols] += jnp.dot(left, weights[rows, :], preferred_element_type=f32)
            return 0

        lax.fori_loop(0, width // depth, one, 0)

    def rotated(first):
        v = qkv[:, first:first + HEAD_SIZE]
        return (v * rope[0] + pltpu.roll(v, HEAD_SIZE // 2, 1) * rope[1]).astype(bf16)

    def project_query(u):
        mate_wait(u)
        first = (u - 1) * unit_cols
        project(w_q.at[u - 1], slice(first, first + unit_cols))
        for j in range(first // HEAD_SIZE, (first + unit_cols) // HEAD_SIZE):
            query[:, j * HEAD_SIZE:(j + 1) * HEAD_SIZE] = rotated(j * HEAD_SIZE)

    def kv_copy(k):
        return remote(
            kv.at[0], kv.at[2 * k], kv_send.at[2 * k], kv_recv.at[2 * k], dev(x, y, z + k, core)
        )

    kv_mate = remote(kv.at[0], kv.at[1], kv_send.at[1], kv_recv.at[1], mate)

    def kv_pass_copy(k):
        to = 2 * k + 1 - 2 * core
        return remote(kv.at[2 * k], kv.at[to], kv_pass_send.at[2 * k], kv_recv.at[to], mate)

    def kv_passes(k):
        return (z >= k) & (2 * k + 1 - 2 * core <= reach)

    def kv_each(low, high_, body):
        def one(k, _):
            body(k)
            return 0

        lax.fori_loop(low, high_, one, 0)

    def kv_start():
        @pl.when(core == 0)
        def _():
            kv_mate.start()

        def one(k):
            @pl.when(z + k < steps)
            def _():
                kv_copy(k).start()

        kv_each(1, reach // 2 + 1, one)

    def kv_wait(d):
        remote(kv.at[d], kv.at[d], kv_send.at[d], kv_recv.at[d], mate).wait_recv()

    def kv_ready():
        def even(k):
            @pl.when(z >= k)
            def _():
                kv_wait(2 * k)

            @pl.when(kv_passes(k))
            def _():
                kv_pass_copy(k).start()

        def odd(k):
            @pl.when(block_id >= 2 * k + 1)
            def _():
                kv_wait(2 * k + 1)

        kv_each(1, reach // 2 + 1, even)
        kv_each(0, reach // 2, odd)

    own_pos = lax.broadcasted_iota(jnp.int32, (block, 1), 0)
    own_start_pos = start - block_id * block
    key_lane = lax.broadcasted_iota(jnp.int32, (1, block), 1)
    scale = HEAD_SIZE ** (-0.5) * float(np.log2(np.e))

    def attend_own(u):
        def one(j, _):
            cols = pl.ds(pl.multiple_of(j * HEAD_SIZE, HEAD_SIZE), HEAD_SIZE)
            keep = (key_lane >= own_start_pos) & (key_lane <= own_pos)
            scores = lax.dot_general(
                query[:, cols], kv[0, :, :HEAD_SIZE], (((1,), (1,)), ((), ())),
                preferred_element_type=f32,
            )
            scores = jnp.where(keep, scores, masked_score)
            new = jnp.max(scores, axis=1, keepdims=True)
            probs = jnp.exp2((scores - new) * scale)
            high[j] = new
            total[j] = jnp.sum(probs, axis=1, keepdims=True)
            accum[:, cols] = jnp.dot(probs.astype(bf16), kv[0, :, HEAD_SIZE:], preferred_element_type=f32)
            return 0

        lax.fori_loop((u - 1) * unit_heads, u * unit_heads, one, 0)

    def attend_earlier(u, d):
        keep = key_lane - d * block >= own_start_pos

        def one(j, _):
            cols = pl.ds(pl.multiple_of(j * HEAD_SIZE, HEAD_SIZE), HEAD_SIZE)
            scores = lax.dot_general(
                query[:, cols], kv[d, :, :HEAD_SIZE], (((1,), (1,)), ((), ())),
                preferred_element_type=f32,
            )
            scores = jnp.where(keep, scores, masked_score)
            old = high[j]
            new = jnp.maximum(old, jnp.max(scores, axis=1, keepdims=True))
            fading = jnp.exp2((old - new) * scale)
            probs = jnp.exp2((scores - new) * scale)
            total[j] = total[j] * fading + jnp.sum(probs, axis=1, keepdims=True)
            update = jnp.dot(probs.astype(bf16), kv[d, :, HEAD_SIZE:], preferred_element_type=f32)
            accum[:, cols] = accum[:, cols] * fading + update
            high[j] = new
            return 0

        lax.fori_loop((u - 1) * unit_heads, u * unit_heads, one, 0)

    def attend_tiles(u):
        tile = block // 4

        def one(j, _):
            cols = pl.ds(pl.multiple_of(j * HEAD_SIZE, HEAD_SIZE), HEAD_SIZE)
            for i in range(4):
                rows = slice(i * tile, (i + 1) * tile)
                spans = [(0, 0, (i + 1) * tile)]
                spans += [(d, 0, block) for d in range(1, reach)]
                spans += [(reach, i * tile, block)]
                parts = []
                for d, low, high_ in spans:
                    scores = lax.dot_general(
                        query[rows, cols], kv[d, low:high_, :HEAD_SIZE], (((1,), (1,)), ((), ())),
                        preferred_element_type=f32,
                    )
                    key_pos = low - d * block + lax.broadcasted_iota(jnp.int32, (1, high_ - low), 1)
                    keep = key_pos >= own_start_pos[rows]
                    if d == 0:
                        keep = keep & (key_pos <= own_pos[rows])
                    parts.append(jnp.where(keep, scores, masked_score))
                top = functools.reduce(jnp.maximum, [jnp.max(p, axis=1, keepdims=True) for p in parts])
                probs = [jnp.exp2((p - top) * scale) for p in parts]
                denom = sum(jnp.sum(p, axis=1, keepdims=True) for p in probs)
                result = sum(
                    jnp.dot(p.astype(bf16), kv[d, low:high_, HEAD_SIZE:], preferred_element_type=f32)
                    for p, (d, low, high_) in zip(probs, spans)
                )
                mixed[group, rows, cols] = (result / denom).astype(bf16)
            return 0

        lax.fori_loop((u - 1) * unit_heads, u * unit_heads, one, 0)

    def mix_cols(u):
        return pl.ds((u - 1) * unit_cols, unit_cols)

    def mix_copy(u, i, x_, y_):
        ref = mixed.at[group, :, mix_cols(u)]
        return remote(ref, ref, mix_send.at[u - 1, i], mix_recv.at[u - 1, group], dev(x_, y_, z, core))

    def attend(u):
        if reach <= 2:
            attend_tiles(u)
        else:
            attend_own(u)
            finish_heads(u)
        for i, (x_, y_) in enumerate(redis_peers()):
            mix_copy(u, i, x_, y_).start()

    def finish_heads(u):
        def one(d, _):
            @pl.when(block_id >= d)
            def _():
                attend_earlier(u, d)
            return 0

        lax.fori_loop(1, reach + 1, one, 0)
        for j in range((u - 1) * unit_heads, u * unit_heads):
            cols = slice(j * HEAD_SIZE, (j + 1) * HEAD_SIZE)
            mixed[group, :, cols] = (accum[:, cols] / total[j]).astype(bf16)

    def mix_wait():
        for u in range(1, first_out):
            for x_, y_ in redis_peers():
                ref = mixed.at[2 * y_ + x_, :, mix_cols(u)]
                remote(ref, ref, mix_send.at[0, 0], mix_recv.at[u - 1, 2 * y_ + x_], mate).wait_recv()

    mate_wait(0)
    project(w_kv, slice(q_cols, q_cols + w_kv.shape[1]))
    kv[0, :, :HEAD_SIZE] = rotated(q_cols)
    kv[0, :, HEAD_SIZE:] = qkv[:, q_cols + HEAD_SIZE:].astype(bf16)
    kv_start()
    for u in range(1, last_in):
        outer_steps(u, 1, steps)
    inner_steps(last_in, 2, steps)
    for u in range(1, last_in):
        project_query(u)
    own_wait(first_out)
    for u in range(first_out, units):
        own_start(u)

    def inner_out(low, high_):
        @pl.when(inner)
        def _():
            def one(s, _):
                for u in range(first_out, units):
                    line_step(u, s)
                return 0

            lax.fori_loop(low, high_, one, 0)

    @pl.when(inner)
    def _():
        project_query(last_in)

    kv_ready()
    for u in range(1, last_in):
        attend(u)
    outer_steps(last_in, 1, steps)

    @pl.when(jnp.logical_not(inner))
    def _():
        project_query(last_in)

    inner_out(1, 2)
    attend(last_in)
    inner_out(2, steps)

    def out_at(g, c):
        return pl.ds(pl.multiple_of(g * col_width + out_first[c], HEAD_SIZE), out_cols[c])

    def out_part(r, c):
        return osend.at[r, :, pl.ds(out_first[c], out_cols[c])]

    def out_copy(c, r):
        return remote(
            out_part(r, c), obuf.at[:, out_at(group, c)], out_send.at[c, r], out_recv.at[c, group],
            dev(core, r // 2, z, r % 2),
        )

    def away(r):
        return (apart == 1) | (h != r)

    def project_out(c):
        cols = slice(out_first[c], out_first[c] + out_cols[c])
        result = None
        for g in range(heads):
            right = w_proj[g // 2, g % 2, :, :, cols]
            if right.shape[1] % 16:
                right = right.astype(f32).reshape(-1, out_cols[c]).astype(bf16)
            else:
                right = right.reshape(-1, out_cols[c])
            term = jnp.dot(mixed[g], right, preferred_element_type=f32)
            result = term if result is None else result + term
        osend[:, :, cols] = result.astype(bf16).reshape(heads, own, out_cols[c])
        for r in range(heads):
            @pl.when(away(r))
            def _():
                out_copy(c, r).start()

        @pl.when(apart == 0)
        def _():
            obuf[:, out_at(group, c)] = osend[h, :, cols]

    for c in range(chunks):
        outer_steps(first_out + c, 1, steps)
        mate_wait(first_out + c)
        if c == 0:
            mix_wait()
        project_out(c)

    for c in range(chunks):
        for g in range(heads):
            @pl.when((apart == 1) | (group != g))
            def _():
                ref = obuf.at[:, out_at(g, c)]
                remote(ref, ref, out_send.at[0, 0], out_recv.at[c, g], mate).wait_recv()
    out_ref[...] = obuf[...]

    for u in range(units):
        def one(row, _):
            @pl.when((row <= z) & (z < steps - 1))
            def _():
                line_copy(u, UP, row).wait_send()

            @pl.when((row >= z) & (z > 0))
            def _():
                line_copy(u, DOWN, row).wait_send()

            mate_copy(u, row).wait_send()
            return 0

        lax.fori_loop(0, steps, one, 0)

    @pl.when(apart == 1)
    def _():
        for u in range(first_out):
            cross_copy(u).wait_send()
        for copy in act_mate:
            copy.wait_send()

    for copy in act_copies + redis_copies:
        copy.wait_send()
    for f in (0, 1):
        @pl.when(apart == 1 - f)
        def _():
            for i in (0, 1):
                relay_copy(i, f).wait_send()

    @pl.when(core == 0)
    def _():
        kv_mate.wait_send()

    def kv_drain(k):
        @pl.when(z + k < steps)
        def _():
            kv_copy(k).wait_send()

        @pl.when(kv_passes(k))
        def _():
            kv_pass_copy(k).wait_send()

    kv_each(1, reach // 2 + 1, kv_drain)
    for u in range(1, first_out):
        for i, (x_, y_) in enumerate(redis_peers()):
            mix_copy(u, i, x_, y_).wait_send()
    for c in range(chunks):
        for r in range(heads):
            @pl.when(away(r))
            def _():
                out_copy(c, r).wait_send()


def on_device(tokens, w_query, key_value_weight, w_out, doc_lengths):
    n = lax.axis_size("blk")
    heads = lax.axis_size("heads")
    assert heads == 4
    q_units, chunks = Q_UNITS, len(OUT_PARTS)
    steps = n // LINE
    own, width = tokens.shape
    block = own * heads
    rows_in, q_cols = w_query.shape
    kv_cols = 2 * key_value_weight.shape[2]
    rows_out = w_out.shape[0]
    col_width = width // heads
    out_cols = tuple(col_width * part // sum(OUT_PARTS) for part in OUT_PARTS)
    q_heads = q_cols // HEAD_SIZE
    reach = n // 4
    units = 1 + q_units + chunks
    half = HEAD_SIZE // 2
    freqs = np.power(rope_base, -2.0 * np.arange(half) / HEAD_SIZE).astype(np.float32)
    freqs = jnp.asarray(np.concatenate([freqs, freqs])[None, :])
    bf16, f32 = jnp.bfloat16, jnp.float32
    dma = pltpu.SemaphoreType.DMA
    return pl.pallas_call(
        functools.partial(layer_kernel, n, heads, out_cols, q_units),
        out_shape=jax.ShapeDtypeStruct((own, width), bf16),
        in_specs=[
            pl.BlockSpec(memory_space=pltpu.VMEM),
            pl.BlockSpec(memory_space=pl.ANY),
            pl.BlockSpec(memory_space=pltpu.VMEM),
            pl.BlockSpec(memory_space=pl.ANY),
            pl.BlockSpec(memory_space=pltpu.SMEM),
            pl.BlockSpec(memory_space=pltpu.VMEM),
        ],
        out_specs=pl.BlockSpec(memory_space=pltpu.VMEM),
        scratch_shapes=[
            pltpu.VMEM((n * rows_in, kv_cols), bf16),
            pltpu.VMEM((q_units, n * rows_in, q_cols // q_units), bf16),
            pltpu.VMEM((2, 2, n, rows_out, col_width), bf16),
            pltpu.VMEM((rows_in, kv_cols), bf16),
            pltpu.VMEM((own, width), bf16),
            pltpu.VMEM((heads, own, width), bf16),
            pltpu.VMEM((block, q_cols + kv_cols), f32),
            pltpu.VMEM((block, q_cols), bf16),
            pltpu.VMEM((reach + 1, block, kv_cols), bf16),
            pltpu.VMEM((q_heads, block, 1), f32),
            pltpu.VMEM((q_heads, block, 1), f32),
            pltpu.VMEM((block, q_cols), f32),
            pltpu.VMEM((heads, block, q_cols), bf16),
            pltpu.VMEM((2, block, HEAD_SIZE), f32),
            pltpu.VMEM((heads, own, col_width), bf16),
            pltpu.VMEM((own, width), bf16),
            dma((units, 2, steps)),
            dma((units, steps)),
            dma((units, 2, steps)),
            dma((1 + q_units,)),
            dma((1 + q_units,)),
            dma((3,)),
            dma((heads,)),
            dma((8,)),
            dma((2, heads)),
            dma((reach + 1,)),
            dma((reach + 1,)),
            dma((reach + 1,)),
            dma((q_units, 3)),
            dma((q_units, heads)),
            dma((chunks, heads)),
            dma((chunks, heads)),
        ],
        compiler_params=pltpu.CompilerParams(
            collective_id=0, has_side_effects=True, vmem_limit_bytes=60 * 1024 * 1024
        ),
    )(tokens, w_query, key_value_weight, w_out, doc_lengths, freqs)


def solution(mesh):
    return jax.shard_map(
        on_device,
        mesh=mesh,
        in_specs=(
            P(("blk", "heads"), None),
            P("blk", "heads"),
            P("blk", None, "heads"),
            P(("heads", "blk"), None),
            P(),
        ),
        out_specs=P(("blk", "heads"), None),
        check_vma=False,
    )
```

```python
import functools

import jax
import jax.numpy as jnp
import numpy as np
from jax import lax
from jax.experimental import pallas as pl
from jax.experimental.pallas import tpu as pltpu
from jax.sharding import PartitionSpec as P

HEAD_SIZE = 128
LINE = 2
Q_UNITS = 2
OUT_PARTS = (4, 2, 2)
LEFT_PARTS = (5, 8)

norm_epsilon = 1e-05
rope_base = 500000.0
masked_score = -1e30
MESH = pl.DeviceIdType.MESH
UP, DOWN = 0, 1


def layer_kernel(
    n, heads, out_cols, q_units,
    tok_ref, w_query_ref, w_keyval_ref, w_out_ref, len_ref, freq_ref, out_ref,
    tok_buf, kv_raw, freq_buf, w_kv, w_q, w_proj, kv_stage, act_stage, acts, qkv, query, kv, high, total, accum, mixed, rope, osend, obuf,
    line_send, mate_send, recv, cross_send, local_sem, load_sem, store_sem, redis_send, redis_recv,
    act_send, act_recv, kv_send, kv_recv, kv_pass_send, mix_send, mix_recv, out_send, out_recv,
):
    f32, bf16 = jnp.float32, jnp.bfloat16
    b = lax.axis_index("blk")
    h = lax.axis_index("heads")
    steps = n // LINE
    z, x = b // LINE, b % LINE
    y, core = h // 2, h % 2
    group = 2 * y + x
    block_id = LINE * z + core
    apart = (x + core) % 2
    reach = n // 4
    own, width = tok_ref.shape
    rows_in = w_query_ref.shape[0]
    block = own * heads
    q_cols = query.shape[1]
    q_heads = q_cols // HEAD_SIZE
    unit_cols = q_cols // q_units
    unit_heads = q_heads // q_units
    col_width = width // heads
    chunks = len(out_cols)
    out_first = [sum(out_cols[:c]) for c in range(chunks)]
    left = width * LEFT_PARTS[0] // LEFT_PARTS[1]
    first_out = 1 + q_units
    units = first_out + chunks

    def dev(x_, y_, z_, c_):
        return {"blk": LINE * z_ + x_, "heads": 2 * y_ + c_}

    mate = dev(x, y, z, 1 - core)

    def remote(src, dst, ss, rs, device):
        return pltpu.make_async_remote_copy(
            src_ref=src, dst_ref=dst, send_sem=ss, recv_sem=rs, device_id=device, device_id_type=MESH
        )

    barrier = pltpu.get_barrier_semaphore()
    for dx, dy, dc in [(i, j, k) for i in (0, 1) for j in (0, 1) for k in (0, 1) if i + j + k]:
        pl.semaphore_signal(
            barrier, inc=1, device_id=dev((x + dx) % 2, (y + dy) % 2, z, (core + dc) % 2), device_id_type=MESH
        )
    span = (reach + 1) // 2
    for d in range(1, span + 1):
        for c_ in (0, 1):
            @pl.when(z + d < steps)
            def _():
                pl.semaphore_signal(barrier, inc=1, device_id=dev(x, y, z + d, c_), device_id_type=MESH)

            @pl.when(z - d >= 0)
            def _():
                pl.semaphore_signal(barrier, inc=1, device_id=dev(x, y, z - d, c_), device_id_type=MESH)
    near = jnp.minimum(z, span) + jnp.minimum(steps - 1 - z, span)
    loads = [
        pltpu.make_async_copy(src, dst, load_sem.at[i])
        for i, (src, dst) in enumerate([(w_keyval_ref, kv_raw), (tok_ref, tok_buf), (freq_ref, freq_buf)])
    ]
    for load in loads:
        load.start()

    def unit_ref(u, k, row):
        i = LINE * row + k
        if u == 0:
            return w_kv.at[pl.ds(pl.multiple_of(i * rows_in, rows_in), rows_in)]
        if u < first_out:
            return w_q.at[u - 1, pl.ds(pl.multiple_of(i * rows_in, rows_in), rows_in)]
        return w_proj.at[:, k, pl.ds(LINE * row, LINE), :, pl.ds(out_first[u - first_out], out_cols[u - first_out])]

    def line_copy(u, direction, row):
        ref = unit_ref(u, core, row)
        z_ = z + 1 if direction == UP else z - 1
        at = row
        if direction == DOWN:
            at = jnp.where(row == z, steps, row)
        return remote(ref, ref, line_send.at[u, at], recv.at[u, core, row], dev(x, y, z_, core))

    def mate_copy(u, row):
        ref = unit_ref(u, core, row)
        return remote(ref, ref, mate_send.at[u, row], recv.at[u, core, row], mate)

    def arrive(u, k, row):
        ref = unit_ref(u, k, row)
        remote(ref, ref, mate_send.at[u, 0], recv.at[u, k, row], mate).wait_recv()

    def query_cols(u):
        return w_query_ref.at[:, pl.ds((u - 1) * unit_cols, unit_cols)]

    def cross_copy(u):
        src = kv_stage if u == 0 else query_cols(u)
        return remote(src, unit_ref(u, x, z), cross_send.at[u], recv.at[u, x, z], dev(1 - x, y, z, 1 - core))

    def keep_query(u):
        return pltpu.make_async_copy(query_cols(u), unit_ref(u, core, z), local_sem.at[u])

    def own_start(u):
        @pl.when(z < steps - 1)
        def _():
            line_copy(u, UP, z).start()

        @pl.when(z > 0)
        def _():
            line_copy(u, DOWN, z).start()

        mate_copy(u, z).start()

    def redis_peers():
        return [(1 - x, y), (x, 1 - y), (1 - x, 1 - y)]

    def redis_copy(i, x_, y_):
        cols = pl.ds(pl.multiple_of((2 * y_ + x_) * col_width, col_width), col_width)
        return remote(
            w_out_ref.at[:, cols], w_proj.at[y, core, b], redis_send.at[i], redis_recv.at[group],
            dev(x_, y_, z, core),
        )

    def keep_out():
        cols = pl.ds(pl.multiple_of(group * col_width, col_width), col_width)
        return pltpu.make_async_copy(w_out_ref.at[:, cols], w_proj.at[y, core, b], local_sem.at[0])

    def own_wait(u):
        if u == 0:
            @pl.when(apart == 1)
            def _():
                arrive(u, core, z)
        elif u < first_out:
            @pl.when(apart == 1)
            def _():
                arrive(u, core, z)

            @pl.when(apart == 0)
            def _():
                keep_query(u).wait()
        elif u == first_out:
            keep_out().wait()
            for x_, y_ in redis_peers():
                ref = w_proj.at[y_, core, LINE * z + x_]
                remote(ref, ref, redis_send.at[0], redis_recv.at[2 * y_ + x_], mate).wait_recv()

    def line_step(u, s):
        @pl.when(z - s >= 0)
        def _():
            arrive(u, core, z - s)

            @pl.when(z < steps - 1)
            def _():
                line_copy(u, UP, z - s).start()

            mate_copy(u, z - s).start()

        @pl.when(z + s <= steps - 1)
        def _():
            arrive(u, core, z + s)

            @pl.when(z > 0)
            def _():
                line_copy(u, DOWN, z + s).start()

            mate_copy(u, z + s).start()

    def line_steps(u, low, high_):
        def one(s, _):
            line_step(u, s)
            return 0

        lax.fori_loop(low, high_, one, 0)

    inner = (z > 0) & (z < steps - 1)

    def inner_steps(u, low, high_):
        @pl.when(inner)
        def _():
            line_steps(u, low, high_)

    def outer_steps(u, low, high_):
        @pl.when(jnp.logical_not(inner))
        def _():
            line_steps(u, low, high_)

    def mate_wait(u):
        def one(row, _):
            arrive(u, 1 - core, row)
            return 0

        lax.fori_loop(0, steps, one, 0)

    @pl.when(apart == 0)
    def _():
        for u in range(1, first_out):
            keep_query(u).start()

    keep_out().start()
    loads[0].wait()
    own_kv = kv_raw[...].reshape(rows_in, w_kv.shape[1])

    @pl.when(apart == 0)
    def _():
        w_kv[pl.ds(pl.multiple_of(b * rows_in, rows_in), rows_in), :] = own_kv

    @pl.when(apart == 1)
    def _():
        kv_stage[...] = own_kv

    loads[1].wait()
    values = tok_buf[...].astype(f32)
    normed = (
        values * lax.rsqrt(jnp.mean(values * values, axis=1, keepdims=True) + norm_epsilon)
    ).astype(bf16)
    act_stage[...] = normed

    @pl.when(apart == 0)
    def _():
        acts[h] = normed

    pl.semaphore_wait(barrier, 7 + 2 * near)

    @pl.when(apart == 0)
    def _():
        own_start(0)
        own_wait(1)
        own_start(1)

    @pl.when(apart == 1)
    def _():
        for u in range(2):
            cross_copy(u).start()

    act_cols = [(0, left), (left, width - left)]

    def act_ref(h_, f):
        return acts.at[h_, :, pl.ds(*act_cols[f])]

    def act_copy(i, h_, f, device, src=None):
        src = act_ref(h_, f) if src is None else src
        return remote(src, act_ref(h_, f), act_send.at[i], act_recv.at[f, h_], device)

    def act_own(i, f, device):
        return act_copy(i, h, f, device, act_stage.at[:, pl.ds(*act_cols[f])])

    def act_wait(h_, f):
        remote(act_ref(h_, f), act_ref(h_, f), act_send.at[0], act_recv.at[f, h_], mate).wait_recv()

    act_copies = [
        act_own(0, 1, dev(x, 1 - y, z, x)),
        act_own(1, 0, dev(1 - x, y, z, x)),
        act_own(2, 0, dev(x, 1 - y, z, x)),
        act_own(3, 1, dev(1 - x, y, z, x)),
    ]
    act_mate = [act_own(4 + f, f, mate) for f in (0, 1)]
    act_copies[0].start()
    act_copies[2].start()

    @pl.when(apart == 1)
    def _():
        act_copies[1].start()
        for u in range(2, first_out):
            cross_copy(u).start()
        for copy in act_mate:
            copy.start()
        act_copies[3].start()

    redis_copies = [redis_copy(i, x_, y_) for i, (x_, y_) in enumerate(redis_peers())]

    relay_y = apart * y + (1 - apart) * (1 - y)

    def relay_copy(i, f):
        c = core if i == 0 else 1 - core
        to = dev(x, 1 - y, z, core) if f == 0 else dev(1 - x, y, z, core)
        return act_copy(6 + i, 2 * relay_y + c, f, to)

    def relay(i):
        for f in (0, 1):
            @pl.when(apart == 1 - f)
            def _():
                act_wait(2 * relay_y + (core if i == 0 else 1 - core), f)
                relay_copy(i, f).start()

    def acts_wait():
        for h_ in range(heads):
            for f in (0, 1):
                mine = (apart == 0) & (h == h_)
                relayed = (apart == 1 - f) & (relay_y == h_ // 2)

                @pl.when(jnp.logical_not(mine | relayed))
                def _():
                    act_wait(h_, f)

    @pl.when(apart == 1)
    def _():
        own_wait(0)
        own_start(0)

    pos = block_id * block + lax.broadcasted_iota(jnp.int32, (block, 1), 0)
    start = jnp.zeros((block, 1), jnp.int32)
    end = jnp.int32(0)
    for i in range(len_ref.shape[0]):
        size = len_ref[i]
        end = end + size
        start = start + jnp.where(pos >= end, size, 0)
    loads[2].wait()
    angle = (pos - start).astype(f32) * freq_buf[...]
    lane = lax.broadcasted_iota(jnp.int32, (block, HEAD_SIZE), 1)
    rope[0] = jnp.cos(angle)
    rope[1] = jnp.where(lane < HEAD_SIZE // 2, -jnp.sin(angle), jnp.sin(angle))
    qkv[...] = jnp.zeros_like(qkv)

    @pl.when(apart == 1)
    def _():
        own_wait(1)
        own_start(1)

    line_steps(0, 1, 2)

    @pl.when(apart == 0)
    def _():
        act_copies[1].start()
        act_copies[3].start()

    relay(0)
    line_steps(0, 2, steps)
    relay(1)
    for copy in redis_copies:
        copy.start()
    last_in = first_out - 1

    @pl.when(inner)
    def _():
        for u in range(2, first_out):
            line_steps(u - 1, 1, steps)
            own_wait(u)
            own_start(u)
        line_steps(last_in, 1, 2)

    @pl.when(jnp.logical_not(inner))
    def _():
        for u in range(2, first_out):
            own_wait(u)
            own_start(u)

    for d in range(1, reach + 1):
        @pl.when(block_id < d)
        def _():
            kv[d] = jnp.zeros_like(kv[d])

    acts_wait()

    depth = min(1024, width)

    def project(weights, cols):
        def one(k, _):
            rows = pl.ds(pl.multiple_of(k * depth, depth), depth)
            left = acts[:, :, rows].reshape(block, depth)
            qkv[:, cols] += jnp.dot(left, weights[rows, :], preferred_element_type=f32)
            return 0

        lax.fori_loop(0, width // depth, one, 0)

    def rotated(first):
        v = qkv[:, first:first + HEAD_SIZE]
        return (v * rope[0] + pltpu.roll(v, HEAD_SIZE // 2, 1) * rope[1]).astype(bf16)

    def project_query(u):
        mate_wait(u)
        first = (u - 1) * unit_cols
        project(w_q.at[u - 1], slice(first, first + unit_cols))
        for j in range(first // HEAD_SIZE, (first + unit_cols) // HEAD_SIZE):
            query[:, j * HEAD_SIZE:(j + 1) * HEAD_SIZE] = rotated(j * HEAD_SIZE)

    def kv_copy(k):
        return remote(
            kv.at[0], kv.at[2 * k], kv_send.at[2 * k], kv_recv.at[2 * k], dev(x, y, z + k, core)
        )

    kv_mate = remote(kv.at[0], kv.at[1], kv_send.at[1], kv_recv.at[1], mate)

    def kv_pass_copy(k):
        to = 2 * k + 1 - 2 * core
        return remote(kv.at[2 * k], kv.at[to], kv_pass_send.at[2 * k], kv_recv.at[to], mate)

    def kv_passes(k):
        return (z >= k) & (2 * k + 1 - 2 * core <= reach)

    def kv_each(low, high_, body):
        def one(k, _):
            body(k)
            return 0

        lax.fori_loop(low, high_, one, 0)

    def kv_start():
        @pl.when(core == 0)
        def _():
            kv_mate.start()

        def one(k):
            @pl.when(z + k < steps)
            def _():
                kv_copy(k).start()

        kv_each(1, reach // 2 + 1, one)

    def kv_wait(d):
        remote(kv.at[d], kv.at[d], kv_send.at[d], kv_recv.at[d], mate).wait_recv()

    def kv_ready():
        def even(k):
            @pl.when(z >= k)
            def _():
                kv_wait(2 * k)

            @pl.when(kv_passes(k))
            def _():
                kv_pass_copy(k).start()

        def odd(k):
            @pl.when(block_id >= 2 * k + 1)
            def _():
                kv_wait(2 * k + 1)

        kv_each(1, reach // 2 + 1, even)
        kv_each(0, reach // 2, odd)

    own_pos = lax.broadcasted_iota(jnp.int32, (block, 1), 0)
    own_start_pos = start - block_id * block
    key_lane = lax.broadcasted_iota(jnp.int32, (1, block), 1)
    scale = HEAD_SIZE ** (-0.5) * float(np.log2(np.e))

    def attend_own(u):
        def one(j, _):
            cols = pl.ds(pl.multiple_of(j * HEAD_SIZE, HEAD_SIZE), HEAD_SIZE)
            keep = (key_lane >= own_start_pos) & (key_lane <= own_pos)
            scores = lax.dot_general(
                query[:, cols], kv[0, :, :HEAD_SIZE], (((1,), (1,)), ((), ())),
                preferred_element_type=f32,
            )
            scores = jnp.where(keep, scores, masked_score)
            new = jnp.max(scores, axis=1, keepdims=True)
            probs = jnp.exp2((scores - new) * scale)
            high[j] = new
            total[j] = jnp.sum(probs, axis=1, keepdims=True)
            accum[:, cols] = jnp.dot(probs.astype(bf16), kv[0, :, HEAD_SIZE:], preferred_element_type=f32)
            return 0

        lax.fori_loop((u - 1) * unit_heads, u * unit_heads, one, 0)

    def attend_earlier(u, d):
        keep = key_lane - d * block >= own_start_pos

        def one(j, _):
            cols = pl.ds(pl.multiple_of(j * HEAD_SIZE, HEAD_SIZE), HEAD_SIZE)
            scores = lax.dot_general(
                query[:, cols], kv[d, :, :HEAD_SIZE], (((1,), (1,)), ((), ())),
                preferred_element_type=f32,
            )
            scores = jnp.where(keep, scores, masked_score)
            old = high[j]
            new = jnp.maximum(old, jnp.max(scores, axis=1, keepdims=True))
            fading = jnp.exp2((old - new) * scale)
            probs = jnp.exp2((scores - new) * scale)
            total[j] = total[j] * fading + jnp.sum(probs, axis=1, keepdims=True)
            update = jnp.dot(probs.astype(bf16), kv[d, :, HEAD_SIZE:], preferred_element_type=f32)
            accum[:, cols] = accum[:, cols] * fading + update
            high[j] = new
            return 0

        lax.fori_loop((u - 1) * unit_heads, u * unit_heads, one, 0)

    def attend_tiles(u):
        tile = block // 4

        def one(j, _):
            cols = pl.ds(pl.multiple_of(j * HEAD_SIZE, HEAD_SIZE), HEAD_SIZE)
            for i in range(4):
                rows = slice(i * tile, (i + 1) * tile)
                spans = [(0, 0, (i + 1) * tile)]
                spans += [(d, 0, block) for d in range(1, reach)]
                spans += [(reach, i * tile, block)]
                parts = []
                for d, low, high_ in spans:
                    scores = lax.dot_general(
                        query[rows, cols], kv[d, low:high_, :HEAD_SIZE], (((1,), (1,)), ((), ())),
                        preferred_element_type=f32,
                    )
                    key_pos = low - d * block + lax.broadcasted_iota(jnp.int32, (1, high_ - low), 1)
                    keep = key_pos >= own_start_pos[rows]
                    if d == 0:
                        keep = keep & (key_pos <= own_pos[rows])
                    parts.append(jnp.where(keep, scores, masked_score))
                top = functools.reduce(jnp.maximum, [jnp.max(p, axis=1, keepdims=True) for p in parts])
                probs = [jnp.exp2((p - top) * scale) for p in parts]
                denom = sum(jnp.sum(p, axis=1, keepdims=True) for p in probs)
                result = sum(
                    jnp.dot(p.astype(bf16), kv[d, low:high_, HEAD_SIZE:], preferred_element_type=f32)
                    for p, (d, low, high_) in zip(probs, spans)
                )
                mixed[group, rows, cols] = (result / denom).astype(bf16)
            return 0

        lax.fori_loop((u - 1) * unit_heads, u * unit_heads, one, 0)

    def mix_cols(u):
        return pl.ds((u - 1) * unit_cols, unit_cols)

    def mix_copy(u, i, x_, y_):
        ref = mixed.at[group, :, mix_cols(u)]
        return remote(ref, ref, mix_send.at[u - 1, i], mix_recv.at[u - 1, group], dev(x_, y_, z, core))

    def attend(u):
        if reach <= 2:
            attend_tiles(u)
        else:
            attend_own(u)
            finish_heads(u)
        for i, (x_, y_) in enumerate(redis_peers()):
            mix_copy(u, i, x_, y_).start()

    def finish_heads(u):
        def one(d, _):
            @pl.when(block_id >= d)
            def _():
                attend_earlier(u, d)
            return 0

        lax.fori_loop(1, reach + 1, one, 0)
        for j in range((u - 1) * unit_heads, u * unit_heads):
            cols = slice(j * HEAD_SIZE, (j + 1) * HEAD_SIZE)
            mixed[group, :, cols] = (accum[:, cols] / total[j]).astype(bf16)

    def mix_wait():
        for u in range(1, first_out):
            for x_, y_ in redis_peers():
                ref = mixed.at[2 * y_ + x_, :, mix_cols(u)]
                remote(ref, ref, mix_send.at[0, 0], mix_recv.at[u - 1, 2 * y_ + x_], mate).wait_recv()

    mate_wait(0)
    project(w_kv, slice(q_cols, q_cols + w_kv.shape[1]))
    kv[0, :, :HEAD_SIZE] = rotated(q_cols)
    kv[0, :, HEAD_SIZE:] = qkv[:, q_cols + HEAD_SIZE:].astype(bf16)
    kv_start()
    for u in range(1, last_in):
        outer_steps(u, 1, steps)
    inner_steps(last_in, 2, steps)
    for u in range(1, last_in):
        project_query(u)
    own_wait(first_out)
    own_start(first_out)

    @pl.when(jnp.logical_not(inner))
    def _():
        for u in range(first_out + 1, units):
            own_start(u)

    @pl.when(inner)
    def _():
        project_query(last_in)

    kv_ready()
    for u in range(1, last_in):
        attend(u)
    outer_steps(last_in, 1, steps)

    @pl.when(jnp.logical_not(inner))
    def _():
        project_query(last_in)

    @pl.when(inner)
    def _():
        line_step(first_out, 1)
        for u in range(first_out + 1, units):
            own_start(u)

    attend(last_in)

    @pl.when(inner)
    def _():
        def one(s, _):
            line_step(first_out, s)
            for u in range(first_out + 1, units):
                line_step(u, s - 1)
            return 0

        lax.fori_loop(2, steps, one, 0)
        for u in range(first_out + 1, units):
            line_step(u, steps - 1)

    def out_at(g, c):
        return pl.ds(pl.multiple_of(g * col_width + out_first[c], HEAD_SIZE), out_cols[c])

    def out_part(r, c):
        return osend.at[r, :, pl.ds(out_first[c], out_cols[c])]

    def out_copy(c, r):
        return remote(
            out_part(r, c), obuf.at[:, out_at(group, c)], out_send.at[c, r], out_recv.at[c, group],
            dev(core, r // 2, z, r % 2),
        )

    def away(r):
        return (apart == 1) | (h != r)

    def project_out(c):
        cols = slice(out_first[c], out_first[c] + out_cols[c])
        result = None
        for g in range(heads):
            right = w_proj[g // 2, g % 2, :, :, cols]
            if right.shape[1] % 16:
                right = right.astype(f32).reshape(-1, out_cols[c]).astype(bf16)
            else:
                right = right.reshape(-1, out_cols[c])
            term = jnp.dot(mixed[g], right, preferred_element_type=f32)
            result = term if result is None else result + term
        osend[:, :, cols] = result.astype(bf16).reshape(heads, own, out_cols[c])
        for r in range(heads):
            @pl.when(away(r))
            def _():
                out_copy(c, r).start()

        @pl.when(apart == 0)
        def _():
            obuf[:, out_at(group, c)] = osend[h, :, cols]

    def drain_unit(u):
        def one(row, _):
            @pl.when((row <= z) & (z < steps - 1))
            def _():
                line_copy(u, UP, row).wait_send()

            @pl.when((row >= z) & (z > 0))
            def _():
                line_copy(u, DOWN, row).wait_send()

            mate_copy(u, row).wait_send()
            return 0

        lax.fori_loop(0, steps, one, 0)

    def drain_in():
        for u in range(first_out):
            drain_unit(u)

        @pl.when(apart == 1)
        def _():
            for u in range(first_out):
                cross_copy(u).wait_send()
            for copy in act_mate:
                copy.wait_send()

        for copy in act_copies + redis_copies:
            copy.wait_send()
        for f in (0, 1):
            @pl.when(apart == 1 - f)
            def _():
                for i in (0, 1):
                    relay_copy(i, f).wait_send()

        @pl.when(core == 0)
        def _():
            kv_mate.wait_send()

        def kv_drain(k):
            @pl.when(z + k < steps)
            def _():
                kv_copy(k).wait_send()

            @pl.when(kv_passes(k))
            def _():
                kv_pass_copy(k).wait_send()

        kv_each(1, reach // 2 + 1, kv_drain)
        for u in range(1, first_out):
            for i, (x_, y_) in enumerate(redis_peers()):
                mix_copy(u, i, x_, y_).wait_send()

    def store_copy(c, g):
        return pltpu.make_async_copy(
            obuf.at[:, out_at(g, c)], out_ref.at[:, out_at(g, c)], store_sem.at[c, g]
        )

    def take_out(c):
        for g in range(heads):
            @pl.when((apart == 1) | (group != g))
            def _():
                ref = obuf.at[:, out_at(g, c)]
                remote(ref, ref, out_send.at[0, 0], out_recv.at[c, g], mate).wait_recv()

            store_copy(c, g).start()

    def drain_out(c):
        drain_unit(first_out + c)
        for r in range(heads):
            @pl.when(away(r))
            def _():
                out_copy(c, r).wait_send()

        for g in range(heads):
            store_copy(c, g).wait()

    for c in range(chunks):
        outer_steps(first_out + c, 1, steps)
        mate_wait(first_out + c)
        if c == 0:
            mix_wait()
        project_out(c)
        if c == 0:
            drain_in()
        if c >= 2:
            take_out(c - 2)
        if c >= 3:
            drain_out(c - 3)
    for c in range(max(chunks - 3, 0), max(chunks - 2, 0)):
        drain_out(c)
    for c in range(max(chunks - 2, 0), chunks):
        take_out(c)
    for c in range(max(chunks - 2, 0), chunks):
        drain_out(c)


def on_device(tokens, w_query, key_value_weight, w_out, doc_lengths):
    n = lax.axis_size("blk")
    heads = lax.axis_size("heads")
    assert heads == 4
    q_units, chunks = Q_UNITS, len(OUT_PARTS)
    steps = n // LINE
    own, width = tokens.shape
    block = own * heads
    rows_in, q_cols = w_query.shape
    kv_cols = 2 * key_value_weight.shape[2]
    rows_out = w_out.shape[0]
    col_width = width // heads
    out_cols = tuple(col_width * part // sum(OUT_PARTS) for part in OUT_PARTS)
    q_heads = q_cols // HEAD_SIZE
    reach = n // 4
    units = 1 + q_units + chunks
    half = HEAD_SIZE // 2
    freqs = np.power(rope_base, -2.0 * np.arange(half) / HEAD_SIZE).astype(np.float32)
    freqs = jnp.asarray(np.concatenate([freqs, freqs])[None, :])
    bf16, f32 = jnp.bfloat16, jnp.float32
    dma = pltpu.SemaphoreType.DMA
    return pl.pallas_call(
        functools.partial(layer_kernel, n, heads, out_cols, q_units),
        out_shape=jax.ShapeDtypeStruct((own, width), bf16),
        in_specs=[pl.BlockSpec(memory_space=pl.ANY)] * 4 + [
            pl.BlockSpec(memory_space=pltpu.SMEM),
            pl.BlockSpec(memory_space=pl.ANY),
        ],
        out_specs=pl.BlockSpec(memory_space=pl.ANY),
        scratch_shapes=[
            pltpu.VMEM((own, width), bf16),
            pltpu.VMEM(key_value_weight.shape, bf16),
            pltpu.VMEM((1, HEAD_SIZE), f32),
            pltpu.VMEM((n * rows_in, kv_cols), bf16),
            pltpu.VMEM((q_units, n * rows_in, q_cols // q_units), bf16),
            pltpu.VMEM((2, 2, n, rows_out, col_width), bf16),
            pltpu.VMEM((rows_in, kv_cols), bf16),
            pltpu.VMEM((own, width), bf16),
            pltpu.VMEM((heads, own, width), bf16),
            pltpu.VMEM((block, q_cols + kv_cols), f32),
            pltpu.VMEM((block, q_cols), bf16),
            pltpu.VMEM((reach + 1, block, kv_cols), bf16),
            pltpu.VMEM((q_heads, block, 1), f32),
            pltpu.VMEM((q_heads, block, 1), f32),
            pltpu.VMEM((block, q_cols), f32),
            pltpu.VMEM((heads, block, q_cols), bf16),
            pltpu.VMEM((2, block, HEAD_SIZE), f32),
            pltpu.VMEM((heads, own, col_width), bf16),
            pltpu.VMEM((own, width), bf16),
            dma((units, steps + 1)),
            dma((units, steps)),
            dma((units, 2, steps)),
            dma((1 + q_units,)),
            dma((1 + q_units,)),
            dma((3,)),
            dma((chunks, heads)),
            dma((3,)),
            dma((heads,)),
            dma((8,)),
            dma((2, heads)),
            dma((reach + 1,)),
            dma((reach + 1,)),
            dma((reach + 1,)),
            dma((q_units, 3)),
            dma((q_units, heads)),
            dma((chunks, heads)),
            dma((chunks, heads)),
        ],
        compiler_params=pltpu.CompilerParams(
            collective_id=0, has_side_effects=True, vmem_limit_bytes=60 * 1024 * 1024
        ),
    )(tokens, w_query, key_value_weight, w_out, doc_lengths, freqs)


def solution(mesh):
    return jax.shard_map(
        on_device,
        mesh=mesh,
        in_specs=(
            P(("blk", "heads"), None),
            P("blk", "heads"),
            P("blk", None, "heads"),
            P(("heads", "blk"), None),
            P(),
        ),
        out_specs=P(("blk", "heads"), None),
        check_vma=False,
    )
```

```python
import functools

import jax
import jax.numpy as jnp
import numpy as np
from jax import lax
from jax.experimental import pallas as pl
from jax.experimental.pallas import tpu as pltpu
from jax.sharding import PartitionSpec as P

HEAD_SIZE = 128
LINE = 2
Q_UNITS = 2
OUT_PARTS = (4, 2, 2)
LEFT_PARTS = (5, 8)

norm_epsilon = 1e-05
rope_base = 500000.0
masked_score = -1e30
MESH = pl.DeviceIdType.MESH
UP, DOWN = 0, 1


def layer_kernel(
    n, heads, out_cols, q_units,
    tok_ref, w_query_ref, w_keyval_ref, w_out_ref, len_ref, freq_ref, out_ref,
    tok_buf, kv_raw, freq_buf, w_kv, w_q, w_proj, kv_stage, act_stage, acts, qkv, query, kv, high, total, accum, mixed, rope, osend, obuf,
    line_send, mate_send, recv, mate_recv, cross_send, local_sem, load_sem, store_sem, redis_send, redis_recv,
    act_send, act_recv, kv_send, kv_recv, kv_pass_send, mix_send, mix_recv, out_send, out_recv,
):
    f32, bf16 = jnp.float32, jnp.bfloat16
    b = lax.axis_index("blk")
    h = lax.axis_index("heads")
    steps = n // LINE
    z, x = b // LINE, b % LINE
    y, core = h // 2, h % 2
    group = 2 * y + x
    block_id = LINE * z + core
    apart = (x + core) % 2
    reach = n // 4
    own, width = tok_ref.shape
    rows_in = w_query_ref.shape[0]
    block = own * heads
    q_cols = query.shape[1]
    q_heads = q_cols // HEAD_SIZE
    unit_cols = q_cols // q_units
    unit_heads = q_heads // q_units
    col_width = width // heads
    chunks = len(out_cols)
    out_first = [sum(out_cols[:c]) for c in range(chunks)]
    left = width * LEFT_PARTS[0] // LEFT_PARTS[1]
    first_out = 1 + q_units
    units = first_out + chunks

    def dev(x_, y_, z_, c_):
        return {"blk": LINE * z_ + x_, "heads": 2 * y_ + c_}

    mate = dev(x, y, z, 1 - core)

    def remote(src, dst, ss, rs, device):
        return pltpu.make_async_remote_copy(
            src_ref=src, dst_ref=dst, send_sem=ss, recv_sem=rs, device_id=device, device_id_type=MESH
        )

    barrier = pltpu.get_barrier_semaphore()
    for dx, dy, dc in [(i, j, k) for i in (0, 1) for j in (0, 1) for k in (0, 1) if i + j + k]:
        pl.semaphore_signal(
            barrier, inc=1, device_id=dev((x + dx) % 2, (y + dy) % 2, z, (core + dc) % 2), device_id_type=MESH
        )
    span = (reach + 1) // 2
    for d in range(1, span + 1):
        for c_ in (0, 1):
            @pl.when(z + d < steps)
            def _():
                pl.semaphore_signal(barrier, inc=1, device_id=dev(x, y, z + d, c_), device_id_type=MESH)

            @pl.when(z - d >= 0)
            def _():
                pl.semaphore_signal(barrier, inc=1, device_id=dev(x, y, z - d, c_), device_id_type=MESH)
    near = jnp.minimum(z, span) + jnp.minimum(steps - 1 - z, span)
    loads = [
        pltpu.make_async_copy(src, dst, load_sem.at[i])
        for i, (src, dst) in enumerate([(w_keyval_ref, kv_raw), (tok_ref, tok_buf), (freq_ref, freq_buf)])
    ]
    for load in loads:
        load.start()

    def unit_ref(u, k, row):
        i = LINE * row + k
        if u == 0:
            return w_kv.at[pl.ds(pl.multiple_of(i * rows_in, rows_in), rows_in)]
        if u < first_out:
            return w_q.at[u - 1, pl.ds(pl.multiple_of(i * rows_in, rows_in), rows_in)]
        return w_proj.at[:, k, pl.ds(LINE * row, LINE), :, pl.ds(out_first[u - first_out], out_cols[u - first_out])]

    def line_copy(u, direction, row):
        ref = unit_ref(u, core, row)
        z_ = z + 1 if direction == UP else z - 1
        at = row
        if direction == DOWN:
            at = jnp.where(row == z, steps, row)
        return remote(ref, ref, line_send.at[u, at], recv.at[u, row], dev(x, y, z_, core))

    def mate_copy(u, row):
        ref = unit_ref(u, core, row)
        return remote(ref, ref, mate_send.at[u], mate_recv.at[u], mate)

    def mate_all(u):
        if u == 0:
            ref = w_kv.at[pl.ds(0, steps * rows_in)]
        elif u < first_out:
            ref = w_q.at[u - 1, pl.ds(0, steps * rows_in)]
        else:
            ref = w_proj.at[:, 0, :, :, pl.ds(out_first[u - first_out], out_cols[u - first_out])]
        return remote(ref, ref, mate_send.at[u], mate_recv.at[u], mate)

    def arrive(u, row):
        ref = unit_ref(u, core, row)
        remote(ref, ref, mate_send.at[u], recv.at[u, row], mate).wait_recv()

    def query_cols(u):
        return w_query_ref.at[:, pl.ds((u - 1) * unit_cols, unit_cols)]

    def cross_copy(u):
        src = kv_stage if u == 0 else query_cols(u)
        return remote(src, unit_ref(u, x, z), cross_send.at[u], recv.at[u, z], dev(1 - x, y, z, 1 - core))

    def keep_query(u):
        return pltpu.make_async_copy(query_cols(u), unit_ref(u, core, z), local_sem.at[u])

    def own_start(u):
        @pl.when(z < steps - 1)
        def _():
            line_copy(u, UP, z).start()

        @pl.when(z > 0)
        def _():
            line_copy(u, DOWN, z).start()

        mate_copy(u, z).start()

    def redis_peers():
        return [(1 - x, y), (x, 1 - y), (1 - x, 1 - y)]

    def redis_copy(x_, y_):
        cols = pl.ds(pl.multiple_of((2 * y_ + x_) * col_width, col_width), col_width)
        return remote(
            w_out_ref.at[:, cols], w_proj.at[y, core, b], redis_send.at[0], redis_recv.at[0],
            dev(x_, y_, z, core),
        )

    def redis_all():
        ref = w_proj.at[0, 0, pl.ds(0, 3)]
        return remote(ref, ref, redis_send.at[0], redis_recv.at[0], mate)

    def keep_out():
        cols = pl.ds(pl.multiple_of(group * col_width, col_width), col_width)
        return pltpu.make_async_copy(w_out_ref.at[:, cols], w_proj.at[y, core, b], local_sem.at[0])

    def own_wait(u):
        if u == 0:
            @pl.when(apart == 1)
            def _():
                arrive(u, z)
        elif u < first_out:
            @pl.when(apart == 1)
            def _():
                arrive(u, z)

            @pl.when(apart == 0)
            def _():
                keep_query(u).wait()
        elif u == first_out:
            keep_out().wait()
            redis_all().wait_recv()

    def line_step(u, s):
        @pl.when(z - s >= 0)
        def _():
            arrive(u, z - s)

            @pl.when(z < steps - 1)
            def _():
                line_copy(u, UP, z - s).start()

            mate_copy(u, z - s).start()

        @pl.when(z + s <= steps - 1)
        def _():
            arrive(u, z + s)

            @pl.when(z > 0)
            def _():
                line_copy(u, DOWN, z + s).start()

            mate_copy(u, z + s).start()

    def line_steps(u, low, high_):
        def one(s, _):
            line_step(u, s)
            return 0

        lax.fori_loop(low, high_, one, 0)

    inner = (z > 0) & (z < steps - 1)

    def inner_steps(u, low, high_):
        @pl.when(inner)
        def _():
            line_steps(u, low, high_)

    def outer_steps(u, low, high_):
        @pl.when(jnp.logical_not(inner))
        def _():
            line_steps(u, low, high_)

    def mate_wait(u):
        mate_all(u).wait_recv()

    @pl.when(apart == 0)
    def _():
        for u in range(1, first_out):
            keep_query(u).start()

    keep_out().start()
    loads[0].wait()
    own_kv = kv_raw[...].reshape(rows_in, w_kv.shape[1])

    @pl.when(apart == 0)
    def _():
        w_kv[pl.ds(pl.multiple_of(b * rows_in, rows_in), rows_in), :] = own_kv

    @pl.when(apart == 1)
    def _():
        kv_stage[...] = own_kv

    loads[1].wait()
    values = tok_buf[...].astype(f32)
    normed = (
        values * lax.rsqrt(jnp.mean(values * values, axis=1, keepdims=True) + norm_epsilon)
    ).astype(bf16)
    act_stage[...] = normed

    @pl.when(apart == 0)
    def _():
        acts[h] = normed

    pl.semaphore_wait(barrier, 7 + 2 * near)

    @pl.when(apart == 0)
    def _():
        own_start(0)
        own_wait(1)
        own_start(1)

    @pl.when(apart == 1)
    def _():
        for u in range(2):
            cross_copy(u).start()

    act_cols = [(0, left), (left, width - left)]

    def act_ref(h_, f):
        return acts.at[h_, :, pl.ds(*act_cols[f])]

    def act_copy(i, h_, f, device, src=None):
        src = act_ref(h_, f) if src is None else src
        return remote(src, act_ref(h_, f), act_send.at[i], act_recv.at[f, h_], device)

    def act_own(i, f, device):
        return act_copy(i, h, f, device, act_stage.at[:, pl.ds(*act_cols[f])])

    def act_wait(h_, f):
        remote(act_ref(h_, f), act_ref(h_, f), act_send.at[0], act_recv.at[f, h_], mate).wait_recv()

    act_copies = [
        act_own(0, 1, dev(x, 1 - y, z, x)),
        act_own(0, 0, dev(1 - x, y, z, x)),
        act_own(0, 0, dev(x, 1 - y, z, x)),
        act_own(0, 1, dev(1 - x, y, z, x)),
    ]
    act_mate = [act_own(1, f, mate) for f in (0, 1)]
    act_copies[0].start()
    act_copies[2].start()

    @pl.when(apart == 1)
    def _():
        act_copies[1].start()
        for u in range(2, first_out):
            cross_copy(u).start()
        for copy in act_mate:
            copy.start()
        act_copies[3].start()

    redis_copies = [redis_copy(x_, y_) for x_, y_ in redis_peers()]

    relay_y = apart * y + (1 - apart) * (1 - y)

    def relay_copy(i, f):
        c = core if i == 0 else 1 - core
        to = dev(x, 1 - y, z, core) if f == 0 else dev(1 - x, y, z, core)
        return act_copy(2 + i, 2 * relay_y + c, f, to)

    def relay(i):
        for f in (0, 1):
            @pl.when(apart == 1 - f)
            def _():
                act_wait(2 * relay_y + (core if i == 0 else 1 - core), f)
                relay_copy(i, f).start()

    def acts_wait():
        for h_ in range(heads):
            for f in (0, 1):
                mine = (apart == 0) & (h == h_)
                relayed = (apart == 1 - f) & (relay_y == h_ // 2)

                @pl.when(jnp.logical_not(mine | relayed))
                def _():
                    act_wait(h_, f)

    @pl.when(apart == 1)
    def _():
        own_wait(0)
        own_start(0)

    pos = block_id * block + lax.broadcasted_iota(jnp.int32, (block, 1), 0)
    start = jnp.zeros((block, 1), jnp.int32)
    end = jnp.int32(0)
    for i in range(len_ref.shape[0]):
        size = len_ref[i]
        end = end + size
        start = start + jnp.where(pos >= end, size, 0)
    loads[2].wait()
    angle = (pos - start).astype(f32) * freq_buf[...]
    lane = lax.broadcasted_iota(jnp.int32, (block, HEAD_SIZE), 1)
    rope[0] = jnp.cos(angle)
    rope[1] = jnp.where(lane < HEAD_SIZE // 2, -jnp.sin(angle), jnp.sin(angle))
    qkv[...] = jnp.zeros_like(qkv)

    @pl.when(apart == 1)
    def _():
        own_wait(1)
        own_start(1)

    line_steps(0, 1, 2)

    @pl.when(apart == 0)
    def _():
        act_copies[1].start()
        act_copies[3].start()

    relay(0)
    line_steps(0, 2, steps)
    relay(1)
    for copy in redis_copies:
        copy.start()
    last_in = first_out - 1

    @pl.when(inner)
    def _():
        for u in range(2, first_out):
            line_steps(u - 1, 1, steps)
            own_wait(u)
            own_start(u)
        line_steps(last_in, 1, 2)

    @pl.when(jnp.logical_not(inner))
    def _():
        for u in range(2, first_out):
            own_wait(u)
            own_start(u)

    for d in range(1, reach + 1):
        @pl.when(block_id < d)
        def _():
            kv[d] = jnp.zeros_like(kv[d])

    acts_wait()

    depth = min(1024, width)

    def project(weights, cols):
        def one(k, _):
            rows = pl.ds(pl.multiple_of(k * depth, depth), depth)
            left = acts[:, :, rows].reshape(block, depth)
            qkv[:, cols] += jnp.dot(left, weights[rows, :], preferred_element_type=f32)
            return 0

        lax.fori_loop(0, width // depth, one, 0)

    def rotated(first):
        v = qkv[:, first:first + HEAD_SIZE]
        return (v * rope[0] + pltpu.roll(v, HEAD_SIZE // 2, 1) * rope[1]).astype(bf16)

    def project_query(u):
        mate_wait(u)
        first = (u - 1) * unit_cols
        project(w_q.at[u - 1], slice(first, first + unit_cols))
        for j in range(first // HEAD_SIZE, (first + unit_cols) // HEAD_SIZE):
            query[:, j * HEAD_SIZE:(j + 1) * HEAD_SIZE] = rotated(j * HEAD_SIZE)

    def kv_copy(k):
        return remote(
            kv.at[0], kv.at[2 * k], kv_send.at[2 * k], kv_recv.at[2 * k], dev(x, y, z + k, core)
        )

    kv_mate = remote(kv.at[0], kv.at[1], kv_send.at[1], kv_recv.at[1], mate)

    def kv_pass_copy(k):
        to = 2 * k + 1 - 2 * core
        return remote(kv.at[2 * k], kv.at[to], kv_pass_send.at[2 * k], kv_recv.at[to], mate)

    def kv_passes(k):
        return (z >= k) & (2 * k + 1 - 2 * core <= reach)

    def kv_each(low, high_, body):
        def one(k, _):
            body(k)
            return 0

        lax.fori_loop(low, high_, one, 0)

    def kv_start():
        @pl.when(core == 0)
        def _():
            kv_mate.start()

        def one(k):
            @pl.when(z + k < steps)
            def _():
                kv_copy(k).start()

        kv_each(1, reach // 2 + 1, one)

    def kv_wait(d):
        remote(kv.at[d], kv.at[d], kv_send.at[d], kv_recv.at[d], mate).wait_recv()

    def kv_ready():
        def even(k):
            @pl.when(z >= k)
            def _():
                kv_wait(2 * k)

            @pl.when(kv_passes(k))
            def _():
                kv_pass_copy(k).start()

        def odd(k):
            @pl.when(block_id >= 2 * k + 1)
            def _():
                kv_wait(2 * k + 1)

        kv_each(1, reach // 2 + 1, even)
        kv_each(0, reach // 2, odd)

    own_pos = lax.broadcasted_iota(jnp.int32, (block, 1), 0)
    own_start_pos = start - block_id * block
    key_lane = lax.broadcasted_iota(jnp.int32, (1, block), 1)
    scale = HEAD_SIZE ** (-0.5) * float(np.log2(np.e))

    def attend_own(u):
        def one(j, _):
            cols = pl.ds(pl.multiple_of(j * HEAD_SIZE, HEAD_SIZE), HEAD_SIZE)
            keep = (key_lane >= own_start_pos) & (key_lane <= own_pos)
            scores = lax.dot_general(
                query[:, cols], kv[0, :, :HEAD_SIZE], (((1,), (1,)), ((), ())),
                preferred_element_type=f32,
            )
            scores = jnp.where(keep, scores, masked_score)
            new = jnp.max(scores, axis=1, keepdims=True)
            probs = jnp.exp2((scores - new) * scale)
            high[j] = new
            total[j] = jnp.sum(probs, axis=1, keepdims=True)
            accum[:, cols] = jnp.dot(probs.astype(bf16), kv[0, :, HEAD_SIZE:], preferred_element_type=f32)
            return 0

        lax.fori_loop((u - 1) * unit_heads, u * unit_heads, one, 0)

    def attend_earlier(u, d):
        keep = key_lane - d * block >= own_start_pos

        def one(j, _):
            cols = pl.ds(pl.multiple_of(j * HEAD_SIZE, HEAD_SIZE), HEAD_SIZE)
            scores = lax.dot_general(
                query[:, cols], kv[d, :, :HEAD_SIZE], (((1,), (1,)), ((), ())),
                preferred_element_type=f32,
            )
            scores = jnp.where(keep, scores, masked_score)
            old = high[j]
            new = jnp.maximum(old, jnp.max(scores, axis=1, keepdims=True))
            fading = jnp.exp2((old - new) * scale)
            probs = jnp.exp2((scores - new) * scale)
            total[j] = total[j] * fading + jnp.sum(probs, axis=1, keepdims=True)
            update = jnp.dot(probs.astype(bf16), kv[d, :, HEAD_SIZE:], preferred_element_type=f32)
            accum[:, cols] = accum[:, cols] * fading + update
            high[j] = new
            return 0

        lax.fori_loop((u - 1) * unit_heads, u * unit_heads, one, 0)

    def attend_tiles(u):
        tile = block // 4

        def one(j, _):
            cols = pl.ds(pl.multiple_of(j * HEAD_SIZE, HEAD_SIZE), HEAD_SIZE)
            for i in range(4):
                rows = slice(i * tile, (i + 1) * tile)
                spans = [(0, 0, (i + 1) * tile)]
                spans += [(d, 0, block) for d in range(1, reach)]
                spans += [(reach, i * tile, block)]
                parts = []
                for d, low, high_ in spans:
                    scores = lax.dot_general(
                        query[rows, cols], kv[d, low:high_, :HEAD_SIZE], (((1,), (1,)), ((), ())),
                        preferred_element_type=f32,
                    )
                    key_pos = low - d * block + lax.broadcasted_iota(jnp.int32, (1, high_ - low), 1)
                    keep = key_pos >= own_start_pos[rows]
                    if d == 0:
                        keep = keep & (key_pos <= own_pos[rows])
                    parts.append(jnp.where(keep, scores, masked_score))
                top = functools.reduce(jnp.maximum, [jnp.max(p, axis=1, keepdims=True) for p in parts])
                probs = [jnp.exp2((p - top) * scale) for p in parts]
                denom = sum(jnp.sum(p, axis=1, keepdims=True) for p in probs)
                result = sum(
                    jnp.dot(p.astype(bf16), kv[d, low:high_, HEAD_SIZE:], preferred_element_type=f32)
                    for p, (d, low, high_) in zip(probs, spans)
                )
                mixed[group, rows, cols] = (result / denom).astype(bf16)
            return 0

        lax.fori_loop((u - 1) * unit_heads, u * unit_heads, one, 0)

    def mix_cols(u):
        return pl.ds((u - 1) * unit_cols, unit_cols)

    def mix_copy(u, x_, y_):
        ref = mixed.at[group, :, mix_cols(u)]
        return remote(ref, ref, mix_send.at[u - 1], mix_recv.at[u - 1], dev(x_, y_, z, core))

    def attend(u):
        if reach <= 2:
            attend_tiles(u)
        else:
            attend_own(u)
            finish_heads(u)
        for x_, y_ in redis_peers():
            mix_copy(u, x_, y_).start()

    def finish_heads(u):
        def one(d, _):
            @pl.when(block_id >= d)
            def _():
                attend_earlier(u, d)
            return 0

        lax.fori_loop(1, reach + 1, one, 0)
        for j in range((u - 1) * unit_heads, u * unit_heads):
            cols = slice(j * HEAD_SIZE, (j + 1) * HEAD_SIZE)
            mixed[group, :, cols] = (accum[:, cols] / total[j]).astype(bf16)

    def mix_all(u):
        ref = mixed.at[pl.ds(0, 3), :, mix_cols(u)]
        return remote(ref, ref, mix_send.at[u - 1], mix_recv.at[u - 1], mate)

    def mix_wait():
        for u in range(1, first_out):
            mix_all(u).wait_recv()

    mate_wait(0)
    project(w_kv, slice(q_cols, q_cols + w_kv.shape[1]))
    kv[0, :, :HEAD_SIZE] = rotated(q_cols)
    kv[0, :, HEAD_SIZE:] = qkv[:, q_cols + HEAD_SIZE:].astype(bf16)
    kv_start()
    for u in range(1, last_in):
        outer_steps(u, 1, steps)
    inner_steps(last_in, 2, steps)
    for u in range(1, last_in):
        project_query(u)
    own_wait(first_out)
    own_start(first_out)

    @pl.when(jnp.logical_not(inner))
    def _():
        for u in range(first_out + 1, units):
            own_start(u)

    @pl.when(inner)
    def _():
        project_query(last_in)

    kv_ready()
    for u in range(1, last_in):
        attend(u)
    outer_steps(last_in, 1, steps)

    @pl.when(jnp.logical_not(inner))
    def _():
        project_query(last_in)

    @pl.when(inner)
    def _():
        line_step(first_out, 1)
        own_start(first_out + 1)

    attend(last_in)

    @pl.when(inner)
    def _():
        line_steps(first_out, 2, steps)
        for u in range(first_out + 1, units):
            if u + 1 < units:
                own_start(u + 1)
            line_steps(u, 1, steps)

    def out_at(g, c):
        return pl.ds(pl.multiple_of(g * col_width + out_first[c], HEAD_SIZE), out_cols[c])

    def out_part(r, c):
        return osend.at[r, :, pl.ds(out_first[c], out_cols[c])]

    def out_copy(c, r):
        return remote(
            out_part(r, c), obuf.at[:, out_at(group, c)], out_send.at[c], out_recv.at[c],
            dev(core, r // 2, z, r % 2),
        )

    def away(r):
        return (apart == 1) | (h != r)

    def project_out(c):
        cols = slice(out_first[c], out_first[c] + out_cols[c])
        result = None
        for g in range(heads):
            right = w_proj[g // 2, g % 2, :, :, cols]
            if right.shape[1] % 16:
                right = right.astype(f32).reshape(-1, out_cols[c]).astype(bf16)
            else:
                right = right.reshape(-1, out_cols[c])
            term = jnp.dot(mixed[g], right, preferred_element_type=f32)
            result = term if result is None else result + term
        osend[:, :, cols] = result.astype(bf16).reshape(heads, own, out_cols[c])
        for r in range(heads):
            @pl.when(away(r))
            def _():
                out_copy(c, r).start()

        @pl.when(apart == 0)
        def _():
            obuf[:, out_at(group, c)] = osend[h, :, cols]

    def drain_unit(u):
        def one(row, _):
            @pl.when((row <= z) & (z < steps - 1))
            def _():
                line_copy(u, UP, row).wait_send()

            @pl.when((row >= z) & (z > 0))
            def _():
                line_copy(u, DOWN, row).wait_send()
            return 0

        lax.fori_loop(0, steps, one, 0)
        mate_all(u).wait_send()

    def act_all(i, count):
        ref = acts.at[pl.ds(0, count)]
        return remote(ref, ref, act_send.at[i], act_recv.at[0, 0], mate)

    def drain_in():
        for u in range(first_out):
            drain_unit(u)

        @pl.when(apart == 1)
        def _():
            for u in range(first_out):
                cross_copy(u).wait_send()
            act_all(1, 1).wait_send()

        act_all(0, 2).wait_send()
        redis_all().wait_send()
        for f in (0, 1):
            @pl.when(apart == 1 - f)
            def _():
                for i in (0, 1):
                    relay_copy(i, f).wait_send()

        @pl.when(core == 0)
        def _():
            kv_mate.wait_send()

        def kv_drain(k):
            @pl.when(z + k < steps)
            def _():
                kv_copy(k).wait_send()

            @pl.when(kv_passes(k))
            def _():
                kv_pass_copy(k).wait_send()

        kv_each(1, reach // 2 + 1, kv_drain)
        for u in range(1, first_out):
            mix_all(u).wait_send()

    def out_each(c, body):
        for count in (heads - 1, heads):
            @pl.when(apart == count - heads + 1)
            def _():
                ref = obuf.at[:, pl.ds(0, count * out_cols[c])]
                body(remote(ref, ref, out_send.at[c], out_recv.at[c], mate))

    def take_out(c):
        out_each(c, lambda copy: copy.wait_recv())
        for g in range(heads):
            pltpu.make_async_copy(
                obuf.at[:, out_at(g, c)], out_ref.at[:, out_at(g, c)], store_sem.at[c]
            ).start()

    def drain_out(c):
        drain_unit(first_out + c)
        out_each(c, lambda copy: copy.wait_send())

    for c in range(chunks):
        outer_steps(first_out + c, 1, steps)
        mate_wait(first_out + c)
        if c == 0:
            mix_wait()
        project_out(c)
        if c == 0:
            drain_in()
    for c in range(chunks):
        drain_out(c)
        take_out(c)
    for c in range(chunks):
        cols = pl.ds(0, heads * out_cols[c])
        pltpu.make_async_copy(obuf.at[:, cols], out_ref.at[:, cols], store_sem.at[c]).wait()


def on_device(tokens, w_query, key_value_weight, w_out, doc_lengths):
    n = lax.axis_size("blk")
    heads = lax.axis_size("heads")
    assert heads == 4
    q_units, chunks = Q_UNITS, len(OUT_PARTS)
    steps = n // LINE
    own, width = tokens.shape
    block = own * heads
    rows_in, q_cols = w_query.shape
    kv_cols = 2 * key_value_weight.shape[2]
    rows_out = w_out.shape[0]
    col_width = width // heads
    out_cols = tuple(col_width * part // sum(OUT_PARTS) for part in OUT_PARTS)
    q_heads = q_cols // HEAD_SIZE
    reach = n // 4
    units = 1 + q_units + chunks
    half = HEAD_SIZE // 2
    freqs = np.power(rope_base, -2.0 * np.arange(half) / HEAD_SIZE).astype(np.float32)
    freqs = jnp.asarray(np.concatenate([freqs, freqs])[None, :])
    bf16, f32 = jnp.bfloat16, jnp.float32
    dma = pltpu.SemaphoreType.DMA
    return pl.pallas_call(
        functools.partial(layer_kernel, n, heads, out_cols, q_units),
        out_shape=jax.ShapeDtypeStruct((own, width), bf16),
        in_specs=[pl.BlockSpec(memory_space=pl.ANY)] * 4 + [
            pl.BlockSpec(memory_space=pltpu.SMEM),
            pl.BlockSpec(memory_space=pl.ANY),
        ],
        out_specs=pl.BlockSpec(memory_space=pl.ANY),
        scratch_shapes=[
            pltpu.VMEM((own, width), bf16),
            pltpu.VMEM(key_value_weight.shape, bf16),
            pltpu.VMEM((1, HEAD_SIZE), f32),
            pltpu.VMEM((n * rows_in, kv_cols), bf16),
            pltpu.VMEM((q_units, n * rows_in, q_cols // q_units), bf16),
            pltpu.VMEM((2, 2, n, rows_out, col_width), bf16),
            pltpu.VMEM((rows_in, kv_cols), bf16),
            pltpu.VMEM((own, width), bf16),
            pltpu.VMEM((heads, own, width), bf16),
            pltpu.VMEM((block, q_cols + kv_cols), f32),
            pltpu.VMEM((block, q_cols), bf16),
            pltpu.VMEM((reach + 1, block, kv_cols), bf16),
            pltpu.VMEM((q_heads, block, 1), f32),
            pltpu.VMEM((q_heads, block, 1), f32),
            pltpu.VMEM((block, q_cols), f32),
            pltpu.VMEM((heads, block, q_cols), bf16),
            pltpu.VMEM((2, block, HEAD_SIZE), f32),
            pltpu.VMEM((heads, own, col_width), bf16),
            pltpu.VMEM((own, width), bf16),
            dma((units, steps + 1)),
            dma((units,)),
            dma((units, steps)),
            dma((units,)),
            dma((1 + q_units,)),
            dma((1 + q_units,)),
            dma((3,)),
            dma((chunks,)),
            dma((1,)),
            dma((1,)),
            dma((4,)),
            dma((2, heads)),
            dma((reach + 1,)),
            dma((reach + 1,)),
            dma((reach + 1,)),
            dma((q_units,)),
            dma((q_units,)),
            dma((chunks,)),
            dma((chunks,)),
        ],
        compiler_params=pltpu.CompilerParams(
            collective_id=0, has_side_effects=True, vmem_limit_bytes=60 * 1024 * 1024
        ),
    )(tokens, w_query, key_value_weight, w_out, doc_lengths, freqs)


def solution(mesh):
    return jax.shard_map(
        on_device,
        mesh=mesh,
        in_specs=(
            P(("blk", "heads"), None),
            P("blk", "heads"),
            P("blk", None, "heads"),
            P(("heads", "blk"), None),
            P(),
        ),
        out_specs=P(("blk", "heads"), None),
        check_vma=False,
    )
```

```python
import functools

import jax
import jax.numpy as jnp
import numpy as np
from jax import lax
from jax.experimental import pallas as pl
from jax.experimental.pallas import tpu as pltpu
from jax.sharding import PartitionSpec as P

HEAD_SIZE = 128
LINE = 2
Q_UNITS = 2
OUT_PARTS = (4, 2, 2)
LEFT_PARTS = (5, 8)

norm_epsilon = 1e-05
rope_base = 500000.0
masked_score = -1e30
MESH = pl.DeviceIdType.MESH
UP, DOWN = 0, 1


def layer_kernel(
    n, heads, out_cols, q_units,
    tok_ref, w_query_ref, w_keyval_ref, w_out_ref, len_ref, freq_ref, out_ref,
    tok_buf, kv_raw, freq_buf, w_kv, w_q, w_proj, kv_stage, act_stage, acts, qkv, query, kv, high, total, accum, mixed, rope, osend,
    line_send, mate_send, recv, mate_recv, cross_send, local_sem, load_sem, store_sem, redis_send, redis_recv,
    act_send, act_recv, kv_send, kv_recv, kv_pass_send, mix_send, mix_recv, out_send, out_recv,
):
    f32, bf16 = jnp.float32, jnp.bfloat16
    b = lax.axis_index("blk")
    h = lax.axis_index("heads")
    steps = n // LINE
    z, x = b // LINE, b % LINE
    y, core = h // 2, h % 2
    group = 2 * y + x
    block_id = LINE * z + core
    apart = (x + core) % 2
    reach = n // 4
    own, width = tok_ref.shape
    rows_in = w_query_ref.shape[0]
    block = own * heads
    q_cols = query.shape[1]
    q_heads = q_cols // HEAD_SIZE
    unit_cols = q_cols // q_units
    unit_heads = q_heads // q_units
    col_width = width // heads
    chunks = len(out_cols)
    out_first = [sum(out_cols[:c]) for c in range(chunks)]
    left = width * LEFT_PARTS[0] // LEFT_PARTS[1]
    first_out = 1 + q_units
    units = first_out + chunks

    def dev(x_, y_, z_, c_):
        return {"blk": LINE * z_ + x_, "heads": 2 * y_ + c_}

    mate = dev(x, y, z, 1 - core)

    def remote(src, dst, ss, rs, device):
        return pltpu.make_async_remote_copy(
            src_ref=src, dst_ref=dst, send_sem=ss, recv_sem=rs, device_id=device, device_id_type=MESH
        )

    barrier = pltpu.get_barrier_semaphore()
    for dx, dy, dc in [(i, j, k) for i in (0, 1) for j in (0, 1) for k in (0, 1) if i + j + k]:
        pl.semaphore_signal(
            barrier, inc=1, device_id=dev((x + dx) % 2, (y + dy) % 2, z, (core + dc) % 2), device_id_type=MESH
        )
    span = (reach + 1) // 2
    for d in range(1, span + 1):
        for c_ in (0, 1):
            @pl.when(z + d < steps)
            def _():
                pl.semaphore_signal(barrier, inc=1, device_id=dev(x, y, z + d, c_), device_id_type=MESH)

            @pl.when(z - d >= 0)
            def _():
                pl.semaphore_signal(barrier, inc=1, device_id=dev(x, y, z - d, c_), device_id_type=MESH)
    near = jnp.minimum(z, span) + jnp.minimum(steps - 1 - z, span)
    loads = [
        pltpu.make_async_copy(src, dst, load_sem.at[i])
        for i, (src, dst) in enumerate([(w_keyval_ref, kv_raw), (tok_ref, tok_buf), (freq_ref, freq_buf)])
    ]
    for load in loads:
        load.start()

    def unit_ref(u, k, row):
        i = LINE * row + k
        if u == 0:
            return w_kv.at[pl.ds(pl.multiple_of(i * rows_in, rows_in), rows_in)]
        if u < first_out:
            return w_q.at[u - 1, pl.ds(pl.multiple_of(i * rows_in, rows_in), rows_in)]
        return w_proj.at[:, k, pl.ds(LINE * row, LINE), :, pl.ds(out_first[u - first_out], out_cols[u - first_out])]

    def line_copy(u, direction, row):
        ref = unit_ref(u, core, row)
        z_ = z + 1 if direction == UP else z - 1
        at = row
        if direction == DOWN:
            at = jnp.where(row == z, steps, row)
        return remote(ref, ref, line_send.at[u, at], recv.at[u, row], dev(x, y, z_, core))

    def mate_copy(u, row):
        ref = unit_ref(u, core, row)
        return remote(ref, ref, mate_send.at[u], mate_recv.at[u], mate)

    def mate_all(u):
        if u == 0:
            ref = w_kv.at[pl.ds(0, steps * rows_in)]
        elif u < first_out:
            ref = w_q.at[u - 1, pl.ds(0, steps * rows_in)]
        else:
            ref = w_proj.at[:, 0, :, :, pl.ds(out_first[u - first_out], out_cols[u - first_out])]
        return remote(ref, ref, mate_send.at[u], mate_recv.at[u], mate)

    def arrive(u, row):
        ref = unit_ref(u, core, row)
        remote(ref, ref, mate_send.at[u], recv.at[u, row], mate).wait_recv()

    def query_cols(u):
        return w_query_ref.at[:, pl.ds((u - 1) * unit_cols, unit_cols)]

    def cross_copy(u):
        src = kv_stage if u == 0 else query_cols(u)
        return remote(src, unit_ref(u, x, z), cross_send.at[u], recv.at[u, z], dev(1 - x, y, z, 1 - core))

    def keep_query(u):
        return pltpu.make_async_copy(query_cols(u), unit_ref(u, core, z), local_sem.at[u])

    def own_start(u):
        @pl.when(z < steps - 1)
        def _():
            line_copy(u, UP, z).start()

        @pl.when(z > 0)
        def _():
            line_copy(u, DOWN, z).start()

        mate_copy(u, z).start()

    def redis_peers():
        return [(1 - x, y), (x, 1 - y), (1 - x, 1 - y)]

    def redis_copy(x_, y_):
        cols = pl.ds(pl.multiple_of((2 * y_ + x_) * col_width, col_width), col_width)
        return remote(
            w_out_ref.at[:, cols], w_proj.at[y, core, b], redis_send.at[0], redis_recv.at[0],
            dev(x_, y_, z, core),
        )

    def redis_all():
        ref = w_proj.at[0, 0, pl.ds(0, 3)]
        return remote(ref, ref, redis_send.at[0], redis_recv.at[0], mate)

    def keep_out():
        cols = pl.ds(pl.multiple_of(group * col_width, col_width), col_width)
        return pltpu.make_async_copy(w_out_ref.at[:, cols], w_proj.at[y, core, b], local_sem.at[0])

    def own_wait(u):
        if u == 0:
            @pl.when(apart == 1)
            def _():
                arrive(u, z)
        elif u < first_out:
            @pl.when(apart == 1)
            def _():
                arrive(u, z)

            @pl.when(apart == 0)
            def _():
                keep_query(u).wait()
        elif u == first_out:
            keep_out().wait()
            redis_all().wait_recv()

    def line_step(u, s):
        @pl.when(z - s >= 0)
        def _():
            arrive(u, z - s)

            @pl.when(z < steps - 1)
            def _():
                line_copy(u, UP, z - s).start()

            mate_copy(u, z - s).start()

        @pl.when(z + s <= steps - 1)
        def _():
            arrive(u, z + s)

            @pl.when(z > 0)
            def _():
                line_copy(u, DOWN, z + s).start()

            mate_copy(u, z + s).start()

    def line_steps(u, low, high_):
        def one(s, _):
            line_step(u, s)
            return 0

        lax.fori_loop(low, high_, one, 0)

    inner = (z > 0) & (z < steps - 1)

    def inner_steps(u, low, high_):
        @pl.when(inner)
        def _():
            line_steps(u, low, high_)

    def outer_steps(u, low, high_):
        @pl.when(jnp.logical_not(inner))
        def _():
            line_steps(u, low, high_)

    def mate_wait(u):
        mate_all(u).wait_recv()

    @pl.when(apart == 0)
    def _():
        for u in range(1, first_out):
            keep_query(u).start()

    keep_out().start()
    loads[0].wait()
    own_kv = kv_raw[...].reshape(rows_in, w_kv.shape[1])

    @pl.when(apart == 0)
    def _():
        w_kv[pl.ds(pl.multiple_of(b * rows_in, rows_in), rows_in), :] = own_kv

    @pl.when(apart == 1)
    def _():
        kv_stage[...] = own_kv

    pl.semaphore_wait(barrier, 7 + 2 * near)

    @pl.when(apart == 0)
    def _():
        own_start(0)
        own_wait(1)
        own_start(1)

    @pl.when(apart == 1)
    def _():
        for u in range(2):
            cross_copy(u).start()

    loads[1].wait()
    values = tok_buf[...].astype(f32)
    normed = (
        values * lax.rsqrt(jnp.mean(values * values, axis=1, keepdims=True) + norm_epsilon)
    ).astype(bf16)
    act_stage[...] = normed

    @pl.when(apart == 0)
    def _():
        acts[h] = normed

    act_cols = [(0, left), (left, width - left)]

    def act_ref(h_, f):
        return acts.at[h_, :, pl.ds(*act_cols[f])]

    def act_copy(i, h_, f, device, src=None):
        src = act_ref(h_, f) if src is None else src
        return remote(src, act_ref(h_, f), act_send.at[i], act_recv.at[f, h_], device)

    def act_own(i, f, device):
        return act_copy(i, h, f, device, act_stage.at[:, pl.ds(*act_cols[f])])

    def act_wait(h_, f):
        remote(act_ref(h_, f), act_ref(h_, f), act_send.at[0], act_recv.at[f, h_], mate).wait_recv()

    act_copies = [
        act_own(0, 1, dev(x, 1 - y, z, x)),
        act_own(0, 0, dev(1 - x, y, z, x)),
        act_own(0, 0, dev(x, 1 - y, z, x)),
        act_own(0, 1, dev(1 - x, y, z, x)),
    ]
    act_mate = [act_own(1, f, mate) for f in (0, 1)]
    act_copies[0].start()
    act_copies[2].start()

    @pl.when(apart == 1)
    def _():
        act_copies[1].start()
        for u in range(2, first_out):
            cross_copy(u).start()
        for copy in act_mate:
            copy.start()
        act_copies[3].start()

    redis_copies = [redis_copy(x_, y_) for x_, y_ in redis_peers()]

    relay_y = apart * y + (1 - apart) * (1 - y)

    def relay_copy(i, f):
        c = core if i == 0 else 1 - core
        to = dev(x, 1 - y, z, core) if f == 0 else dev(1 - x, y, z, core)
        return act_copy(2 + i, 2 * relay_y + c, f, to)

    def relay(i):
        for f in (0, 1):
            @pl.when(apart == 1 - f)
            def _():
                act_wait(2 * relay_y + (core if i == 0 else 1 - core), f)
                relay_copy(i, f).start()

    def acts_wait():
        for h_ in range(heads):
            for f in (0, 1):
                mine = (apart == 0) & (h == h_)
                relayed = (apart == 1 - f) & (relay_y == h_ // 2)

                @pl.when(jnp.logical_not(mine | relayed))
                def _():
                    act_wait(h_, f)

    @pl.when(apart == 1)
    def _():
        own_wait(0)
        own_start(0)

    pos = block_id * block + lax.broadcasted_iota(jnp.int32, (block, 1), 0)
    start = jnp.zeros((block, 1), jnp.int32)
    end = jnp.int32(0)
    for i in range(len_ref.shape[0]):
        size = len_ref[i]
        end = end + size
        start = start + jnp.where(pos >= end, size, 0)
    loads[2].wait()
    angle = (pos - start).astype(f32) * freq_buf[...]
    lane = lax.broadcasted_iota(jnp.int32, (block, HEAD_SIZE), 1)
    rope[0] = jnp.cos(angle)
    rope[1] = jnp.where(lane < HEAD_SIZE // 2, -jnp.sin(angle), jnp.sin(angle))
    qkv[...] = jnp.zeros_like(qkv)

    @pl.when(apart == 1)
    def _():
        own_wait(1)
        own_start(1)

    line_steps(0, 1, 2)

    @pl.when(apart == 0)
    def _():
        act_copies[1].start()
        act_copies[3].start()

    relay(0)
    line_steps(0, 2, steps)
    relay(1)
    for copy in redis_copies:
        copy.start()
    last_in = first_out - 1

    @pl.when(inner)
    def _():
        for u in range(2, first_out):
            line_steps(u - 1, 1, steps)
            own_wait(u)
            own_start(u)
        line_steps(last_in, 1, 2)

    @pl.when(jnp.logical_not(inner))
    def _():
        for u in range(2, first_out):
            own_wait(u)
            own_start(u)

    for d in range(1, reach + 1):
        @pl.when(block_id < d)
        def _():
            kv[d] = jnp.zeros_like(kv[d])

    acts_wait()

    depth = min(1024, width)

    def project(weights, cols):
        def one(k, _):
            rows = pl.ds(pl.multiple_of(k * depth, depth), depth)
            left = acts[:, :, rows].reshape(block, depth)
            qkv[:, cols] += jnp.dot(left, weights[rows, :], preferred_element_type=f32)
            return 0

        lax.fori_loop(0, width // depth, one, 0)

    def rotated(first):
        v = qkv[:, first:first + HEAD_SIZE]
        return (v * rope[0] + pltpu.roll(v, HEAD_SIZE // 2, 1) * rope[1]).astype(bf16)

    def project_query(u):
        mate_wait(u)
        first = (u - 1) * unit_cols
        project(w_q.at[u - 1], slice(first, first + unit_cols))
        for j in range(first // HEAD_SIZE, (first + unit_cols) // HEAD_SIZE):
            query[:, j * HEAD_SIZE:(j + 1) * HEAD_SIZE] = rotated(j * HEAD_SIZE)

    def kv_copy(k):
        return remote(
            kv.at[0], kv.at[2 * k], kv_send.at[2 * k], kv_recv.at[2 * k], dev(x, y, z + k, core)
        )

    kv_mate = remote(kv.at[0], kv.at[1], kv_send.at[1], kv_recv.at[1], mate)

    def kv_pass_copy(k):
        to = 2 * k + 1 - 2 * core
        return remote(kv.at[2 * k], kv.at[to], kv_pass_send.at[2 * k], kv_recv.at[to], mate)

    def kv_passes(k):
        return (z >= k) & (2 * k + 1 - 2 * core <= reach)

    def kv_each(low, high_, body):
        def one(k, _):
            body(k)
            return 0

        lax.fori_loop(low, high_, one, 0)

    def kv_start():
        @pl.when(core == 0)
        def _():
            kv_mate.start()

        def one(k):
            @pl.when(z + k < steps)
            def _():
                kv_copy(k).start()

        kv_each(1, reach // 2 + 1, one)

    def kv_wait(d):
        remote(kv.at[d], kv.at[d], kv_send.at[d], kv_recv.at[d], mate).wait_recv()

    def kv_ready():
        def even(k):
            @pl.when(z >= k)
            def _():
                kv_wait(2 * k)

            @pl.when(kv_passes(k))
            def _():
                kv_pass_copy(k).start()

        def odd(k):
            @pl.when(block_id >= 2 * k + 1)
            def _():
                kv_wait(2 * k + 1)

        kv_each(1, reach // 2 + 1, even)
        kv_each(0, reach // 2, odd)

    own_pos = lax.broadcasted_iota(jnp.int32, (block, 1), 0)
    own_start_pos = start - block_id * block
    key_lane = lax.broadcasted_iota(jnp.int32, (1, block), 1)
    scale = HEAD_SIZE ** (-0.5) * float(np.log2(np.e))

    def attend_own(u):
        def one(j, _):
            cols = pl.ds(pl.multiple_of(j * HEAD_SIZE, HEAD_SIZE), HEAD_SIZE)
            keep = (key_lane >= own_start_pos) & (key_lane <= own_pos)
            scores = lax.dot_general(
                query[:, cols], kv[0, :, :HEAD_SIZE], (((1,), (1,)), ((), ())),
                preferred_element_type=f32,
            )
            scores = jnp.where(keep, scores, masked_score)
            new = jnp.max(scores, axis=1, keepdims=True)
            probs = jnp.exp2((scores - new) * scale)
            high[j] = new
            total[j] = jnp.sum(probs, axis=1, keepdims=True)
            accum[:, cols] = jnp.dot(probs.astype(bf16), kv[0, :, HEAD_SIZE:], preferred_element_type=f32)
            return 0

        lax.fori_loop((u - 1) * unit_heads, u * unit_heads, one, 0)

    def attend_earlier(u, d):
        keep = key_lane - d * block >= own_start_pos

        def one(j, _):
            cols = pl.ds(pl.multiple_of(j * HEAD_SIZE, HEAD_SIZE), HEAD_SIZE)
            scores = lax.dot_general(
                query[:, cols], kv[d, :, :HEAD_SIZE], (((1,), (1,)), ((), ())),
                preferred_element_type=f32,
            )
            scores = jnp.where(keep, scores, masked_score)
            old = high[j]
            new = jnp.maximum(old, jnp.max(scores, axis=1, keepdims=True))
            fading = jnp.exp2((old - new) * scale)
            probs = jnp.exp2((scores - new) * scale)
            total[j] = total[j] * fading + jnp.sum(probs, axis=1, keepdims=True)
            update = jnp.dot(probs.astype(bf16), kv[d, :, HEAD_SIZE:], preferred_element_type=f32)
            accum[:, cols] = accum[:, cols] * fading + update
            high[j] = new
            return 0

        lax.fori_loop((u - 1) * unit_heads, u * unit_heads, one, 0)

    def attend_tiles(u):
        tile = block // 4

        def one(j, _):
            cols = pl.ds(pl.multiple_of(j * HEAD_SIZE, HEAD_SIZE), HEAD_SIZE)
            for i in range(4):
                rows = slice(i * tile, (i + 1) * tile)
                spans = [(0, 0, (i + 1) * tile)]
                spans += [(d, 0, block) for d in range(1, reach)]
                spans += [(reach, i * tile, block)]
                parts = []
                for d, low, high_ in spans:
                    scores = lax.dot_general(
                        query[rows, cols], kv[d, low:high_, :HEAD_SIZE], (((1,), (1,)), ((), ())),
                        preferred_element_type=f32,
                    )
                    key_pos = low - d * block + lax.broadcasted_iota(jnp.int32, (1, high_ - low), 1)
                    keep = key_pos >= own_start_pos[rows]
                    if d == 0:
                        keep = keep & (key_pos <= own_pos[rows])
                    parts.append(jnp.where(keep, scores, masked_score))
                top = functools.reduce(jnp.maximum, [jnp.max(p, axis=1, keepdims=True) for p in parts])
                probs = [jnp.exp2((p - top) * scale) for p in parts]
                denom = sum(jnp.sum(p, axis=1, keepdims=True) for p in probs)
                result = sum(
                    jnp.dot(p.astype(bf16), kv[d, low:high_, HEAD_SIZE:], preferred_element_type=f32)
                    for p, (d, low, high_) in zip(probs, spans)
                )
                mixed[group, rows, cols] = (result / denom).astype(bf16)
            return 0

        lax.fori_loop((u - 1) * unit_heads, u * unit_heads, one, 0)

    def mix_cols(u):
        return pl.ds((u - 1) * unit_cols, unit_cols)

    def mix_copy(u, x_, y_):
        ref = mixed.at[group, :, mix_cols(u)]
        return remote(ref, ref, mix_send.at[u - 1], mix_recv.at[u - 1], dev(x_, y_, z, core))

    def attend(u):
        if reach <= 2:
            attend_tiles(u)
        else:
            attend_own(u)
            finish_heads(u)
        for x_, y_ in redis_peers():
            mix_copy(u, x_, y_).start()

    def finish_heads(u):
        def one(d, _):
            @pl.when(block_id >= d)
            def _():
                attend_earlier(u, d)
            return 0

        lax.fori_loop(1, reach + 1, one, 0)
        for j in range((u - 1) * unit_heads, u * unit_heads):
            cols = slice(j * HEAD_SIZE, (j + 1) * HEAD_SIZE)
            mixed[group, :, cols] = (accum[:, cols] / total[j]).astype(bf16)

    def mix_all(u):
        ref = mixed.at[pl.ds(0, 3), :, mix_cols(u)]
        return remote(ref, ref, mix_send.at[u - 1], mix_recv.at[u - 1], mate)

    def mix_wait():
        for u in range(1, first_out):
            mix_all(u).wait_recv()

    mate_wait(0)
    project(w_kv, slice(q_cols, q_cols + w_kv.shape[1]))
    kv[0, :, :HEAD_SIZE] = rotated(q_cols)
    kv[0, :, HEAD_SIZE:] = qkv[:, q_cols + HEAD_SIZE:].astype(bf16)
    kv_start()
    for u in range(1, last_in):
        outer_steps(u, 1, steps)
    inner_steps(last_in, 2, steps)
    for u in range(1, last_in):
        project_query(u)
    own_wait(first_out)
    own_start(first_out)

    @pl.when(jnp.logical_not(inner))
    def _():
        for u in range(first_out + 1, units):
            own_start(u)

    @pl.when(inner)
    def _():
        project_query(last_in)

    kv_ready()
    for u in range(1, last_in):
        attend(u)
    outer_steps(last_in, 1, steps)

    @pl.when(jnp.logical_not(inner))
    def _():
        project_query(last_in)

    @pl.when(inner)
    def _():
        line_step(first_out, 1)
        own_start(first_out + 1)

    attend(last_in)

    @pl.when(inner)
    def _():
        line_steps(first_out, 2, steps)
        for u in range(first_out + 1, units):
            if u + 1 < units:
                own_start(u + 1)
            line_steps(u, 1, steps)

    def out_at(g, c):
        return pl.ds(pl.multiple_of(g * col_width + out_first[c], HEAD_SIZE), out_cols[c])

    def out_part(r, c):
        return osend.at[r, :, pl.ds(out_first[c], out_cols[c])]

    def out_copy(c, y_, c_):
        return remote(
            out_part(2 * y_ + c_, c), out_ref.at[:, out_at(group, c)], out_send.at[c], out_recv.at[c],
            dev(core, y_, z, c_),
        )

    def keep_result(c):
        return pltpu.make_async_copy(out_part(h, c), out_ref.at[:, out_at(group, c)], store_sem.at[c])

    def project_out(c):
        cols = slice(out_first[c], out_first[c] + out_cols[c])
        rights = []
        for g in range(heads):
            right = w_proj[g // 2, g % 2, :, :, cols]
            if right.shape[1] % 16:
                right = right.astype(f32).reshape(-1, out_cols[c]).astype(bf16)
            else:
                right = right.reshape(-1, out_cols[c])
            rights.append(right)
        for far in (1, 0):
            y_ = far * (1 - y) + (1 - far) * y
            rows = pl.ds(pl.multiple_of(y_ * 2 * own, 2 * own), 2 * own)
            result = None
            for g in range(heads):
                term = jnp.dot(mixed[g, rows, :], rights[g], preferred_element_type=f32)
                result = term if result is None else result + term
            osend[pl.ds(2 * y_, 2), :, cols] = result.astype(bf16).reshape(2, own, out_cols[c])
            if far:
                for c_ in (0, 1):
                    out_copy(c, y_, c_).start()
                continue

            @pl.when(apart == 1)
            def _():
                for c_ in (0, 1):
                    out_copy(c, y, c_).start()

            @pl.when(apart == 0)
            def _():
                out_copy(c, y, 1 - core).start()
                keep_result(c).start()

    def drain_unit(u):
        def one(row, _):
            @pl.when((row <= z) & (z < steps - 1))
            def _():
                line_copy(u, UP, row).wait_send()

            @pl.when((row >= z) & (z > 0))
            def _():
                line_copy(u, DOWN, row).wait_send()
            return 0

        lax.fori_loop(0, steps, one, 0)
        mate_all(u).wait_send()

    def act_all(i, count):
        ref = acts.at[pl.ds(0, count)]
        return remote(ref, ref, act_send.at[i], act_recv.at[0, 0], mate)

    def drain_in():
        for u in range(first_out):
            drain_unit(u)

        @pl.when(apart == 1)
        def _():
            for u in range(first_out):
                cross_copy(u).wait_send()
            act_all(1, 1).wait_send()

        act_all(0, 2).wait_send()
        redis_all().wait_send()
        for f in (0, 1):
            @pl.when(apart == 1 - f)
            def _():
                for i in (0, 1):
                    relay_copy(i, f).wait_send()

        @pl.when(core == 0)
        def _():
            kv_mate.wait_send()

        def kv_drain(k):
            @pl.when(z + k < steps)
            def _():
                kv_copy(k).wait_send()

            @pl.when(kv_passes(k))
            def _():
                kv_pass_copy(k).wait_send()

        kv_each(1, reach // 2 + 1, kv_drain)
        for u in range(1, first_out):
            mix_all(u).wait_send()

    def out_each(c, body):
        for count in (heads - 1, heads):
            @pl.when(apart == count - heads + 1)
            def _():
                ref = out_ref.at[:, pl.ds(0, count * out_cols[c])]
                body(remote(ref, ref, out_send.at[c], out_recv.at[c], mate))

    for c in range(chunks):
        outer_steps(first_out + c, 1, steps)
        mate_wait(first_out + c)
        if c == 0:
            mix_wait()
        project_out(c)
        if c == 0:
            drain_in()
    for c in range(chunks):
        drain_unit(first_out + c)
        out_each(c, lambda copy: copy.wait_send())
    for c in range(chunks):
        out_each(c, lambda copy: copy.wait_recv())

        @pl.when(apart == 0)
        def _():
            keep_result(c).wait()


def on_device(tokens, w_query, key_value_weight, w_out, doc_lengths):
    n = lax.axis_size("blk")
    heads = lax.axis_size("heads")
    assert heads == 4
    q_units, chunks = Q_UNITS, len(OUT_PARTS)
    steps = n // LINE
    own, width = tokens.shape
    block = own * heads
    rows_in, q_cols = w_query.shape
    kv_cols = 2 * key_value_weight.shape[2]
    rows_out = w_out.shape[0]
    col_width = width // heads
    out_cols = tuple(col_width * part // sum(OUT_PARTS) for part in OUT_PARTS)
    q_heads = q_cols // HEAD_SIZE
    reach = n // 4
    units = 1 + q_units + chunks
    half = HEAD_SIZE // 2
    freqs = np.power(rope_base, -2.0 * np.arange(half) / HEAD_SIZE).astype(np.float32)
    freqs = jnp.asarray(np.concatenate([freqs, freqs])[None, :])
    bf16, f32 = jnp.bfloat16, jnp.float32
    dma = pltpu.SemaphoreType.DMA
    return pl.pallas_call(
        functools.partial(layer_kernel, n, heads, out_cols, q_units),
        out_shape=jax.ShapeDtypeStruct((own, width), bf16),
        in_specs=[pl.BlockSpec(memory_space=pl.ANY)] * 4 + [
            pl.BlockSpec(memory_space=pltpu.SMEM),
            pl.BlockSpec(memory_space=pl.ANY),
        ],
        out_specs=pl.BlockSpec(memory_space=pl.ANY),
        scratch_shapes=[
            pltpu.VMEM((own, width), bf16),
            pltpu.VMEM(key_value_weight.shape, bf16),
            pltpu.VMEM((1, HEAD_SIZE), f32),
            pltpu.VMEM((n * rows_in, kv_cols), bf16),
            pltpu.VMEM((q_units, n * rows_in, q_cols // q_units), bf16),
            pltpu.VMEM((2, 2, n, rows_out, col_width), bf16),
            pltpu.VMEM((rows_in, kv_cols), bf16),
            pltpu.VMEM((own, width), bf16),
            pltpu.VMEM((heads, own, width), bf16),
            pltpu.VMEM((block, q_cols + kv_cols), f32),
            pltpu.VMEM((block, q_cols), bf16),
            pltpu.VMEM((reach + 1, block, kv_cols), bf16),
            pltpu.VMEM((q_heads, block, 1), f32),
            pltpu.VMEM((q_heads, block, 1), f32),
            pltpu.VMEM((block, q_cols), f32),
            pltpu.VMEM((heads, block, q_cols), bf16),
            pltpu.VMEM((2, block, HEAD_SIZE), f32),
            pltpu.VMEM((heads, own, col_width), bf16),
            dma((units, steps + 1)),
            dma((units,)),
            dma((units, steps)),
            dma((units,)),
            dma((1 + q_units,)),
            dma((1 + q_units,)),
            dma((3,)),
            dma((chunks,)),
            dma((1,)),
            dma((1,)),
            dma((4,)),
            dma((2, heads)),
            dma((reach + 1,)),
            dma((reach + 1,)),
            dma((reach + 1,)),
            dma((q_units,)),
            dma((q_units,)),
            dma((chunks,)),
            dma((chunks,)),
        ],
        compiler_params=pltpu.CompilerParams(
            collective_id=0, has_side_effects=True, vmem_limit_bytes=60 * 1024 * 1024
        ),
    )(tokens, w_query, key_value_weight, w_out, doc_lengths, freqs)


def solution(mesh):
    return jax.shard_map(
        on_device,
        mesh=mesh,
        in_specs=(
            P(("blk", "heads"), None),
            P("blk", "heads"),
            P("blk", None, "heads"),
            P(("heads", "blk"), None),
            P(),
        ),
        out_specs=P(("blk", "heads"), None),
        check_vma=False,
    )
```

```python
import functools

import jax
import jax.numpy as jnp
import numpy as np
from jax import lax
from jax.experimental import pallas as pl
from jax.experimental.pallas import tpu as pltpu
from jax.sharding import PartitionSpec as P

HEAD_SIZE = 128
LINE = 2
Q_UNITS = 2
OUT_PARTS = (4, 2, 2)
LEFT_PARTS = (5, 8)

norm_epsilon = 1e-05
rope_base = 500000.0
masked_score = -1e30
MESH = pl.DeviceIdType.MESH
UP, DOWN = 0, 1


def layer_kernel(
    n, heads, out_cols, q_units,
    tok_ref, w_query_ref, w_keyval_ref, w_out_ref, len_ref, freq_ref, out_ref,
    tok_buf, kv_raw, freq_buf, len_buf, w_kv, w_q, w_proj, kv_stage, act_stage, acts, qkv, query, kv, high, total, accum, mixed, rope, osend,
    line_send, mate_send, recv, mate_recv, cross_send, local_sem, load_sem, store_sem, redis_send, redis_recv,
    act_send, act_recv, kv_send, kv_recv, kv_pass_send, mix_send, mix_recv, out_send, out_recv,
):
    f32, bf16 = jnp.float32, jnp.bfloat16
    b = lax.axis_index("blk")
    h = lax.axis_index("heads")
    steps = n // LINE
    z, x = b // LINE, b % LINE
    y, core = h // 2, h % 2
    group = 2 * y + x
    block_id = LINE * z + core
    apart = (x + core) % 2
    reach = n // 4
    own, width = tok_ref.shape
    rows_in = w_query_ref.shape[0]
    block = own * heads
    q_cols = query.shape[1]
    q_heads = q_cols // HEAD_SIZE
    unit_cols = q_cols // q_units
    unit_heads = q_heads // q_units
    col_width = width // heads
    chunks = len(out_cols)
    out_first = [sum(out_cols[:c]) for c in range(chunks)]
    left = width * LEFT_PARTS[0] // LEFT_PARTS[1]
    first_out = 1 + q_units
    units = first_out + chunks

    def dev(x_, y_, z_, c_):
        return {"blk": LINE * z_ + x_, "heads": 2 * y_ + c_}

    mate = dev(x, y, z, 1 - core)

    def remote(src, dst, ss, rs, device):
        return pltpu.make_async_remote_copy(
            src_ref=src, dst_ref=dst, send_sem=ss, recv_sem=rs, device_id=device, device_id_type=MESH
        )

    barrier = pltpu.get_barrier_semaphore()
    for dx, dy, dc in [(i, j, k) for i in (0, 1) for j in (0, 1) for k in (0, 1) if i + j + k]:
        pl.semaphore_signal(
            barrier, inc=1, device_id=dev((x + dx) % 2, (y + dy) % 2, z, (core + dc) % 2), device_id_type=MESH
        )
    span = (reach + 1) // 2
    for d in range(1, span + 1):
        for c_ in (0, 1):
            @pl.when(z + d < steps)
            def _():
                pl.semaphore_signal(barrier, inc=1, device_id=dev(x, y, z + d, c_), device_id_type=MESH)

            @pl.when(z - d >= 0)
            def _():
                pl.semaphore_signal(barrier, inc=1, device_id=dev(x, y, z - d, c_), device_id_type=MESH)
    near = jnp.minimum(z, span) + jnp.minimum(steps - 1 - z, span)
    loads = [
        pltpu.make_async_copy(src, dst, load_sem.at[i])
        for i, (src, dst) in enumerate([(w_keyval_ref, kv_raw), (tok_ref, tok_buf), (freq_ref, freq_buf), (len_ref, len_buf)])
    ]
    for load in loads:
        load.start()

    def unit_ref(u, k, row):
        i = LINE * row + k
        if u == 0:
            return w_kv.at[pl.ds(pl.multiple_of(i * rows_in, rows_in), rows_in)]
        if u < first_out:
            return w_q.at[u - 1, pl.ds(pl.multiple_of(i * rows_in, rows_in), rows_in)]
        return w_proj.at[:, k, pl.ds(LINE * row, LINE), :, pl.ds(out_first[u - first_out], out_cols[u - first_out])]

    def line_copy(u, direction, row):
        ref = unit_ref(u, core, row)
        z_ = z + 1 if direction == UP else z - 1
        at = row
        if direction == DOWN:
            at = jnp.where(row == z, steps, row)
        return remote(ref, ref, line_send.at[u, at], recv.at[u, row], dev(x, y, z_, core))

    def mate_copy(u, row):
        ref = unit_ref(u, core, row)
        return remote(ref, ref, mate_send.at[u], mate_recv.at[u], mate)

    def mate_all(u):
        if u == 0:
            ref = w_kv.at[pl.ds(0, steps * rows_in)]
        elif u < first_out:
            ref = w_q.at[u - 1, pl.ds(0, steps * rows_in)]
        else:
            ref = w_proj.at[:, 0, :, :, pl.ds(out_first[u - first_out], out_cols[u - first_out])]
        return remote(ref, ref, mate_send.at[u], mate_recv.at[u], mate)

    def arrive(u, row):
        ref = unit_ref(u, core, row)
        remote(ref, ref, mate_send.at[u], recv.at[u, row], mate).wait_recv()

    def query_cols(u):
        return w_query_ref.at[:, pl.ds((u - 1) * unit_cols, unit_cols)]

    def cross_copy(u):
        src = kv_stage if u == 0 else query_cols(u)
        return remote(src, unit_ref(u, x, z), cross_send.at[u], recv.at[u, z], dev(1 - x, y, z, 1 - core))

    def keep_query(u):
        return pltpu.make_async_copy(query_cols(u), unit_ref(u, core, z), local_sem.at[u])

    def own_start(u):
        @pl.when(z < steps - 1)
        def _():
            line_copy(u, UP, z).start()

        @pl.when(z > 0)
        def _():
            line_copy(u, DOWN, z).start()

        mate_copy(u, z).start()

    def redis_peers():
        return [(1 - x, y), (x, 1 - y), (1 - x, 1 - y)]

    def redis_copy(x_, y_):
        cols = pl.ds(pl.multiple_of((2 * y_ + x_) * col_width, col_width), col_width)
        return remote(
            w_out_ref.at[:, cols], w_proj.at[y, core, b], redis_send.at[0], redis_recv.at[0],
            dev(x_, y_, z, core),
        )

    def redis_all():
        ref = w_proj.at[0, 0, pl.ds(0, 3)]
        return remote(ref, ref, redis_send.at[0], redis_recv.at[0], mate)

    def keep_out():
        cols = pl.ds(pl.multiple_of(group * col_width, col_width), col_width)
        return pltpu.make_async_copy(w_out_ref.at[:, cols], w_proj.at[y, core, b], local_sem.at[0])

    def own_wait(u):
        if u == 0:
            @pl.when(apart == 1)
            def _():
                arrive(u, z)
        elif u < first_out:
            @pl.when(apart == 1)
            def _():
                arrive(u, z)

            @pl.when(apart == 0)
            def _():
                keep_query(u).wait()
        elif u == first_out:
            keep_out().wait()
            redis_all().wait_recv()

    def line_step(u, s):
        @pl.when(z - s >= 0)
        def _():
            arrive(u, z - s)

            @pl.when(z < steps - 1)
            def _():
                line_copy(u, UP, z - s).start()

            mate_copy(u, z - s).start()

        @pl.when(z + s <= steps - 1)
        def _():
            arrive(u, z + s)

            @pl.when(z > 0)
            def _():
                line_copy(u, DOWN, z + s).start()

            mate_copy(u, z + s).start()

    def line_steps(u, low, high_):
        def one(s, _):
            line_step(u, s)
            return 0

        lax.fori_loop(low, high_, one, 0)

    inner = (z > 0) & (z < steps - 1)

    def inner_steps(u, low, high_):
        @pl.when(inner)
        def _():
            line_steps(u, low, high_)

    def outer_steps(u, low, high_):
        @pl.when(jnp.logical_not(inner))
        def _():
            line_steps(u, low, high_)

    def mate_wait(u):
        mate_all(u).wait_recv()

    @pl.when(apart == 0)
    def _():
        for u in range(1, first_out):
            keep_query(u).start()

    keep_out().start()
    loads[0].wait()
    own_kv = kv_raw[...].reshape(rows_in, w_kv.shape[1])

    @pl.when(apart == 0)
    def _():
        w_kv[pl.ds(pl.multiple_of(b * rows_in, rows_in), rows_in), :] = own_kv

    @pl.when(apart == 1)
    def _():
        kv_stage[...] = own_kv

    pl.semaphore_wait(barrier, 7 + 2 * near)

    @pl.when(apart == 0)
    def _():
        own_start(0)
        own_wait(1)
        own_start(1)

    @pl.when(apart == 1)
    def _():
        for u in range(2):
            cross_copy(u).start()

    loads[1].wait()
    values = tok_buf[...].astype(f32)
    normed = (
        values * lax.rsqrt(jnp.mean(values * values, axis=1, keepdims=True) + norm_epsilon)
    ).astype(bf16)
    act_stage[...] = normed

    @pl.when(apart == 0)
    def _():
        acts[h] = normed

    act_cols = [(0, left), (left, width - left)]

    def act_ref(h_, f):
        return acts.at[h_, :, pl.ds(*act_cols[f])]

    def act_copy(i, h_, f, device, src=None):
        src = act_ref(h_, f) if src is None else src
        return remote(src, act_ref(h_, f), act_send.at[i], act_recv.at[f, h_], device)

    def act_own(i, f, device):
        return act_copy(i, h, f, device, act_stage.at[:, pl.ds(*act_cols[f])])

    def act_wait(h_, f):
        remote(act_ref(h_, f), act_ref(h_, f), act_send.at[0], act_recv.at[f, h_], mate).wait_recv()

    act_copies = [
        act_own(0, 1, dev(x, 1 - y, z, x)),
        act_own(0, 0, dev(1 - x, y, z, x)),
        act_own(0, 0, dev(x, 1 - y, z, x)),
        act_own(0, 1, dev(1 - x, y, z, x)),
    ]
    act_mate = [act_own(1, f, mate) for f in (0, 1)]
    act_copies[0].start()
    act_copies[2].start()

    @pl.when(apart == 1)
    def _():
        act_copies[1].start()
        for u in range(2, first_out):
            cross_copy(u).start()
        for copy in act_mate:
            copy.start()
        act_copies[3].start()

    redis_copies = [redis_copy(x_, y_) for x_, y_ in redis_peers()]

    relay_y = apart * y + (1 - apart) * (1 - y)

    def relay_copy(i, f):
        c = core if i == 0 else 1 - core
        to = dev(x, 1 - y, z, core) if f == 0 else dev(1 - x, y, z, core)
        return act_copy(2 + i, 2 * relay_y + c, f, to)

    def relay(i):
        for f in (0, 1):
            @pl.when(apart == 1 - f)
            def _():
                act_wait(2 * relay_y + (core if i == 0 else 1 - core), f)
                relay_copy(i, f).start()

    def acts_wait():
        for h_ in range(heads):
            for f in (0, 1):
                mine = (apart == 0) & (h == h_)
                relayed = (apart == 1 - f) & (relay_y == h_ // 2)

                @pl.when(jnp.logical_not(mine | relayed))
                def _():
                    act_wait(h_, f)

    @pl.when(apart == 1)
    def _():
        own_wait(0)
        own_start(0)

    loads[2].wait()
    loads[3].wait()
    pos = block_id * block + lax.broadcasted_iota(jnp.int32, (block, 1), 0)
    start = jnp.zeros((block, 1), jnp.int32)
    end = jnp.int32(0)
    for i in range(len_ref.shape[0]):
        size = len_buf[i]
        end = end + size
        start = start + jnp.where(pos >= end, size, 0)
    angle = (pos - start).astype(f32) * freq_buf[...]
    lane = lax.broadcasted_iota(jnp.int32, (block, HEAD_SIZE), 1)
    rope[0] = jnp.cos(angle)
    rope[1] = jnp.where(lane < HEAD_SIZE // 2, -jnp.sin(angle), jnp.sin(angle))
    qkv[...] = jnp.zeros_like(qkv)

    @pl.when(apart == 1)
    def _():
        own_wait(1)
        own_start(1)

    line_steps(0, 1, 2)

    @pl.when(apart == 0)
    def _():
        act_copies[1].start()
        act_copies[3].start()

    relay(0)
    line_steps(0, 2, steps)
    relay(1)
    for copy in redis_copies:
        copy.start()
    last_in = first_out - 1

    @pl.when(inner)
    def _():
        for u in range(2, first_out):
            line_steps(u - 1, 1, steps)
            own_wait(u)
            own_start(u)
        line_steps(last_in, 1, 2)

    @pl.when(jnp.logical_not(inner))
    def _():
        for u in range(2, first_out):
            own_wait(u)
            own_start(u)

    for d in range(1, reach + 1):
        @pl.when(block_id < d)
        def _():
            kv[d] = jnp.zeros_like(kv[d])

    acts_wait()

    depth = min(1024, width)

    def project(weights, cols):
        def one(k, _):
            rows = pl.ds(pl.multiple_of(k * depth, depth), depth)
            left = acts[:, :, rows].reshape(block, depth)
            qkv[:, cols] += jnp.dot(left, weights[rows, :], preferred_element_type=f32)
            return 0

        lax.fori_loop(0, width // depth, one, 0)

    def rotated(first):
        v = qkv[:, first:first + HEAD_SIZE]
        return (v * rope[0] + pltpu.roll(v, HEAD_SIZE // 2, 1) * rope[1]).astype(bf16)

    def project_query(u):
        mate_wait(u)
        first = (u - 1) * unit_cols
        project(w_q.at[u - 1], slice(first, first + unit_cols))
        for j in range(first // HEAD_SIZE, (first + unit_cols) // HEAD_SIZE):
            query[:, j * HEAD_SIZE:(j + 1) * HEAD_SIZE] = rotated(j * HEAD_SIZE)

    def kv_copy(k):
        return remote(
            kv.at[0], kv.at[2 * k], kv_send.at[2 * k], kv_recv.at[2 * k], dev(x, y, z + k, core)
        )

    kv_mate = remote(kv.at[0], kv.at[1], kv_send.at[1], kv_recv.at[1], mate)

    def kv_pass_copy(k):
        to = 2 * k + 1 - 2 * core
        return remote(kv.at[2 * k], kv.at[to], kv_pass_send.at[2 * k], kv_recv.at[to], mate)

    def kv_passes(k):
        return (z >= k) & (2 * k + 1 - 2 * core <= reach)

    def kv_each(low, high_, body):
        def one(k, _):
            body(k)
            return 0

        lax.fori_loop(low, high_, one, 0)

    def kv_start():
        @pl.when(core == 0)
        def _():
            kv_mate.start()

        def one(k):
            @pl.when(z + k < steps)
            def _():
                kv_copy(k).start()

        kv_each(1, reach // 2 + 1, one)

    def kv_wait(d):
        remote(kv.at[d], kv.at[d], kv_send.at[d], kv_recv.at[d], mate).wait_recv()

    def kv_ready():
        def even(k):
            @pl.when(z >= k)
            def _():
                kv_wait(2 * k)

            @pl.when(kv_passes(k))
            def _():
                kv_pass_copy(k).start()

        def odd(k):
            @pl.when(block_id >= 2 * k + 1)
            def _():
                kv_wait(2 * k + 1)

        kv_each(1, reach // 2 + 1, even)
        kv_each(0, reach // 2, odd)

    own_pos = lax.broadcasted_iota(jnp.int32, (block, 1), 0)
    own_start_pos = start - block_id * block
    key_lane = lax.broadcasted_iota(jnp.int32, (1, block), 1)
    scale = HEAD_SIZE ** (-0.5) * float(np.log2(np.e))

    def attend_own(u):
        def one(j, _):
            cols = pl.ds(pl.multiple_of(j * HEAD_SIZE, HEAD_SIZE), HEAD_SIZE)
            keep = (key_lane >= own_start_pos) & (key_lane <= own_pos)
            scores = lax.dot_general(
                query[:, cols], kv[0, :, :HEAD_SIZE], (((1,), (1,)), ((), ())),
                preferred_element_type=f32,
            )
            scores = jnp.where(keep, scores, masked_score)
            new = jnp.max(scores, axis=1, keepdims=True)
            probs = jnp.exp2((scores - new) * scale)
            high[j] = new
            total[j] = jnp.sum(probs, axis=1, keepdims=True)
            accum[:, cols] = jnp.dot(probs.astype(bf16), kv[0, :, HEAD_SIZE:], preferred_element_type=f32)
            return 0

        lax.fori_loop((u - 1) * unit_heads, u * unit_heads, one, 0)

    def attend_earlier(u, d):
        keep = key_lane - d * block >= own_start_pos

        def one(j, _):
            cols = pl.ds(pl.multiple_of(j * HEAD_SIZE, HEAD_SIZE), HEAD_SIZE)
            scores = lax.dot_general(
                query[:, cols], kv[d, :, :HEAD_SIZE], (((1,), (1,)), ((), ())),
                preferred_element_type=f32,
            )
            scores = jnp.where(keep, scores, masked_score)
            old = high[j]
            new = jnp.maximum(old, jnp.max(scores, axis=1, keepdims=True))
            fading = jnp.exp2((old - new) * scale)
            probs = jnp.exp2((scores - new) * scale)
            total[j] = total[j] * fading + jnp.sum(probs, axis=1, keepdims=True)
            update = jnp.dot(probs.astype(bf16), kv[d, :, HEAD_SIZE:], preferred_element_type=f32)
            accum[:, cols] = accum[:, cols] * fading + update
            high[j] = new
            return 0

        lax.fori_loop((u - 1) * unit_heads, u * unit_heads, one, 0)

    def attend_tiles(u):
        tile = block // 4

        def one(j, _):
            cols = pl.ds(pl.multiple_of(j * HEAD_SIZE, HEAD_SIZE), HEAD_SIZE)
            for i in range(4):
                rows = slice(i * tile, (i + 1) * tile)
                spans = [(0, 0, (i + 1) * tile)]
                spans += [(d, 0, block) for d in range(1, reach)]
                spans += [(reach, i * tile, block)]
                parts = []
                for d, low, high_ in spans:
                    scores = lax.dot_general(
                        query[rows, cols], kv[d, low:high_, :HEAD_SIZE], (((1,), (1,)), ((), ())),
                        preferred_element_type=f32,
                    )
                    key_pos = low - d * block + lax.broadcasted_iota(jnp.int32, (1, high_ - low), 1)
                    keep = key_pos >= own_start_pos[rows]
                    if d == 0:
                        keep = keep & (key_pos <= own_pos[rows])
                    parts.append(jnp.where(keep, scores, masked_score))
                top = functools.reduce(jnp.maximum, [jnp.max(p, axis=1, keepdims=True) for p in parts])
                probs = [jnp.exp2((p - top) * scale) for p in parts]
                denom = sum(jnp.sum(p, axis=1, keepdims=True) for p in probs)
                result = sum(
                    jnp.dot(p.astype(bf16), kv[d, low:high_, HEAD_SIZE:], preferred_element_type=f32)
                    for p, (d, low, high_) in zip(probs, spans)
                )
                mixed[group, rows, cols] = (result / denom).astype(bf16)
            return 0

        lax.fori_loop((u - 1) * unit_heads, u * unit_heads, one, 0)

    def mix_cols(u):
        return pl.ds((u - 1) * unit_cols, unit_cols)

    def mix_copy(u, x_, y_):
        ref = mixed.at[group, :, mix_cols(u)]
        return remote(ref, ref, mix_send.at[u - 1], mix_recv.at[u - 1], dev(x_, y_, z, core))

    def attend(u):
        if reach <= 2:
            attend_tiles(u)
        else:
            attend_own(u)
            finish_heads(u)
        for x_, y_ in redis_peers():
            mix_copy(u, x_, y_).start()

    def finish_heads(u):
        def one(d, _):
            @pl.when(block_id >= d)
            def _():
                attend_earlier(u, d)
            return 0

        lax.fori_loop(1, reach + 1, one, 0)
        for j in range((u - 1) * unit_heads, u * unit_heads):
            cols = slice(j * HEAD_SIZE, (j + 1) * HEAD_SIZE)
            mixed[group, :, cols] = (accum[:, cols] / total[j]).astype(bf16)

    def mix_all(u):
        ref = mixed.at[pl.ds(0, 3), :, mix_cols(u)]
        return remote(ref, ref, mix_send.at[u - 1], mix_recv.at[u - 1], mate)

    def mix_wait():
        for u in range(1, first_out):
            mix_all(u).wait_recv()

    mate_wait(0)
    project(w_kv, slice(q_cols, q_cols + w_kv.shape[1]))
    kv[0, :, :HEAD_SIZE] = rotated(q_cols)
    kv[0, :, HEAD_SIZE:] = qkv[:, q_cols + HEAD_SIZE:].astype(bf16)
    kv_start()
    for u in range(1, last_in):
        outer_steps(u, 1, steps)
    inner_steps(last_in, 2, steps)
    for u in range(1, last_in):
        project_query(u)
    own_wait(first_out)
    own_start(first_out)

    @pl.when(jnp.logical_not(inner))
    def _():
        for u in range(first_out + 1, units):
            own_start(u)

    @pl.when(inner)
    def _():
        project_query(last_in)

    kv_ready()
    for u in range(1, last_in):
        attend(u)
    outer_steps(last_in, 1, steps)

    @pl.when(jnp.logical_not(inner))
    def _():
        project_query(last_in)

    @pl.when(inner)
    def _():
        line_step(first_out, 1)
        own_start(first_out + 1)

    attend(last_in)

    @pl.when(inner)
    def _():
        line_steps(first_out, 2, steps)
        for u in range(first_out + 1, units):
            if u + 1 < units:
                own_start(u + 1)
            line_steps(u, 1, steps)

    def out_at(g, c):
        return pl.ds(pl.multiple_of(g * col_width + out_first[c], HEAD_SIZE), out_cols[c])

    def out_part(r, c):
        return osend.at[r, :, pl.ds(out_first[c], out_cols[c])]

    def out_copy(c, y_, c_):
        return remote(
            out_part(2 * y_ + c_, c), out_ref.at[:, out_at(group, c)], out_send.at[c], out_recv.at[c],
            dev(core, y_, z, c_),
        )

    def keep_result(c):
        return pltpu.make_async_copy(out_part(h, c), out_ref.at[:, out_at(group, c)], store_sem.at[c])

    def project_out(c):
        cols = slice(out_first[c], out_first[c] + out_cols[c])
        rights = []
        for g in range(heads):
            right = w_proj[g // 2, g % 2, :, :, cols]
            if right.shape[1] % 16:
                right = right.astype(f32).reshape(-1, out_cols[c]).astype(bf16)
            else:
                right = right.reshape(-1, out_cols[c])
            rights.append(right)
        for far in (1, 0):
            y_ = far * (1 - y) + (1 - far) * y
            rows = pl.ds(pl.multiple_of(y_ * 2 * own, 2 * own), 2 * own)
            result = None
            for g in range(heads):
                term = jnp.dot(mixed[g, rows, :], rights[g], preferred_element_type=f32)
                result = term if result is None else result + term
            osend[pl.ds(2 * y_, 2), :, cols] = result.astype(bf16).reshape(2, own, out_cols[c])
            if far:
                for c_ in (0, 1):
                    out_copy(c, y_, c_).start()
                continue

            @pl.when(apart == 1)
            def _():
                for c_ in (0, 1):
                    out_copy(c, y, c_).start()

            @pl.when(apart == 0)
            def _():
                out_copy(c, y, 1 - core).start()
                keep_result(c).start()

    def drain_unit(u):
        def one(row, _):
            @pl.when((row <= z) & (z < steps - 1))
            def _():
                line_copy(u, UP, row).wait_send()

            @pl.when((row >= z) & (z > 0))
            def _():
                line_copy(u, DOWN, row).wait_send()
            return 0

        lax.fori_loop(0, steps, one, 0)
        mate_all(u).wait_send()

    def act_all(i, count):
        ref = acts.at[pl.ds(0, count)]
        return remote(ref, ref, act_send.at[i], act_recv.at[0, 0], mate)

    def drain_in():
        for u in range(first_out):
            drain_unit(u)

        @pl.when(apart == 1)
        def _():
            for u in range(first_out):
                cross_copy(u).wait_send()
            act_all(1, 1).wait_send()

        act_all(0, 2).wait_send()
        redis_all().wait_send()
        for f in (0, 1):
            @pl.when(apart == 1 - f)
            def _():
                for i in (0, 1):
                    relay_copy(i, f).wait_send()

        @pl.when(core == 0)
        def _():
            kv_mate.wait_send()

        def kv_drain(k):
            @pl.when(z + k < steps)
            def _():
                kv_copy(k).wait_send()

            @pl.when(kv_passes(k))
            def _():
                kv_pass_copy(k).wait_send()

        kv_each(1, reach // 2 + 1, kv_drain)
        for u in range(1, first_out):
            mix_all(u).wait_send()

    def out_each(c, body):
        for count in (heads - 1, heads):
            @pl.when(apart == count - heads + 1)
            def _():
                ref = out_ref.at[:, pl.ds(0, count * out_cols[c])]
                body(remote(ref, ref, out_send.at[c], out_recv.at[c], mate))

    for c in range(chunks):
        outer_steps(first_out + c, 1, steps)
        mate_wait(first_out + c)
        if c == 0:
            mix_wait()
        project_out(c)
        if c == 0:
            drain_in()
    for c in range(chunks):
        drain_unit(first_out + c)
        out_each(c, lambda copy: copy.wait_send())
    for c in range(chunks):
        out_each(c, lambda copy: copy.wait_recv())

        @pl.when(apart == 0)
        def _():
            keep_result(c).wait()


def on_device(tokens, w_query, key_value_weight, w_out, doc_lengths):
    n = lax.axis_size("blk")
    heads = lax.axis_size("heads")
    assert heads == 4
    q_units, chunks = Q_UNITS, len(OUT_PARTS)
    steps = n // LINE
    own, width = tokens.shape
    block = own * heads
    rows_in, q_cols = w_query.shape
    kv_cols = 2 * key_value_weight.shape[2]
    rows_out = w_out.shape[0]
    col_width = width // heads
    out_cols = tuple(col_width * part // sum(OUT_PARTS) for part in OUT_PARTS)
    q_heads = q_cols // HEAD_SIZE
    reach = n // 4
    units = 1 + q_units + chunks
    half = HEAD_SIZE // 2
    freqs = np.power(rope_base, -2.0 * np.arange(half) / HEAD_SIZE).astype(np.float32)
    freqs = jnp.asarray(np.concatenate([freqs, freqs])[None, :])
    bf16, f32 = jnp.bfloat16, jnp.float32
    dma = pltpu.SemaphoreType.DMA
    return pl.pallas_call(
        functools.partial(layer_kernel, n, heads, out_cols, q_units),
        out_shape=jax.ShapeDtypeStruct((own, width), bf16),
        in_specs=[pl.BlockSpec(memory_space=pl.ANY)] * 6,
        out_specs=pl.BlockSpec(memory_space=pl.ANY),
        scratch_shapes=[
            pltpu.VMEM((own, width), bf16),
            pltpu.VMEM(key_value_weight.shape, bf16),
            pltpu.VMEM((1, HEAD_SIZE), f32),
            pltpu.SMEM(doc_lengths.shape, jnp.int32),
            pltpu.VMEM((n * rows_in, kv_cols), bf16),
            pltpu.VMEM((q_units, n * rows_in, q_cols // q_units), bf16),
            pltpu.VMEM((2, 2, n, rows_out, col_width), bf16),
            pltpu.VMEM((rows_in, kv_cols), bf16),
            pltpu.VMEM((own, width), bf16),
            pltpu.VMEM((heads, own, width), bf16),
            pltpu.VMEM((block, q_cols + kv_cols), f32),
            pltpu.VMEM((block, q_cols), bf16),
            pltpu.VMEM((reach + 1, block, kv_cols), bf16),
            pltpu.VMEM((q_heads, block, 1), f32),
            pltpu.VMEM((q_heads, block, 1), f32),
            pltpu.VMEM((block, q_cols), f32),
            pltpu.VMEM((heads, block, q_cols), bf16),
            pltpu.VMEM((2, block, HEAD_SIZE), f32),
            pltpu.VMEM((heads, own, col_width), bf16),
            dma((units, steps + 1)),
            dma((units,)),
            dma((units, steps)),
            dma((units,)),
            dma((1 + q_units,)),
            dma((1 + q_units,)),
            dma((4,)),
            dma((chunks,)),
            dma((1,)),
            dma((1,)),
            dma((4,)),
            dma((2, heads)),
            dma((reach + 1,)),
            dma((reach + 1,)),
            dma((reach + 1,)),
            dma((q_units,)),
            dma((q_units,)),
            dma((chunks,)),
            dma((chunks,)),
        ],
        compiler_params=pltpu.CompilerParams(
            collective_id=0, has_side_effects=True, vmem_limit_bytes=60 * 1024 * 1024
        ),
    )(tokens, w_query, key_value_weight, w_out, doc_lengths, freqs)


def solution(mesh):
    return jax.shard_map(
        on_device,
        mesh=mesh,
        in_specs=(
            P(("blk", "heads"), None),
            P("blk", "heads"),
            P("blk", None, "heads"),
            P(("heads", "blk"), None),
            P(),
        ),
        out_specs=P(("blk", "heads"), None),
        check_vma=False,
    )
```

```python
import functools

import jax
import jax.numpy as jnp
import numpy as np
from jax import lax
from jax.experimental import pallas as pl
from jax.experimental.pallas import tpu as pltpu
from jax.sharding import PartitionSpec as P

HEAD_SIZE = 128
LINE = 2
Q_UNITS = 2
OUT_PARTS = (4, 2, 2)
LEFT_PARTS = (5, 8)

norm_epsilon = 1e-05
rope_base = 500000.0
masked_score = -1e30
MESH = pl.DeviceIdType.MESH
UP, DOWN = 0, 1


def layer_kernel(
    n, heads, out_cols, q_units,
    tok_ref, w_query_ref, w_keyval_ref, w_out_ref, len_ref, freq_ref, out_ref,
    tok_buf, kv_raw, freq_buf, len_buf, w_kv, w_q, w_proj, kv_stage, act_stage, acts, qkv, query, kv, high, total, accum, mixed, rope, osend,
    line_send, mate_send, recv, mate_recv, cross_send, local_sem, load_sem, store_sem, redis_send, redis_recv,
    act_send, act_recv, kv_send, kv_recv, kv_pass_send, mix_send, mix_recv, out_send, out_recv,
):
    f32, bf16 = jnp.float32, jnp.bfloat16
    b = lax.axis_index("blk")
    h = lax.axis_index("heads")
    steps = n // LINE
    z, x = b // LINE, b % LINE
    y, core = h // 2, h % 2
    group = 2 * y + x
    block_id = LINE * z + core
    apart = (x + core) % 2
    reach = n // 4
    own, width = tok_ref.shape
    rows_in = w_query_ref.shape[0]
    block = own * heads
    q_cols = query.shape[1]
    q_heads = q_cols // HEAD_SIZE
    unit_cols = q_cols // q_units
    unit_heads = q_heads // q_units
    col_width = width // heads
    chunks = len(out_cols)
    out_first = [sum(out_cols[:c]) for c in range(chunks)]
    left = width * LEFT_PARTS[0] // LEFT_PARTS[1]
    first_out = 1 + q_units
    units = first_out + chunks

    def dev(x_, y_, z_, c_):
        return {"blk": LINE * z_ + x_, "heads": 2 * y_ + c_}

    mate = dev(x, y, z, 1 - core)

    def remote(src, dst, ss, rs, device):
        return pltpu.make_async_remote_copy(
            src_ref=src, dst_ref=dst, send_sem=ss, recv_sem=rs, device_id=device, device_id_type=MESH
        )

    barrier = pltpu.get_barrier_semaphore()
    for dx, dy, dc in [(i, j, k) for i in (0, 1) for j in (0, 1) for k in (0, 1) if i + j + k]:
        pl.semaphore_signal(
            barrier, inc=1, device_id=dev((x + dx) % 2, (y + dy) % 2, z, (core + dc) % 2), device_id_type=MESH
        )
    span = max(reach // 2, 1)
    for d in range(1, span + 1):
        @pl.when(z + d < steps)
        def _():
            pl.semaphore_signal(barrier, inc=1, device_id=dev(x, y, z + d, core), device_id_type=MESH)

        @pl.when(z - d >= 0)
        def _():
            pl.semaphore_signal(barrier, inc=1, device_id=dev(x, y, z - d, core), device_id_type=MESH)
    near = jnp.minimum(z, span) + jnp.minimum(steps - 1 - z, span)
    loads = [
        pltpu.make_async_copy(src, dst, load_sem.at[i])
        for i, (src, dst) in enumerate([(w_keyval_ref, kv_raw), (tok_ref, tok_buf), (freq_ref, freq_buf), (len_ref, len_buf)])
    ]
    for load in loads:
        load.start()

    def unit_ref(u, k, row):
        i = LINE * row + k
        if u == 0:
            return w_kv.at[pl.ds(pl.multiple_of(i * rows_in, rows_in), rows_in)]
        if u < first_out:
            return w_q.at[u - 1, pl.ds(pl.multiple_of(i * rows_in, rows_in), rows_in)]
        return w_proj.at[:, k, pl.ds(LINE * row, LINE), :, pl.ds(out_first[u - first_out], out_cols[u - first_out])]

    def line_copy(u, direction, row):
        ref = unit_ref(u, core, row)
        z_ = z + 1 if direction == UP else z - 1
        at = row
        if direction == DOWN:
            at = jnp.where(row == z, steps, row)
        return remote(ref, ref, line_send.at[u, at], recv.at[u, row], dev(x, y, z_, core))

    def mate_copy(u, row):
        ref = unit_ref(u, core, row)
        return remote(ref, ref, mate_send.at[u], mate_recv.at[u], mate)

    def mate_all(u):
        if u == 0:
            ref = w_kv.at[pl.ds(0, steps * rows_in)]
        elif u < first_out:
            ref = w_q.at[u - 1, pl.ds(0, steps * rows_in)]
        else:
            ref = w_proj.at[:, 0, :, :, pl.ds(out_first[u - first_out], out_cols[u - first_out])]
        return remote(ref, ref, mate_send.at[u], mate_recv.at[u], mate)

    def arrive(u, row):
        ref = unit_ref(u, core, row)
        remote(ref, ref, mate_send.at[u], recv.at[u, row], mate).wait_recv()

    def query_cols(u):
        return w_query_ref.at[:, pl.ds((u - 1) * unit_cols, unit_cols)]

    def cross_copy(u):
        src = kv_stage if u == 0 else query_cols(u)
        return remote(src, unit_ref(u, x, z), cross_send.at[u], recv.at[u, z], dev(1 - x, y, z, 1 - core))

    def keep_query(u):
        return pltpu.make_async_copy(query_cols(u), unit_ref(u, core, z), local_sem.at[u])

    def own_start(u):
        @pl.when(z < steps - 1)
        def _():
            line_copy(u, UP, z).start()

        @pl.when(z > 0)
        def _():
            line_copy(u, DOWN, z).start()

        mate_copy(u, z).start()

    def redis_peers():
        return [(1 - x, y), (x, 1 - y), (1 - x, 1 - y)]

    def redis_copy(x_, y_):
        cols = pl.ds(pl.multiple_of((2 * y_ + x_) * col_width, col_width), col_width)
        return remote(
            w_out_ref.at[:, cols], w_proj.at[y, core, b], redis_send.at[0], redis_recv.at[0],
            dev(x_, y_, z, core),
        )

    def redis_all():
        ref = w_proj.at[0, 0, pl.ds(0, 3)]
        return remote(ref, ref, redis_send.at[0], redis_recv.at[0], mate)

    def keep_out():
        cols = pl.ds(pl.multiple_of(group * col_width, col_width), col_width)
        return pltpu.make_async_copy(w_out_ref.at[:, cols], w_proj.at[y, core, b], local_sem.at[0])

    def own_wait(u):
        if u == 0:
            @pl.when(apart == 1)
            def _():
                arrive(u, z)
        elif u < first_out:
            @pl.when(apart == 1)
            def _():
                arrive(u, z)

            @pl.when(apart == 0)
            def _():
                keep_query(u).wait()
        elif u == first_out:
            keep_out().wait()
            redis_all().wait_recv()

    def line_step(u, s):
        @pl.when(z - s >= 0)
        def _():
            arrive(u, z - s)

            @pl.when(z < steps - 1)
            def _():
                line_copy(u, UP, z - s).start()

            mate_copy(u, z - s).start()

        @pl.when(z + s <= steps - 1)
        def _():
            arrive(u, z + s)

            @pl.when(z > 0)
            def _():
                line_copy(u, DOWN, z + s).start()

            mate_copy(u, z + s).start()

    def line_steps(u, low, high_):
        def one(s, _):
            line_step(u, s)
            return 0

        lax.fori_loop(low, high_, one, 0)

    inner = (z > 0) & (z < steps - 1)

    def inner_steps(u, low, high_):
        @pl.when(inner)
        def _():
            line_steps(u, low, high_)

    def outer_steps(u, low, high_):
        @pl.when(jnp.logical_not(inner))
        def _():
            line_steps(u, low, high_)

    def mate_wait(u):
        mate_all(u).wait_recv()

    @pl.when(apart == 0)
    def _():
        for u in range(1, first_out):
            keep_query(u).start()

    keep_out().start()
    loads[0].wait()
    own_kv = kv_raw[...].reshape(rows_in, w_kv.shape[1])

    @pl.when(apart == 0)
    def _():
        w_kv[pl.ds(pl.multiple_of(b * rows_in, rows_in), rows_in), :] = own_kv

    @pl.when(apart == 1)
    def _():
        kv_stage[...] = own_kv

    pl.semaphore_wait(barrier, 7 + near)

    @pl.when(apart == 0)
    def _():
        own_start(0)
        own_wait(1)
        own_start(1)

    @pl.when(apart == 1)
    def _():
        for u in range(2):
            cross_copy(u).start()

    loads[1].wait()
    values = tok_buf[...].astype(f32)
    normed = (
        values * lax.rsqrt(jnp.mean(values * values, axis=1, keepdims=True) + norm_epsilon)
    ).astype(bf16)
    act_stage[...] = normed

    @pl.when(apart == 0)
    def _():
        acts[h] = normed

    act_cols = [(0, left), (left, width - left)]

    def act_ref(h_, f):
        return acts.at[h_, :, pl.ds(*act_cols[f])]

    def act_copy(i, h_, f, device, src=None):
        src = act_ref(h_, f) if src is None else src
        return remote(src, act_ref(h_, f), act_send.at[i], act_recv.at[f, h_], device)

    def act_own(i, f, device):
        return act_copy(i, h, f, device, act_stage.at[:, pl.ds(*act_cols[f])])

    def act_wait(h_, f):
        remote(act_ref(h_, f), act_ref(h_, f), act_send.at[0], act_recv.at[f, h_], mate).wait_recv()

    act_copies = [
        act_own(0, 1, dev(x, 1 - y, z, x)),
        act_own(0, 0, dev(1 - x, y, z, x)),
        act_own(0, 0, dev(x, 1 - y, z, x)),
        act_own(0, 1, dev(1 - x, y, z, x)),
    ]
    act_mate = [act_own(1, f, mate) for f in (0, 1)]
    act_copies[0].start()
    act_copies[2].start()

    @pl.when(apart == 1)
    def _():
        act_copies[1].start()
        for u in range(2, first_out):
            cross_copy(u).start()
        for copy in act_mate:
            copy.start()
        act_copies[3].start()

    redis_copies = [redis_copy(x_, y_) for x_, y_ in redis_peers()]

    relay_y = apart * y + (1 - apart) * (1 - y)

    def relay_copy(i, f):
        c = core if i == 0 else 1 - core
        to = dev(x, 1 - y, z, core) if f == 0 else dev(1 - x, y, z, core)
        return act_copy(2 + i, 2 * relay_y + c, f, to)

    def relay(i):
        for f in (0, 1):
            @pl.when(apart == 1 - f)
            def _():
                act_wait(2 * relay_y + (core if i == 0 else 1 - core), f)
                relay_copy(i, f).start()

    def acts_wait():
        for h_ in range(heads):
            for f in (0, 1):
                mine = (apart == 0) & (h == h_)
                relayed = (apart == 1 - f) & (relay_y == h_ // 2)

                @pl.when(jnp.logical_not(mine | relayed))
                def _():
                    act_wait(h_, f)

    @pl.when(apart == 1)
    def _():
        own_wait(0)
        own_start(0)

    loads[2].wait()
    loads[3].wait()
    pos = block_id * block + lax.broadcasted_iota(jnp.int32, (block, 1), 0)
    start = jnp.zeros((block, 1), jnp.int32)
    end = jnp.int32(0)
    for i in range(len_ref.shape[0]):
        size = len_buf[i]
        end = end + size
        start = start + jnp.where(pos >= end, size, 0)
    angle = (pos - start).astype(f32) * freq_buf[...]
    lane = lax.broadcasted_iota(jnp.int32, (block, HEAD_SIZE), 1)
    rope[0] = jnp.cos(angle)
    rope[1] = jnp.where(lane < HEAD_SIZE // 2, -jnp.sin(angle), jnp.sin(angle))
    qkv[...] = jnp.zeros_like(qkv)

    @pl.when(apart == 1)
    def _():
        own_wait(1)
        own_start(1)

    line_steps(0, 1, 2)

    @pl.when(apart == 0)
    def _():
        act_copies[1].start()
        act_copies[3].start()

    relay(0)
    line_steps(0, 2, steps)
    relay(1)
    for copy in redis_copies:
        copy.start()
    last_in = first_out - 1

    @pl.when(inner)
    def _():
        for u in range(2, first_out):
            line_steps(u - 1, 1, steps)
            own_wait(u)
            own_start(u)
        line_steps(last_in, 1, 2)

    @pl.when(jnp.logical_not(inner))
    def _():
        for u in range(2, first_out):
            own_wait(u)
            own_start(u)

    for d in range(1, reach + 1):
        @pl.when(block_id < d)
        def _():
            kv[d] = jnp.zeros_like(kv[d])

    acts_wait()

    depth = min(1024, width)

    def project(weights, cols):
        def one(k, _):
            rows = pl.ds(pl.multiple_of(k * depth, depth), depth)
            left = acts[:, :, rows].reshape(block, depth)
            qkv[:, cols] += jnp.dot(left, weights[rows, :], preferred_element_type=f32)
            return 0

        lax.fori_loop(0, width // depth, one, 0)

    def rotated(first):
        v = qkv[:, first:first + HEAD_SIZE]
        return (v * rope[0] + pltpu.roll(v, HEAD_SIZE // 2, 1) * rope[1]).astype(bf16)

    def project_query(u):
        mate_wait(u)
        first = (u - 1) * unit_cols
        project(w_q.at[u - 1], slice(first, first + unit_cols))
        for j in range(first // HEAD_SIZE, (first + unit_cols) // HEAD_SIZE):
            query[:, j * HEAD_SIZE:(j + 1) * HEAD_SIZE] = rotated(j * HEAD_SIZE)

    def kv_copy(k):
        return remote(
            kv.at[0], kv.at[2 * k], kv_send.at[2 * k], kv_recv.at[2 * k], dev(x, y, z + k, core)
        )

    kv_mate = remote(kv.at[0], kv.at[1], kv_send.at[1], kv_recv.at[1], mate)

    def kv_pass_copy(k):
        to = 2 * k + 1 - 2 * core
        return remote(kv.at[2 * k], kv.at[to], kv_pass_send.at[2 * k], kv_recv.at[to], mate)

    def kv_passes(k):
        return (z >= k) & (2 * k + 1 - 2 * core <= reach)

    def kv_each(low, high_, body):
        def one(k, _):
            body(k)
            return 0

        lax.fori_loop(low, high_, one, 0)

    def kv_start():
        @pl.when(core == 0)
        def _():
            kv_mate.start()

        def one(k):
            @pl.when(z + k < steps)
            def _():
                kv_copy(k).start()

        kv_each(1, reach // 2 + 1, one)

    def kv_wait(d):
        remote(kv.at[d], kv.at[d], kv_send.at[d], kv_recv.at[d], mate).wait_recv()

    def kv_ready():
        def even(k):
            @pl.when(z >= k)
            def _():
                kv_wait(2 * k)

            @pl.when(kv_passes(k))
            def _():
                kv_pass_copy(k).start()

        def odd(k):
            @pl.when(block_id >= 2 * k + 1)
            def _():
                kv_wait(2 * k + 1)

        kv_each(1, reach // 2 + 1, even)
        kv_each(0, reach // 2, odd)

    own_pos = lax.broadcasted_iota(jnp.int32, (block, 1), 0)
    own_start_pos = start - block_id * block
    key_lane = lax.broadcasted_iota(jnp.int32, (1, block), 1)
    scale = HEAD_SIZE ** (-0.5) * float(np.log2(np.e))

    def attend_own(u):
        def one(j, _):
            cols = pl.ds(pl.multiple_of(j * HEAD_SIZE, HEAD_SIZE), HEAD_SIZE)
            keep = (key_lane >= own_start_pos) & (key_lane <= own_pos)
            scores = lax.dot_general(
                query[:, cols], kv[0, :, :HEAD_SIZE], (((1,), (1,)), ((), ())),
                preferred_element_type=f32,
            )
            scores = jnp.where(keep, scores, masked_score)
            new = jnp.max(scores, axis=1, keepdims=True)
            probs = jnp.exp2((scores - new) * scale)
            high[j] = new
            total[j] = jnp.sum(probs, axis=1, keepdims=True)
            accum[:, cols] = jnp.dot(probs.astype(bf16), kv[0, :, HEAD_SIZE:], preferred_element_type=f32)
            return 0

        lax.fori_loop((u - 1) * unit_heads, u * unit_heads, one, 0)

    def attend_earlier(u, d):
        keep = key_lane - d * block >= own_start_pos

        def one(j, _):
            cols = pl.ds(pl.multiple_of(j * HEAD_SIZE, HEAD_SIZE), HEAD_SIZE)
            scores = lax.dot_general(
                query[:, cols], kv[d, :, :HEAD_SIZE], (((1,), (1,)), ((), ())),
                preferred_element_type=f32,
            )
            scores = jnp.where(keep, scores, masked_score)
            old = high[j]
            new = jnp.maximum(old, jnp.max(scores, axis=1, keepdims=True))
            fading = jnp.exp2((old - new) * scale)
            probs = jnp.exp2((scores - new) * scale)
            total[j] = total[j] * fading + jnp.sum(probs, axis=1, keepdims=True)
            update = jnp.dot(probs.astype(bf16), kv[d, :, HEAD_SIZE:], preferred_element_type=f32)
            accum[:, cols] = accum[:, cols] * fading + update
            high[j] = new
            return 0

        lax.fori_loop((u - 1) * unit_heads, u * unit_heads, one, 0)

    def attend_tiles(u):
        tile = block // 4

        def one(j, _):
            cols = pl.ds(pl.multiple_of(j * HEAD_SIZE, HEAD_SIZE), HEAD_SIZE)
            for i in range(4):
                rows = slice(i * tile, (i + 1) * tile)
                spans = [(0, 0, (i + 1) * tile)]
                spans += [(d, 0, block) for d in range(1, reach)]
                spans += [(reach, i * tile, block)]
                parts = []
                for d, low, high_ in spans:
                    scores = lax.dot_general(
                        query[rows, cols], kv[d, low:high_, :HEAD_SIZE], (((1,), (1,)), ((), ())),
                        preferred_element_type=f32,
                    )
                    key_pos = low - d * block + lax.broadcasted_iota(jnp.int32, (1, high_ - low), 1)
                    keep = key_pos >= own_start_pos[rows]
                    if d == 0:
                        keep = keep & (key_pos <= own_pos[rows])
                    parts.append(jnp.where(keep, scores, masked_score))
                top = functools.reduce(jnp.maximum, [jnp.max(p, axis=1, keepdims=True) for p in parts])
                probs = [jnp.exp2((p - top) * scale) for p in parts]
                denom = sum(jnp.sum(p, axis=1, keepdims=True) for p in probs)
                result = sum(
                    jnp.dot(p.astype(bf16), kv[d, low:high_, HEAD_SIZE:], preferred_element_type=f32)
                    for p, (d, low, high_) in zip(probs, spans)
                )
                mixed[group, rows, cols] = (result / denom).astype(bf16)
            return 0

        lax.fori_loop((u - 1) * unit_heads, u * unit_heads, one, 0)

    def mix_cols(u):
        return pl.ds((u - 1) * unit_cols, unit_cols)

    def mix_copy(u, x_, y_):
        ref = mixed.at[group, :, mix_cols(u)]
        return remote(ref, ref, mix_send.at[u - 1], mix_recv.at[u - 1], dev(x_, y_, z, core))

    def attend(u):
        if reach <= 2:
            attend_tiles(u)
        else:
            attend_own(u)
            finish_heads(u)
        for x_, y_ in redis_peers():
            mix_copy(u, x_, y_).start()

    def finish_heads(u):
        def one(d, _):
            @pl.when(block_id >= d)
            def _():
                attend_earlier(u, d)
            return 0

        lax.fori_loop(1, reach + 1, one, 0)
        for j in range((u - 1) * unit_heads, u * unit_heads):
            cols = slice(j * HEAD_SIZE, (j + 1) * HEAD_SIZE)
            mixed[group, :, cols] = (accum[:, cols] / total[j]).astype(bf16)

    def mix_all(u):
        ref = mixed.at[pl.ds(0, 3), :, mix_cols(u)]
        return remote(ref, ref, mix_send.at[u - 1], mix_recv.at[u - 1], mate)

    def mix_wait():
        for u in range(1, first_out):
            mix_all(u).wait_recv()

    mate_wait(0)
    project(w_kv, slice(q_cols, q_cols + w_kv.shape[1]))
    kv[0, :, :HEAD_SIZE] = rotated(q_cols)
    kv[0, :, HEAD_SIZE:] = qkv[:, q_cols + HEAD_SIZE:].astype(bf16)
    kv_start()
    for u in range(1, last_in):
        outer_steps(u, 1, steps)
    inner_steps(last_in, 2, steps)
    for u in range(1, last_in):
        project_query(u)
    own_wait(first_out)
    own_start(first_out)

    @pl.when(jnp.logical_not(inner))
    def _():
        for u in range(first_out + 1, units):
            own_start(u)

    @pl.when(inner)
    def _():
        project_query(last_in)

    kv_ready()
    for u in range(1, last_in):
        attend(u)
    outer_steps(last_in, 1, steps)

    @pl.when(jnp.logical_not(inner))
    def _():
        project_query(last_in)

    @pl.when(inner)
    def _():
        line_step(first_out, 1)
        own_start(first_out + 1)

    attend(last_in)

    @pl.when(inner)
    def _():
        line_steps(first_out, 2, steps)
        for u in range(first_out + 1, units):
            if u + 1 < units:
                own_start(u + 1)
            line_steps(u, 1, steps)

    def out_at(g, c):
        return pl.ds(pl.multiple_of(g * col_width + out_first[c], HEAD_SIZE), out_cols[c])

    def out_part(r, c):
        return osend.at[r, :, pl.ds(out_first[c], out_cols[c])]

    def out_copy(c, y_, c_):
        return remote(
            out_part(2 * y_ + c_, c), out_ref.at[:, out_at(group, c)], out_send.at[c], out_recv.at[c],
            dev(core, y_, z, c_),
        )

    def keep_result(c):
        return pltpu.make_async_copy(out_part(h, c), out_ref.at[:, out_at(group, c)], store_sem.at[c])

    def project_out(c):
        cols = slice(out_first[c], out_first[c] + out_cols[c])
        rights = []
        for g in range(heads):
            right = w_proj[g // 2, g % 2, :, :, cols]
            if right.shape[1] % 16:
                right = right.astype(f32).reshape(-1, out_cols[c]).astype(bf16)
            else:
                right = right.reshape(-1, out_cols[c])
            rights.append(right)
        for far in (1, 0):
            y_ = far * (1 - y) + (1 - far) * y
            rows = pl.ds(pl.multiple_of(y_ * 2 * own, 2 * own), 2 * own)
            result = None
            for g in range(heads):
                term = jnp.dot(mixed[g, rows, :], rights[g], preferred_element_type=f32)
                result = term if result is None else result + term
            osend[pl.ds(2 * y_, 2), :, cols] = result.astype(bf16).reshape(2, own, out_cols[c])
            if far:
                for c_ in (0, 1):
                    out_copy(c, y_, c_).start()
                continue

            @pl.when(apart == 1)
            def _():
                for c_ in (0, 1):
                    out_copy(c, y, c_).start()

            @pl.when(apart == 0)
            def _():
                out_copy(c, y, 1 - core).start()
                keep_result(c).start()

    def drain_unit(u):
        def one(row, _):
            @pl.when((row <= z) & (z < steps - 1))
            def _():
                line_copy(u, UP, row).wait_send()

            @pl.when((row >= z) & (z > 0))
            def _():
                line_copy(u, DOWN, row).wait_send()
            return 0

        lax.fori_loop(0, steps, one, 0)
        mate_all(u).wait_send()

    def act_all(i, count):
        ref = acts.at[pl.ds(0, count)]
        return remote(ref, ref, act_send.at[i], act_recv.at[0, 0], mate)

    def drain_in():
        for u in range(first_out):
            drain_unit(u)

        @pl.when(apart == 1)
        def _():
            for u in range(first_out):
                cross_copy(u).wait_send()
            act_all(1, 1).wait_send()

        act_all(0, 2).wait_send()
        redis_all().wait_send()
        for f in (0, 1):
            @pl.when(apart == 1 - f)
            def _():
                for i in (0, 1):
                    relay_copy(i, f).wait_send()

        @pl.when(core == 0)
        def _():
            kv_mate.wait_send()

        def kv_drain(k):
            @pl.when(z + k < steps)
            def _():
                kv_copy(k).wait_send()

            @pl.when(kv_passes(k))
            def _():
                kv_pass_copy(k).wait_send()

        kv_each(1, reach // 2 + 1, kv_drain)
        for u in range(1, first_out):
            mix_all(u).wait_send()

    def out_each(c, body):
        for count in (heads - 1, heads):
            @pl.when(apart == count - heads + 1)
            def _():
                ref = out_ref.at[:, pl.ds(0, count * out_cols[c])]
                body(remote(ref, ref, out_send.at[c], out_recv.at[c], mate))

    for c in range(chunks):
        outer_steps(first_out + c, 1, steps)
        mate_wait(first_out + c)
        if c == 0:
            mix_wait()
        project_out(c)
        if c == 0:
            drain_in()
    for c in range(chunks):
        drain_unit(first_out + c)
        out_each(c, lambda copy: copy.wait_send())
    for c in range(chunks):
        out_each(c, lambda copy: copy.wait_recv())

        @pl.when(apart == 0)
        def _():
            keep_result(c).wait()


def on_device(tokens, w_query, key_value_weight, w_out, doc_lengths):
    n = lax.axis_size("blk")
    heads = lax.axis_size("heads")
    assert heads == 4
    q_units, chunks = Q_UNITS, len(OUT_PARTS)
    steps = n // LINE
    own, width = tokens.shape
    block = own * heads
    rows_in, q_cols = w_query.shape
    kv_cols = 2 * key_value_weight.shape[2]
    rows_out = w_out.shape[0]
    col_width = width // heads
    out_cols = tuple(col_width * part // sum(OUT_PARTS) for part in OUT_PARTS)
    q_heads = q_cols // HEAD_SIZE
    reach = n // 4
    units = 1 + q_units + chunks
    half = HEAD_SIZE // 2
    freqs = np.power(rope_base, -2.0 * np.arange(half) / HEAD_SIZE).astype(np.float32)
    freqs = jnp.asarray(np.concatenate([freqs, freqs])[None, :])
    bf16, f32 = jnp.bfloat16, jnp.float32
    dma = pltpu.SemaphoreType.DMA
    return pl.pallas_call(
        functools.partial(layer_kernel, n, heads, out_cols, q_units),
        out_shape=jax.ShapeDtypeStruct((own, width), bf16),
        in_specs=[pl.BlockSpec(memory_space=pl.ANY)] * 6,
        out_specs=pl.BlockSpec(memory_space=pl.ANY),
        scratch_shapes=[
            pltpu.VMEM((own, width), bf16),
            pltpu.VMEM(key_value_weight.shape, bf16),
            pltpu.VMEM((1, HEAD_SIZE), f32),
            pltpu.SMEM(doc_lengths.shape, jnp.int32),
            pltpu.VMEM((n * rows_in, kv_cols), bf16),
            pltpu.VMEM((q_units, n * rows_in, q_cols // q_units), bf16),
            pltpu.VMEM((2, 2, n, rows_out, col_width), bf16),
            pltpu.VMEM((rows_in, kv_cols), bf16),
            pltpu.VMEM((own, width), bf16),
            pltpu.VMEM((heads, own, width), bf16),
            pltpu.VMEM((block, q_cols + kv_cols), f32),
            pltpu.VMEM((block, q_cols), bf16),
            pltpu.VMEM((reach + 1, block, kv_cols), bf16),
            pltpu.VMEM((q_heads, block, 1), f32),
            pltpu.VMEM((q_heads, block, 1), f32),
            pltpu.VMEM((block, q_cols), f32),
            pltpu.VMEM((heads, block, q_cols), bf16),
            pltpu.VMEM((2, block, HEAD_SIZE), f32),
            pltpu.VMEM((heads, own, col_width), bf16),
            dma((units, steps + 1)),
            dma((units,)),
            dma((units, steps)),
            dma((units,)),
            dma((1 + q_units,)),
            dma((1 + q_units,)),
            dma((4,)),
            dma((chunks,)),
            dma((1,)),
            dma((1,)),
            dma((4,)),
            dma((2, heads)),
            dma((reach + 1,)),
            dma((reach + 1,)),
            dma((reach + 1,)),
            dma((q_units,)),
            dma((q_units,)),
            dma((chunks,)),
            dma((chunks,)),
        ],
        compiler_params=pltpu.CompilerParams(
            collective_id=0, has_side_effects=True, vmem_limit_bytes=60 * 1024 * 1024
        ),
    )(tokens, w_query, key_value_weight, w_out, doc_lengths, freqs)


def solution(mesh):
    return jax.shard_map(
        on_device,
        mesh=mesh,
        in_specs=(
            P(("blk", "heads"), None),
            P("blk", "heads"),
            P("blk", None, "heads"),
            P(("heads", "blk"), None),
            P(),
        ),
        out_specs=P(("blk", "heads"), None),
        check_vma=False,
    )
```
